256 devices in a mesh: gx: 8 (over z), gy: 8 (over y, core), gz: 4 (over x).
Axes of the slice: x: 4, y: 4, z: 8, core: 2. Of those that a mesh axis runs over, the one named last changes fastest.
Arguments:
- density: float32 [64, 64, 512], P('gx', 'gy', 'gz'), may hold values from 0.5 to 2
- base_velocity: float32 [3, 64, 64, 512], P(None, 'gx', 'gy', 'gz'), may hold values from -0.4 to 0.4
- cells: int32 [3, 65536], P(None, ('gx', 'gy', 'gz')), may hold values from 0 to 511, as said below
- offsets: float32 [3, 65536], P(None, ('gx', 'gy', 'gz')), may hold values from 0 to 1
- target: float32 [3, 65536], P(None, ('gx', 'gy', 'gz')), may hold values from -0.4 to 0.4
- stiffness: float32 [65536], P(('gx', 'gy', 'gz')), may hold values from 0.01 to 0.1
- counts: int32 [256], P(('gx', 'gy', 'gz')), may hold values from 1 to 256, as said below
Outputs:
- forces: float32 [3, 65536], P(None, ('gx', 'gy', 'gz'))
The draws below stay inside these ranges and needn't reach their ends.
Inputs may be any that keep to these rules, and one draw needn't show every extreme that they name: `cells`: each marker's cell lies inside the lattice block of the device that holds its slot. `counts`: some device holds exactly 256 live markers in every draw.
All inputs are finite; a program needn't handle non-finite values.
Results may differ from the reference program's by a relative error of at most 0.0001.
Values sent between devices are 32-bit elements; how exact they have to be, the bound alone decides.
No kernel may reach another device: no remote copies, remote signals or barrier semaphores. Data moves between devices by JAX's collectives and lax.ppermute only.
A program may use at most 64 MiB of HBM per device.

```python
import math
import jax
import jax.numpy as jnp
from jax import lax

CX = 8
CY = 8
CZ = 128
CAP = 256
ITERS = 3
NX = 64
NY = 64
NZ = 512
SLOTS = 65536
DEVICES = 256


def draw_cells(key, part):
    blocks_y = NY // CY
    blocks_z = NZ // CZ
    device = jnp.arange(SLOTS, dtype=jnp.int32) // CAP
    block_x = device // (blocks_y * blocks_z)
    block_y = device // blocks_z % blocks_y
    block_z = device % blocks_z
    keys = jax.random.split(key, 3)
    inside_x = jax.random.randint(keys[0], (SLOTS,), 0, CX, dtype=jnp.int32)
    inside_y = jax.random.randint(keys[1], (SLOTS,), 0, CY, dtype=jnp.int32)
    inside_z = jax.random.randint(keys[2], (SLOTS,), 0, CZ, dtype=jnp.int32)
    return jnp.stack([block_x * CX + inside_x, block_y * CY + inside_y, block_z * CZ + inside_z]).astype(jnp.int32)


def draw_counts(key, part):
    keys = jax.random.split(key, 3)
    divisor = 1 + jax.random.randint(keys[0], (DEVICES,), 0, 6, dtype=jnp.int32)
    jitter = jax.random.randint(keys[1], (DEVICES,), 0, CAP // 8 + 1, dtype=jnp.int32)
    loads = jnp.maximum(CAP // divisor - jitter, 1)
    fullest = jax.random.randint(keys[2], (), 0, DEVICES, dtype=jnp.int32)
    loads = jnp.where(jnp.arange(DEVICES, dtype=jnp.int32) == fullest, CAP, loads)
    return loads.astype(jnp.int32)


def levels(stream_key, extent, shards, low, largest):
    level, own = 1.0, jax.random.fold_in(stream_key, 6)
    for axis_at, blocks in shards:
        steps = jnp.exp(jax.random.uniform(jax.random.fold_in(own, axis_at), (blocks,), jnp.float32, low / len(shards), largest / len(shards)))
        level = level * jnp.repeat(steps, extent[axis_at] // blocks).reshape([-1 if axis == axis_at else 1 for axis in range(len(extent))])
    return level


def normal_values(stream_key, dims, scale, limit, shards=(), kind=jnp.bfloat16):
    values = scale * jax.random.normal(stream_key, dims, jnp.float32)
    if shards:
        values = values * levels(stream_key, dims, shards, -0.22, 0.18)
    return jnp.clip(values, -limit, limit).astype(kind)


def setup_inputs(seed: int = 0) -> dict:
    seeds = jax.random.split(jax.random.key(seed), 8)
    return {
        "density": jnp.clip(jnp.exp(math.log(2.0) - 1.3862944 * jax.random.uniform(seeds[0], (NX, NY, NZ), jnp.float32) ** levels(seeds[0], (NX, NY, NZ), ((0, 8), (1, 8), (2, 4)), -0.2, 0.2)), 0.5, 2.0),
        "base_velocity": normal_values(seeds[1], (3, NX, NY, NZ), 0.05, 0.4, ((1, 8), (2, 8), (3, 4)), jnp.float32),
        "cells": draw_cells(jax.random.fold_in(seeds[7], 71), 0),
        "offsets": jnp.clip(1.0 * jax.random.uniform(seeds[3], (3, SLOTS), jnp.float32) ** levels(seeds[3], (3, SLOTS), ((1, 256),), -0.2, 0.2), 0.0, 1.0),
        "target": normal_values(seeds[4], (3, SLOTS), 0.05, 0.4, ((1, 256),), jnp.float32),
        "stiffness": jnp.clip(jnp.exp(math.log(0.1) - 2.3025851 * jax.random.uniform(seeds[5], (SLOTS,), jnp.float32) ** levels(seeds[5], (SLOTS,), ((0, 256),), -0.2, 0.2)), 0.01, 0.1),
        "counts": draw_counts(jax.random.fold_in(seeds[7], 71), 0),
    }


def moving_directions():
    listing = []
    for along_x in (-1, 0, 1):
        for along_y in (-1, 0, 1):
            for along_z in (-1, 0, 1):
                order = abs(along_x) + abs(along_y) + abs(along_z)
                if order == 1:
                    listing.append((along_x, along_y, along_z, 1.0 / 18.0))
                elif order == 2:
                    listing.append((along_x, along_y, along_z, 1.0 / 36.0))
    return listing

def delta_weights(fraction):

    def inner(radius):
        return (3.0 - 2.0 * radius + jnp.sqrt(1.0 + 4.0 * radius - 4.0 * radius * radius)) / 8.0

    def outer(radius):
        return (5.0 - 2.0 * radius - jnp.sqrt(-7.0 + 12.0 * radius - 4.0 * radius * radius)) / 8.0
    return jnp.stack([outer(1.0 + fraction), inner(fraction), inner(1.0 - fraction), outer(2.0 - fraction)])

def reference(density, base_velocity, cells, offsets, target, stiffness, counts):
    live = (jnp.arange(CAP, dtype=jnp.int32)[None, :] < counts[:, None]).reshape(-1).astype(jnp.float32)
    scale = lax.rsqrt(density)
    weight_x = delta_weights(offsets[0])
    weight_y = delta_weights(offsets[1])
    weight_z = delta_weights(offsets[2])
    index_x = [((cells[0] + shift - 1) % NX).astype(jnp.int32) for shift in range(4)]
    index_y = [((cells[1] + shift - 1) % NY).astype(jnp.int32) for shift in range(4)]
    index_z = [((cells[2] + shift - 1) % NZ).astype(jnp.int32) for shift in range(4)]
    directions = moving_directions()

    def interpolate(field):
        total = jnp.zeros((3, SLOTS), jnp.float32)
        for first in range(4):
            for second in range(4):
                for third in range(4):
                    weight = weight_x[first] * weight_y[second] * weight_z[third]
                    total = total + field[:, index_x[first], index_y[second], index_z[third]] * weight
        return total

    def spread(vector):
        grid = jnp.zeros((3, NX, NY, NZ), jnp.float32)
        for first in range(4):
            for second in range(4):
                for third in range(4):
                    weight = weight_x[first] * weight_y[second] * weight_z[third]
                    grid = grid.at[:, index_x[first], index_y[second], index_z[third]].add(vector * weight)
        return grid

    def apply(vector):
        moved = scale * spread(vector)
        post = [jnp.zeros((NX, NY, NZ), jnp.float32) for component in range(3)]
        for along_x, along_y, along_z, share in directions:
            population = 3.0 * share * (along_x * moved[0] + along_y * moved[1] + along_z * moved[2])
            shifted = jnp.roll(population, (along_x, along_y, along_z), axis=(0, 1, 2))
            for component, along in enumerate((along_x, along_y, along_z)):
                if along != 0:
                    post[component] = post[component] + along * shifted
        velocity = scale * (moved + jnp.stack(post)) * 0.5
        return live * (interpolate(velocity) + stiffness * vector)
    right = live * (target - interpolate(base_velocity))
    solution = jnp.zeros_like(right)
    residual = right
    direction = right
    norm_now = jnp.sum(residual * residual)
    for step in range(ITERS):
        image = apply(direction)
        alpha = norm_now / jnp.sum(direction * image)
        solution = solution + alpha * direction
        residual = residual - alpha * image
        norm_next = jnp.sum(residual * residual)
        direction = residual + norm_next / norm_now * direction
        norm_now = norm_next
    return solution
```

```python
import jax
import jax.numpy as jnp
from jax import lax
from jax.experimental import pallas as pl
from jax.experimental.pallas import tpu as pltpu
from jax.sharding import Mesh
from jax.sharding import PartitionSpec as P

GY = ("gy_0", "gy_1")
GX_GY_GZ = ("gx", "gy_0", "gy_1", "gz")

PLANES = 13
YPAD = 16
ROWS = PLANES * YPAD
INNER = 11 * YPAD
LANES = 256
BLOCKS = 9
MARKERS = 256
COLS = BLOCKS * MARKERS
F32 = jnp.float32
BF16 = jnp.bfloat16
PARAMS = pltpu.CompilerParams(vmem_limit_bytes=48 * 1024 * 1024)


def shifted(shard, axis, by):
    length = lax.axis_size(axis)
    return lax.ppermute(shard, axis, [(i, (i + by) % length) for i in range(length)])


def halves(value):
    high = value.astype(BF16)
    return high, (value - high.astype(F32)).astype(BF16)


def transposed_dot(left, right):
    return lax.dot_general(left, right, (((1,), (1,)), ((), ())), preferred_element_type=F32)


def plain_dot(left, right):
    return lax.dot_general(left, right, (((1,), (0,)), ((), ())), preferred_element_type=F32)


def delta_rows(extent, cell, fraction):
    step = lax.broadcasted_iota(jnp.int32, (extent, cell.shape[1]), 0).astype(F32) - cell
    radius = jnp.abs(step - fraction)
    near = (step == 0.0) | (step == 1.0)
    far = (step == -1.0) | (step == 2.0)
    inner = (3.0 - 2.0 * radius + jnp.sqrt(jnp.maximum(1.0 + 4.0 * radius - 4.0 * radius * radius, 0.0))) / 8.0
    outer = (5.0 - 2.0 * radius - jnp.sqrt(jnp.maximum(-7.0 + 12.0 * radius - 4.0 * radius * radius, 0.0))) / 8.0
    return jnp.where(near, inner, jnp.where(far, outer, 0.0))


def assemble_kernel(own, below_x, above_x, below_y, above_y, main, low, high):
    main[...] = jnp.ones(main.shape, F32)
    for field in range(4):
        for plane in range(PLANES):
            row = field * ROWS + plane * YPAD
            if plane < 2:
                piece = below_x[field, plane]
            elif plane < 10:
                piece = own[field, plane - 2]
            else:
                piece = above_x[field, plane - 10]
            main[row + 2 : row + 10, :] = piece
            main[row : row + 2, :] = below_y[field, plane]
            main[row + 10 : row + 13, :] = above_y[field, plane]
    for block in range(7):
        turned = main[block * 128 : block * 128 + 128, :].T
        low[:, block * 128 : block * 128 + 128] = turned[0:8]
        high[:, block * 128 : block * 128 + 128] = turned[120:128]


def tables_kernel(own, below_x, above_x, below_y, above_y, plane_weights, z_high, z_low):
    pieces = [(own, 0, 0.0, 0.0), (below_x, 0, -8.0, 0.0), (above_x, 0, 8.0, 0.0)]
    for group, along_y in ((below_y, -8.0), (above_y, 8.0)):
        for part, along_x in enumerate((0.0, -8.0, 8.0)):
            pieces.append((group, 16 * part, along_x, along_y))
    for block, (ref, first, along_x, along_y) in enumerate(pieces):
        for half in range(2):
            row = lambda k: ref[first + 2 * k + half : first + 2 * k + half + 1, :]
            place = slice(block * 256 + half * 128, block * 256 + half * 128 + 128)
            plane_weights[0:16, place] = delta_rows(16, row(0) + (along_x + 2.0), row(3))
            plane_weights[16:32, place] = delta_rows(16, row(1) + (along_y + 2.0), row(4))
            high, rest = halves(delta_rows(144, row(2) + 2.0, row(5)))
            z_high[0:144, place] = high
            z_low[0:144, place] = rest
    z_high[144:256, :] = jnp.zeros((112, COLS), BF16)
    z_low[144:256, :] = jnp.zeros((112, COLS), BF16)


def interpolated(velocity, plane_weights, z_high, z_low):
    rows = []
    for field in velocity:
        high, rest = halves(field)
        partial = plain_dot(high, z_high) + plain_dot(rest, z_high) + plain_dot(high, z_low)
        total = jnp.zeros((YPAD, MARKERS), F32)
        for plane in range(11):
            total = total + partial[plane * YPAD : plane * YPAD + YPAD] * plane_weights[plane + 1 : plane + 2, 0:MARKERS]
        line = jnp.sum(total * plane_weights[16:32, 0:MARKERS], axis=0, keepdims=True)
        rows += [line[:, 0:128], line[:, 128:256]]
    rows.append(jnp.zeros((2, 128), F32))
    return jnp.concatenate(rows, axis=0)


def setup_kernel(main, low, high, plane_weights, z_high, z_low, aux, scale, start, wide):
    lane = lax.broadcasted_iota(jnp.int32, (128, 128), 1)
    row8 = lax.broadcasted_iota(jnp.int32, (8, 128), 0)
    for block in range(7):
        place = slice(block * 128, block * 128 + 128)
        edge = jnp.where(row8 < 2, pltpu.roll(high[:, place], 2, 0), pltpu.roll(low[:, place], 2, 0))
        edge = jnp.concatenate([edge, jnp.zeros((120, 128), F32)], axis=0).T
        body_rows = pltpu.roll(main[place, :], 2, 1)
        wide[place, 0:128] = jnp.where(lane < 2, edge, body_rows)
        wide[place, 128:256] = jnp.where(lane < 2, body_rows, jnp.where(lane < 5, edge, 1.0))
    scale[...] = lax.rsqrt(wide[3 * ROWS : 4 * ROWS, :])
    velocity = [wide[c * ROWS + YPAD : c * ROWS + YPAD + INNER, :] for c in range(3)]
    image = interpolated(velocity, plane_weights, z_high[:, 0:MARKERS], z_low[:, 0:MARKERS])
    start[...] = aux[0:8, :] * (aux[16:24, :] - image)


def spread_kernel(
    own, below_x, above_x, below_y, above_y, plane_weights, z_high, z_low, scale, velocity, low, high, left_high, left_low, field, edges
):
    pieces = [(own, 0), (below_x, 0), (above_x, 0)]
    pieces += [(below_y, 8 * part) for part in range(3)] + [(above_y, 8 * part) for part in range(3)]
    for block, (ref, first) in enumerate(pieces):
        for half in range(2):
            place = slice(block * 256 + half * 128, block * 256 + half * 128 + 128)
            along_y = plane_weights[16:32, place]
            vector = [ref[first + 2 * c + half : first + 2 * c + half + 1, :] * along_y for c in range(3)]
            for plane in range(PLANES):
                along_x = plane_weights[plane : plane + 1, place]
                for c in range(3):
                    top, rest = halves(vector[c] * along_x)
                    row = c * ROWS + plane * YPAD
                    left_high[row : row + YPAD, place] = top
                    left_low[row : row + YPAD, place] = rest
    for c in range(3):
        rows = slice(c * ROWS, c * ROWS + ROWS)
        moved = transposed_dot(left_high[rows, :], z_high[...])
        moved += transposed_dot(left_low[rows, :], z_high[...])
        moved += transposed_dot(left_high[rows, :], z_low[...])
        field[rows, :] = moved * scale[...]
    axial, diagonal = 1.0 / 6.0, 1.0 / 12.0
    up_y = lambda a: pltpu.roll(a, 1, 0)
    down_y = lambda a: pltpu.roll(a, YPAD - 1, 0)
    up_z = lambda a: pltpu.roll(a, 1, 1)
    down_z = lambda a: pltpu.roll(a, LANES - 1, 1)
    onward = [None] * PLANES
    back = [None] * PLANES
    still = [None] * PLANES
    lane = lax.broadcasted_iota(jnp.int32, (YPAD, 128), 1)
    edges[INNER:256, :] = jnp.zeros((256 - INNER, 128), F32)
    for plane in range(PLANES):
        gx, gy, gz = (field[c * ROWS + plane * YPAD : c * ROWS + plane * YPAD + YPAD, :] for c in range(3))
        hx, hy, hz = gx * diagonal, gy * diagonal, gz * diagonal
        sum_xy, dif_xy = hx + hy, hx - hy
        zx_up, zy_up, zz_up = up_z(hx), up_z(hy), up_z(hz)
        zx_dn, zy_dn, zz_dn = down_z(hx), down_z(hy), down_z(hz)
        xz_sum_up, xz_sum_dn, xz_dif_up, xz_dif_dn = zx_up + zz_up, zx_dn + zz_dn, zx_up - zz_up, zx_dn - zz_dn
        xy_sum_up, xy_sum_dn, xy_dif_up, xy_dif_dn = up_y(sum_xy), down_y(sum_xy), up_y(dif_xy), down_y(dif_xy)
        ax = gx * axial
        onward[plane] = (
            ax + ((xy_sum_up + xy_dif_dn) + (xz_sum_up + xz_dif_dn)),
            xy_sum_up - xy_dif_dn,
            xz_sum_up - xz_dif_dn,
        )
        back[plane] = (
            ax + ((xy_sum_dn + xy_dif_up) + (xz_sum_dn + xz_dif_up)),
            xy_sum_dn - xy_dif_up,
            xz_sum_dn - xz_dif_up,
        )
        yz_same = up_y(zy_up + zz_up)
        yz_same_dn = down_y(zy_dn + zz_dn)
        yz_cross = up_y(zy_dn - zz_dn)
        yz_cross_dn = down_y(zy_up - zz_up)
        same, cross = yz_same + yz_same_dn, yz_cross + yz_cross_dn
        still[plane] = (
            gx,
            gy + ((up_y(hy) + down_y(hy)) * 2.0 + (same + cross)),
            gz + ((zz_up + zz_dn) * 2.0 + (same - cross)),
        )
        if plane >= 2:
            out = plane - 1
            factor = scale[out * YPAD : out * YPAD + YPAD, :] * 0.5
            first = (out - 1) * YPAD
            packed = jnp.zeros((YPAD, 128), F32)
            for c in range(3):
                value = (still[out][c] + (onward[out - 1][c] + back[out + 1][c])) * factor
                velocity[c * INNER + first : c * INNER + first + YPAD, :] = value
                near = value[:, 0:128]
                beyond = value[:, 128:256]
                near = pltpu.roll(near, 4 * c, 1) if c else near
                packed = jnp.where((lane >= 4 * c) & (lane < 4 * c + 4), near, packed)
                at = 16 + 4 * c
                packed = jnp.where((lane >= at) & (lane < at + 4), pltpu.roll(beyond, at - 1, 1), packed)
            edges[first : first + YPAD, :] = packed
    for block in range(2):
        place = slice(block * 128, block * 128 + 128)
        turned = edges[place, :].T
        low[:, place] = turned[0:16]
        high[:, place] = turned[16:32]


def apply_image(velocity, low, high, plane_weights, z_high, z_low, aux, vector):
    lane = lax.broadcasted_iota(jnp.int32, (INNER, 128), 1)
    columns = []
    for block in range(2):
        place = slice(block * 128, block * 128 + 128)
        columns.append(jnp.concatenate([high[:, place], low[:, place], jnp.zeros((96, 128), F32)], axis=0).T)
    edge = jnp.concatenate(columns, axis=0)[0:INNER]
    fields = []
    for c in range(3):
        mine = velocity[c * INNER : c * INNER + INNER, :]
        near = jnp.where((lane >= 1) & (lane < 5), pltpu.roll(edge, (1 - 4 * c) % 128, 1), 0.0)
        beyond = jnp.where(lane < 4, pltpu.roll(edge, (112 - 4 * c) % 128, 1), 0.0)
        fields.append(mine + jnp.concatenate([near, beyond], axis=1))
    image = interpolated(fields, plane_weights, z_high[:, 0:MARKERS], z_low[:, 0:MARKERS])
    return aux[0:8, :] * (image + aux[8:16, :] * vector[...])


def image_kernel(velocity, low, high, plane_weights, z_high, z_low, aux, vector, result):
    result[...] = apply_image(velocity, low, high, plane_weights, z_high, z_low, aux, vector)


def two_sum(a, b):
    total = a + b
    part = total - a
    return total, (a - (total - part)) + (b - part)


def fast_two_sum(a, b):
    total = a + b
    return total, b - (total - a)


def split(a):
    scaled = a * 4097.0
    high = scaled - (scaled - a)
    return high, a - high


def two_product(a, b):
    product = a * b
    a_high, a_low = split(a)
    b_high, b_low = split(b)
    return product, ((a_high * b_high - product) + a_high * b_low + a_low * b_high) + a_low * b_low


def pair_add(a, b):
    head, tail = two_sum(a[0], b[0])
    return fast_two_sum(head, tail + (a[1] + b[1]))


def pair_negative(a):
    return (-a[0], -a[1])


def pair_multiply(a, b):
    head, tail = two_product(a[0], b[0])
    return fast_two_sum(head, tail + (a[0] * b[1] + a[1] * b[0]))


def pair_divide(a, b):
    first = a[0] / b[0]
    rest = pair_add(a, pair_negative(pair_multiply((first, jnp.zeros_like(first)), b)))
    return fast_two_sum(first, rest[0] / b[0])


ENTRIES = ((0, 0), (0, 1), (0, 2), (0, 3), (1, 1), (1, 2), (1, 3), (2, 2), (2, 3))


def last_kernel(velocity, low, high, plane_weights, z_high, z_low, aux, first, second, third, sums):
    fourth = apply_image(velocity, low, high, plane_weights, z_high, z_low, aux, third)
    vectors = [first[...], second[...], third[...], fourth]
    lane = lax.broadcasted_iota(jnp.int32, (8, 128), 1)
    packed = jnp.zeros((8, 128), F32)
    for at, (i, j) in enumerate(ENTRIES):
        value = two_product(vectors[i], vectors[j])
        for axis, steps in ((0, (4, 2, 1)), (1, (64, 32, 16, 8, 4, 2, 1))):
            for step in steps:
                value = pair_add(value, (pltpu.roll(value[0], step, axis), pltpu.roll(value[1], step, axis)))
        packed = jnp.where(lane == at, value[0], jnp.where(lane == 16 + at, value[1], packed))
    for block in range(sums.shape[0] // 8):
        sums[block * 8 : block * 8 + 8, :] = packed


def finish_kernel(gathered, first, second, third, forces):
    a = gathered[...]
    count = a.shape[0]
    value = (a, pltpu.roll(a, 112, 1))
    while count > 8:
        count //= 2
        value = pair_add(
            (value[0][0:count], value[1][0:count]), (value[0][count : 2 * count], value[1][count : 2 * count])
        )
    for step in (4, 2, 1):
        value = pair_add(value, (pltpu.roll(value[0], step, 0), pltpu.roll(value[1], step, 0)))
    lane = lax.broadcasted_iota(jnp.int32, (8, 128), 1)
    gram = {}
    for at, (i, j) in enumerate(ENTRIES):
        entry = tuple(
            jnp.broadcast_to(jnp.sum(jnp.where(lane == at, v, 0.0), axis=1, keepdims=True), (8, 128)) for v in value
        )
        gram[i, j] = entry
        gram[j, i] = entry
    add, times = pair_add, pair_multiply
    minus = lambda a, b: pair_add(a, pair_negative(b))

    def form(left, right, shift):
        total = None
        for i, a in enumerate(left):
            for j, b in enumerate(right):
                term = times(times(a, b), gram[i, j + shift])
                total = term if total is None else add(total, term)
        return total

    one = (jnp.ones((8, 128), F32), jnp.zeros((8, 128), F32))
    alpha0 = pair_divide(gram[0, 0], gram[0, 1])
    residual = [one, pair_negative(alpha0)]
    norm1 = form(residual, residual, 0)
    beta0 = pair_divide(norm1, gram[0, 0])
    along1 = [add(one, beta0), pair_negative(alpha0)]
    alpha1 = pair_divide(norm1, form(along1, along1, 1))
    residual = [one, minus(residual[1], times(alpha1, along1[0])), pair_negative(times(alpha1, along1[1]))]
    norm2 = form(residual, residual, 0)
    beta1 = pair_divide(norm2, norm1)
    along2 = [add(one, times(beta1, along1[0])), add(residual[1], times(beta1, along1[1])), residual[2]]
    alpha2 = pair_divide(norm2, form(along2, along2, 1))
    weight0 = add(alpha0, add(times(alpha1, along1[0]), times(alpha2, along2[0])))
    weight1 = add(times(alpha1, along1[1]), times(alpha2, along2[1]))
    weight2 = times(alpha2, along2[2])
    total = weight0[0] * first[...] + (weight1[0] * second[...] + weight2[0] * third[...])
    for c in range(3):
        forces[c : c + 1, 0:128] = total[2 * c : 2 * c + 1, :]
        forces[c : c + 1, 128:256] = total[2 * c + 1 : 2 * c + 2, :]


def call(kernel, name, outs, *operands, scratch=()):
    whole = pl.BlockSpec(memory_space=pltpu.VMEM)
    return pl.pallas_call(
        kernel,
        name=name,
        out_shape=[jax.ShapeDtypeStruct(shape, kind) for shape, kind in outs],
        in_specs=[whole] * len(operands),
        out_specs=[whole] * len(outs),
        scratch_shapes=list(scratch),
        compiler_params=PARAMS,
    )(*operands)


def body(density, base_velocity, cells, offsets, target, stiffness, counts):
    anchor = jnp.stack([lax.axis_index("gx") * 8, lax.axis_index(GY) * 8, lax.axis_index("gz") * 128])
    local = (cells - anchor[:, None]).astype(F32)
    lines = lambda a: a.reshape(-1, 128)
    zeros = lambda n: jnp.zeros((n, 128), F32)
    markers = jnp.concatenate([lines(local), lines(offsets), zeros(4)], axis=0)
    live = lines((jnp.arange(MARKERS, dtype=jnp.int32) < counts[0]).astype(F32))
    stiff = lines(stiffness)
    aux = jnp.concatenate(
        [live, live, live, zeros(2), stiff, stiff, stiff, zeros(2), lines(target), zeros(2)], axis=0
    )
    fields = jnp.concatenate([base_velocity, density[None]], axis=0)

    below_x = shifted(fields[:, 6:8], "gx", 1)
    above_x = shifted(fields[:, 0:3], "gx", -1)
    marks_below_x, marks_above_x = shifted(markers, "gx", 1), shifted(markers, "gx", -1)
    deep = jnp.concatenate([below_x, fields, above_x], axis=1)
    below_y = shifted(deep[:, :, 6:8], GY, 1)
    above_y = shifted(deep[:, :, 0:3], GY, -1)
    marks = jnp.concatenate([markers, marks_below_x, marks_above_x], axis=0)
    marks_below_y, marks_above_y = shifted(marks, GY, 1), shifted(marks, GY, -1)
    main, low, high = call(
        assemble_kernel, "assemble", [((896, 128), F32), ((8, 896), F32), ((8, 896), F32)],
        fields, below_x, above_x, below_y, above_y,
    )
    plane_weights, z_high, z_low = call(
        tables_kernel, "tables", [((32, COLS), F32), ((256, COLS), BF16), ((256, COLS), BF16)],
        markers, marks_below_x, marks_above_x, marks_below_y, marks_above_y,
    )
    from_above = shifted(low, "gz", -1)
    from_below = shifted(high, "gz", 1)
    tables = (plane_weights, z_high, z_low)
    scale, start = call(
        setup_kernel, "setup", [((ROWS, LANES), F32), ((8, 128), F32)],
        main, from_above, from_below, *tables, aux,
        scratch=[pltpu.VMEM((896, LANES), F32)],
    )

    def spread(vector):
        below, above = shifted(vector, "gx", 1), shifted(vector, "gx", -1)
        three = jnp.concatenate([vector, below, above], axis=0)
        below_three, above_three = shifted(three, GY, 1), shifted(three, GY, -1)
        velocity, low, high = call(
            spread_kernel, "spread", [((3 * INNER, LANES), F32), ((16, 256), F32), ((16, 256), F32)],
            vector, below, above, below_three, above_three, *tables, scale,
            scratch=[
                pltpu.VMEM((3 * ROWS, COLS), BF16), pltpu.VMEM((3 * ROWS, COLS), BF16),
                pltpu.VMEM((3 * ROWS, LANES), F32), pltpu.VMEM((256, 128), F32),
            ],
        )
        return velocity, shifted(low, "gz", -1), shifted(high, "gz", 1)

    vectors = [start]
    for step in range(2):
        (image,) = call(
            image_kernel, "image", [((8, 128), F32)],
            *spread(vectors[-1]), *tables, aux, vectors[-1],
        )
        vectors.append(image)
    (sums,) = call(
        last_kernel, "last", [((256, 128), F32)],
        *spread(vectors[-1]), *tables, aux, *vectors,
    )
    gathered = lax.all_to_all(sums, GX_GY_GZ, 0, 0, tiled=True)
    (forces,) = call(finish_kernel, "finish", [((3, MARKERS), F32)], gathered, *vectors)
    return forces


def solution(mesh):
    finer = Mesh(
        mesh.devices.reshape(mesh.shape["gx"], 4, 2, mesh.shape["gz"]), ("gx", "gy_0", "gy_1", "gz")
    )
    return jax.shard_map(
        body,
        mesh=finer,
        in_specs=(
            P("gx", GY, "gz"),
            P(None, "gx", GY, "gz"),
            P(None, GX_GY_GZ),
            P(None, GX_GY_GZ),
            P(None, GX_GY_GZ),
            P(GX_GY_GZ),
            P(GX_GY_GZ),
        ),
        out_specs=P(None, GX_GY_GZ),
        check_vma=False,
    )
```

```python
import jax
import jax.numpy as jnp
from jax import lax
from jax.experimental import pallas as pl
from jax.experimental.pallas import tpu as pltpu
from jax.sharding import Mesh
from jax.sharding import PartitionSpec as P

GY = ("gy_0", "gy_1")
GX_GY_GZ = ("gx", "gy_0", "gy_1", "gz")

PLANES = 13
YPAD = 16
ROWS = PLANES * YPAD
INNER = 11 * YPAD
LANES = 256
BLOCKS = 9
MARKERS = 256
COLS = BLOCKS * MARKERS
F32 = jnp.float32
BF16 = jnp.bfloat16
PARAMS = pltpu.CompilerParams(vmem_limit_bytes=48 * 1024 * 1024)


def shifted(shard, axis, by):
    length = lax.axis_size(axis)
    return lax.ppermute(shard, axis, [(i, (i + by) % length) for i in range(length)])


def halves(value):
    high = value.astype(BF16)
    return high, (value - high.astype(F32)).astype(BF16)


def transposed_dot(left, right):
    return lax.dot_general(left, right, (((1,), (1,)), ((), ())), preferred_element_type=F32)


def plain_dot(left, right):
    return lax.dot_general(left, right, (((1,), (0,)), ((), ())), preferred_element_type=F32)


def delta_rows(extent, cell, fraction):
    step = lax.broadcasted_iota(jnp.int32, (extent, cell.shape[1]), 0).astype(F32) - cell
    radius = jnp.abs(step - fraction)
    near = (step == 0.0) | (step == 1.0)
    far = (step == -1.0) | (step == 2.0)
    inner = (3.0 - 2.0 * radius + jnp.sqrt(jnp.maximum(1.0 + 4.0 * radius - 4.0 * radius * radius, 0.0))) / 8.0
    outer = (5.0 - 2.0 * radius - jnp.sqrt(jnp.maximum(-7.0 + 12.0 * radius - 4.0 * radius * radius, 0.0))) / 8.0
    return jnp.where(near, inner, jnp.where(far, outer, 0.0))


def pack_kernel(
    density_in, base_in, cells_in, offsets_in, target_in, stiffness_in, counts, fields, marks, aux, upward, downward,
    density, base, cells, offsets, target, stiffness, arrived,
):
    sources = (density_in, base_in, cells_in, offsets_in, target_in, stiffness_in)
    places = (density, base, cells, offsets, target, stiffness)
    copies = [pltpu.make_async_copy(a, b, arrived.at[i]) for i, (a, b) in enumerate(zip(sources, places))]
    for copy in copies:
        copy.start()
    for copy in copies:
        copy.wait()
    for plane in range(8):
        for field in range(4):
            piece = density[plane] if field == 3 else base[field, plane]
            fields[(field * 8 + plane) * 8 : (field * 8 + plane) * 8 + 8, :] = piece
            row = (field * 8 + plane) * 2
            upward[row : row + 2, :] = piece[6:8]
            row = (field * 8 + plane) * 3
            downward[row : row + 3, :] = piece[0:3]
    lane = lax.broadcasted_iota(jnp.int32, (1, 128), 1)
    marks[12:16, :] = jnp.zeros((4, 128), F32)
    for group in range(3):
        aux[8 * group + 6 : 8 * group + 8, :] = jnp.zeros((2, 128), F32)
    for half in range(2):
        place = slice(half * 128, half * 128 + 128)
        live = jnp.where(lane + half * 128 < counts[0], 1.0, 0.0).astype(F32)
        for k in range(3):
            inside = cells[k : k + 1, place] & (7, 7, 127)[k]
            row = 2 * k + half
            marks[row : row + 1, :] = inside.astype(F32)
            marks[row + 6 : row + 7, :] = offsets[k : k + 1, place]
            aux[row : row + 1, :] = live
            aux[row + 8 : row + 9, :] = stiffness[0:1, place]
            aux[row + 16 : row + 17, :] = target[k : k + 1, place]
    upward[64:80, :] = marks[...]
    downward[96:112, :] = marks[...]


def deepen_kernel(fields, marks, below, above, deep, three, upward, downward):
    for field in range(4):
        for plane in range(8):
            at = field * 8 + plane
            row = at * YPAD
            deep[row : row + 2, :] = below[at * 2 : at * 2 + 2, :]
            deep[row + 2 : row + 10, :] = fields[at * 8 : at * 8 + 8, :]
            deep[row + 10 : row + 13, :] = above[at * 3 : at * 3 + 3, :]
            deep[row + 13 : row + 16, :] = jnp.ones((3, 128), F32)
    for field in range(4):
        upward[field * 32 : field * 32 + 32, :] = deep[field * 128 + 96 : field * 128 + 128, :]
        downward[field * 48 : field * 48 + 48, :] = deep[field * 128 : field * 128 + 48, :]
    three[0:16, :] = marks[...]
    three[16:32, :] = below[64:80, :]
    three[32:48, :] = above[96:112, :]
    upward[128:176, :] = three[...]
    downward[192:240, :] = three[...]


def assemble_kernel(deep, below, above, main, low, high):
    for field in range(4):
        row = field * ROWS
        main[row : row + 32, :] = below[field * 32 : field * 32 + 32, :]
        main[row + 32 : row + 160, :] = deep[field * 128 : field * 128 + 128, :]
        main[row + 160 : row + 208, :] = above[field * 48 : field * 48 + 48, :]
    main[4 * ROWS : 896, :] = jnp.ones((896 - 4 * ROWS, 128), F32)
    for block in range(7):
        turned = main[block * 128 : block * 128 + 128, :].T
        low[:, block * 128 : block * 128 + 128] = turned[0:8]
        high[:, block * 128 : block * 128 + 128] = turned[120:128]


def tables_kernel(three, below, above, plane_weights, z_high, z_low):
    for group, (ref, first, along_x) in enumerate(((three, 0, 0.0), (below, 128, -8.0), (above, 192, 8.0))):
        for part, along_y in enumerate((0.0, -8.0, 8.0)):
            for half in range(2):
                top = first + 16 * part + half
                row = lambda k: ref[top + 2 * k : top + 2 * k + 1, :]
                start = (3 * group + part) * 256 + half * 128
                place = slice(start, start + 128)
                plane_weights[0:16, place] = delta_rows(16, row(0) + (along_x + 2.0), row(3))
                plane_weights[16:32, place] = delta_rows(16, row(1) + (along_y + 2.0), row(4))
                high, rest = halves(delta_rows(144, row(2) + 2.0, row(5)))
                z_high[0:144, place] = high
                z_low[0:144, place] = rest
    z_high[144:256, :] = jnp.zeros((112, COLS), BF16)
    z_low[144:256, :] = jnp.zeros((112, COLS), BF16)


def fill_left(group, refs, planes, plane_weights, left_high, left_low):
    for part, (ref, first) in enumerate(refs):
        for half in range(2):
            column = part * 256 + half * 128
            place = slice(column, column + 128)
            weight = slice(group * 768 + column, group * 768 + column + 128)
            along_y = plane_weights[16:32, weight]
            vector = [ref[first + 2 * c + half : first + 2 * c + half + 1, :] * along_y for c in range(3)]
            for at, plane in enumerate(planes):
                along_x = plane_weights[plane : plane + 1, weight]
                for c in range(3):
                    top, rest = halves(vector[c] * along_x)
                    row = (c * len(planes) + at) * YPAD
                    left_high[row : row + YPAD, place] = top
                    left_low[row : row + YPAD, place] = rest


def spread_group(group, left_high, left_low, z_high, z_low):
    columns = slice(group * 768, group * 768 + 768)
    high = left_high[...]
    total = transposed_dot(high, z_high[:, columns]) + transposed_dot(left_low[...], z_high[:, columns])
    return total + transposed_dot(high, z_low[:, columns])


def own_spread_kernel(own, below, above, plane_weights, z_high, z_low, moved, left_high, left_low):
    refs = [(own, 0), (below, 0), (above, 0)]
    fill_left(0, refs, range(1, 12), plane_weights, left_high, left_low)
    moved[...] = spread_group(0, left_high, left_low, z_high, z_low)


def interpolated(velocity, plane_weights, z_high, z_low):
    rows = []
    for field in velocity:
        high, rest = halves(field)
        partial = plain_dot(high, z_high) + plain_dot(rest, z_high) + plain_dot(high, z_low)
        total = jnp.zeros((YPAD, MARKERS), F32)
        for plane in range(11):
            total = total + partial[plane * YPAD : plane * YPAD + YPAD] * plane_weights[plane + 1 : plane + 2, 0:MARKERS]
        line = jnp.sum(total * plane_weights[16:32, 0:MARKERS], axis=0, keepdims=True)
        rows += [line[:, 0:128], line[:, 128:256]]
    rows.append(jnp.zeros((2, 128), F32))
    return jnp.concatenate(rows, axis=0)


def setup_kernel(main, low, high, plane_weights, z_high, z_low, aux, scale, start, wide):
    lane = lax.broadcasted_iota(jnp.int32, (128, 128), 1)
    row8 = lax.broadcasted_iota(jnp.int32, (8, 128), 0)
    for block in range(7):
        place = slice(block * 128, block * 128 + 128)
        edge = jnp.where(row8 < 2, pltpu.roll(high[:, place], 2, 0), pltpu.roll(low[:, place], 2, 0))
        edge = jnp.concatenate([edge, jnp.zeros((120, 128), F32)], axis=0).T
        body_rows = pltpu.roll(main[place, :], 2, 1)
        wide[place, 0:128] = jnp.where(lane < 2, edge, body_rows)
        wide[place, 128:256] = jnp.where(lane < 2, body_rows, jnp.where(lane < 5, edge, 1.0))
    scale[...] = lax.rsqrt(wide[3 * ROWS : 4 * ROWS, :])
    velocity = [wide[c * ROWS + YPAD : c * ROWS + YPAD + INNER, :] for c in range(3)]
    image = interpolated(velocity, plane_weights, z_high[:, 0:MARKERS], z_low[:, 0:MARKERS])
    start[...] = aux[0:8, :] * (aux[16:24, :] - image)


def spread_kernel(
    moved, below, above, plane_weights, z_high, z_low, scale, velocity, low, high, b_high, b_low, a_high, a_low, field, edges
):
    fill_left(1, [(below, 8 * part) for part in range(3)], range(0, 4), plane_weights, b_high, b_low)
    fill_left(2, [(above, 8 * part) for part in range(3)], range(9, 13), plane_weights, a_high, a_low)
    first = spread_group(1, b_high, b_low, z_high, z_low)
    final = spread_group(2, a_high, a_low, z_high, z_low)
    for c in range(3):
        for plane in range(PLANES):
            parts = []
            if 1 <= plane <= 11:
                row = c * INNER + (plane - 1) * YPAD
                parts.append(moved[row : row + YPAD, :])
            if plane < 4:
                parts.append(first[c * 64 + plane * YPAD : c * 64 + plane * YPAD + YPAD])
            if plane >= 9:
                parts.append(final[c * 64 + (plane - 9) * YPAD : c * 64 + (plane - 9) * YPAD + YPAD])
            total = parts[0] if len(parts) == 1 else parts[0] + parts[1]
            row = c * ROWS + plane * YPAD
            field[row : row + YPAD, :] = total * scale[plane * YPAD : plane * YPAD + YPAD, :]
    axial, diagonal = 1.0 / 6.0, 1.0 / 12.0
    up_y = lambda a: pltpu.roll(a, 1, 0)
    down_y = lambda a: pltpu.roll(a, YPAD - 1, 0)
    up_z = lambda a: pltpu.roll(a, 1, 1)
    down_z = lambda a: pltpu.roll(a, LANES - 1, 1)
    onward = [None] * PLANES
    back = [None] * PLANES
    still = [None] * PLANES
    lane = lax.broadcasted_iota(jnp.int32, (YPAD, 128), 1)
    edges[INNER:256, :] = jnp.zeros((256 - INNER, 128), F32)
    for plane in range(PLANES):
        gx, gy, gz = (field[c * ROWS + plane * YPAD : c * ROWS + plane * YPAD + YPAD, :] for c in range(3))
        hx, hy, hz = gx * diagonal, gy * diagonal, gz * diagonal
        sum_xy, dif_xy = hx + hy, hx - hy
        zx_up, zy_up, zz_up = up_z(hx), up_z(hy), up_z(hz)
        zx_dn, zy_dn, zz_dn = down_z(hx), down_z(hy), down_z(hz)
        xz_sum_up, xz_sum_dn, xz_dif_up, xz_dif_dn = zx_up + zz_up, zx_dn + zz_dn, zx_up - zz_up, zx_dn - zz_dn
        xy_sum_up, xy_sum_dn, xy_dif_up, xy_dif_dn = up_y(sum_xy), down_y(sum_xy), up_y(dif_xy), down_y(dif_xy)
        ax = gx * axial
        onward[plane] = (
            ax + ((xy_sum_up + xy_dif_dn) + (xz_sum_up + xz_dif_dn)),
            xy_sum_up - xy_dif_dn,
            xz_sum_up - xz_dif_dn,
        )
        back[plane] = (
            ax + ((xy_sum_dn + xy_dif_up) + (xz_sum_dn + xz_dif_up)),
            xy_sum_dn - xy_dif_up,
            xz_sum_dn - xz_dif_up,
        )
        yz_same = up_y(zy_up + zz_up)
        yz_same_dn = down_y(zy_dn + zz_dn)
        yz_cross = up_y(zy_dn - zz_dn)
        yz_cross_dn = down_y(zy_up - zz_up)
        same, cross = yz_same + yz_same_dn, yz_cross + yz_cross_dn
        still[plane] = (
            gx,
            gy + ((up_y(hy) + down_y(hy)) * 2.0 + (same + cross)),
            gz + ((zz_up + zz_dn) * 2.0 + (same - cross)),
        )
        if plane >= 2:
            out = plane - 1
            factor = scale[out * YPAD : out * YPAD + YPAD, :] * 0.5
            first = (out - 1) * YPAD
            packed = jnp.zeros((YPAD, 128), F32)
            for c in range(3):
                value = (still[out][c] + (onward[out - 1][c] + back[out + 1][c])) * factor
                velocity[c * INNER + first : c * INNER + first + YPAD, :] = value
                near = value[:, 0:128]
                beyond = value[:, 128:256]
                near = pltpu.roll(near, 4 * c, 1) if c else near
                packed = jnp.where((lane >= 4 * c) & (lane < 4 * c + 4), near, packed)
                at = 16 + 4 * c
                packed = jnp.where((lane >= at) & (lane < at + 4), pltpu.roll(beyond, at - 1, 1), packed)
            edges[first : first + YPAD, :] = packed
    for block in range(2):
        place = slice(block * 128, block * 128 + 128)
        turned = edges[place, :].T
        low[:, place] = turned[0:16]
        high[:, place] = turned[16:32]


def apply_image(velocity, low, high, plane_weights, z_high, z_low, aux, vector):
    lane = lax.broadcasted_iota(jnp.int32, (INNER, 128), 1)
    columns = []
    for block in range(2):
        place = slice(block * 128, block * 128 + 128)
        columns.append(jnp.concatenate([high[:, place], low[:, place], jnp.zeros((96, 128), F32)], axis=0).T)
    edge = jnp.concatenate(columns, axis=0)[0:INNER]
    fields = []
    for c in range(3):
        mine = velocity[c * INNER : c * INNER + INNER, :]
        near = jnp.where((lane >= 1) & (lane < 5), pltpu.roll(edge, (1 - 4 * c) % 128, 1), 0.0)
        beyond = jnp.where(lane < 4, pltpu.roll(edge, (112 - 4 * c) % 128, 1), 0.0)
        fields.append(mine + jnp.concatenate([near, beyond], axis=1))
    image = interpolated(fields, plane_weights, z_high[:, 0:MARKERS], z_low[:, 0:MARKERS])
    return aux[0:8, :] * (image + aux[8:16, :] * vector[...])


def image_kernel(velocity, low, high, plane_weights, z_high, z_low, aux, vector, result):
    result[...] = apply_image(velocity, low, high, plane_weights, z_high, z_low, aux, vector)


def two_sum(a, b):
    total = a + b
    part = total - a
    return total, (a - (total - part)) + (b - part)


def fast_two_sum(a, b):
    total = a + b
    return total, b - (total - a)


def split(a):
    scaled = a * 4097.0
    high = scaled - (scaled - a)
    return high, a - high


def two_product(a, b):
    product = a * b
    a_high, a_low = split(a)
    b_high, b_low = split(b)
    return product, ((a_high * b_high - product) + a_high * b_low + a_low * b_high) + a_low * b_low


def pair_add(a, b):
    head, tail = two_sum(a[0], b[0])
    return fast_two_sum(head, tail + (a[1] + b[1]))


def pair_negative(a):
    return (-a[0], -a[1])


def pair_multiply(a, b):
    head, tail = two_product(a[0], b[0])
    return fast_two_sum(head, tail + (a[0] * b[1] + a[1] * b[0]))


def pair_divide(a, b):
    first = a[0] / b[0]
    rest = pair_add(a, pair_negative(pair_multiply((first, jnp.zeros_like(first)), b)))
    return fast_two_sum(first, rest[0] / b[0])


ENTRIES = ((0, 0), (0, 1), (0, 2), (0, 3), (1, 1), (1, 2), (1, 3), (2, 2), (2, 3))


def last_kernel(velocity, low, high, plane_weights, z_high, z_low, aux, first, second, third, sums):
    fourth = apply_image(velocity, low, high, plane_weights, z_high, z_low, aux, third)
    vectors = [first[...], second[...], third[...], fourth]
    lane = lax.broadcasted_iota(jnp.int32, (8, 128), 1)
    packed = jnp.zeros((8, 128), F32)
    for at, (i, j) in enumerate(ENTRIES):
        value = two_product(vectors[i], vectors[j])
        for axis, steps in ((0, (4, 2, 1)), (1, (64, 32, 16, 8, 4, 2, 1))):
            for step in steps:
                value = pair_add(value, (pltpu.roll(value[0], step, axis), pltpu.roll(value[1], step, axis)))
        packed = jnp.where(lane == at, value[0], jnp.where(lane == 16 + at, value[1], packed))
    for block in range(sums.shape[0] // 8):
        sums[block * 8 : block * 8 + 8, :] = packed


def finish_kernel(gathered, first, second, third, forces):
    a = gathered[...]
    count = a.shape[0]
    value = (a, pltpu.roll(a, 112, 1))
    while count > 8:
        count //= 2
        value = pair_add(
            (value[0][0:count], value[1][0:count]), (value[0][count : 2 * count], value[1][count : 2 * count])
        )
    for step in (4, 2, 1):
        value = pair_add(value, (pltpu.roll(value[0], step, 0), pltpu.roll(value[1], step, 0)))
    lane = lax.broadcasted_iota(jnp.int32, (8, 128), 1)
    gram = {}
    for at, (i, j) in enumerate(ENTRIES):
        entry = tuple(
            jnp.broadcast_to(jnp.sum(jnp.where(lane == at, v, 0.0), axis=1, keepdims=True), (8, 128)) for v in value
        )
        gram[i, j] = entry
        gram[j, i] = entry
    add, times = pair_add, pair_multiply
    minus = lambda a, b: pair_add(a, pair_negative(b))

    def form(left, right, shift):
        total = None
        for i, a in enumerate(left):
            for j, b in enumerate(right):
                term = times(times(a, b), gram[i, j + shift])
                total = term if total is None else add(total, term)
        return total

    one = (jnp.ones((8, 128), F32), jnp.zeros((8, 128), F32))
    alpha0 = pair_divide(gram[0, 0], gram[0, 1])
    residual = [one, pair_negative(alpha0)]
    norm1 = form(residual, residual, 0)
    beta0 = pair_divide(norm1, gram[0, 0])
    along1 = [add(one, beta0), pair_negative(alpha0)]
    alpha1 = pair_divide(norm1, form(along1, along1, 1))
    residual = [one, minus(residual[1], times(alpha1, along1[0])), pair_negative(times(alpha1, along1[1]))]
    norm2 = form(residual, residual, 0)
    beta1 = pair_divide(norm2, norm1)
    along2 = [add(one, times(beta1, along1[0])), add(residual[1], times(beta1, along1[1])), residual[2]]
    alpha2 = pair_divide(norm2, form(along2, along2, 1))
    weight0 = add(alpha0, add(times(alpha1, along1[0]), times(alpha2, along2[0])))
    weight1 = add(times(alpha1, along1[1]), times(alpha2, along2[1]))
    weight2 = times(alpha2, along2[2])
    total = weight0[0] * first[...] + (weight1[0] * second[...] + weight2[0] * third[...])
    for c in range(3):
        forces[c : c + 1, 0:128] = total[2 * c : 2 * c + 1, :]
        forces[c : c + 1, 128:256] = total[2 * c + 1 : 2 * c + 2, :]


def call(kernel, name, outs, *operands, specs=None, scratch=()):
    whole = pl.BlockSpec(memory_space=pltpu.VMEM)
    return pl.pallas_call(
        kernel,
        name=name,
        out_shape=[jax.ShapeDtypeStruct(shape, kind) for shape, kind in outs],
        in_specs=[whole] * len(operands) if specs is None else specs,
        out_specs=[whole] * len(outs),
        scratch_shapes=list(scratch),
        compiler_params=PARAMS,
    )(*operands)


def body(density, base_velocity, cells, offsets, target, stiffness, counts):
    fields, marks, aux, upward, downward = call(
        pack_kernel, "pack",
        [((256, 128), F32), ((16, 128), F32), ((24, 128), F32), ((80, 128), F32), ((112, 128), F32)],
        *(pltpu.with_memory_space_constraint(a, pltpu.HBM) for a in (density, base_velocity, cells, offsets, target, stiffness.reshape(1, MARKERS))), counts,
        specs=[pl.BlockSpec(memory_space=pltpu.HBM)] * 6 + [pl.BlockSpec(memory_space=pltpu.SMEM)],
        scratch=[
            pltpu.VMEM((8, 8, 128), F32), pltpu.VMEM((3, 8, 8, 128), F32), pltpu.VMEM((3, MARKERS), jnp.int32),
            pltpu.VMEM((3, MARKERS), F32), pltpu.VMEM((3, MARKERS), F32), pltpu.VMEM((1, MARKERS), F32),
            pltpu.SemaphoreType.DMA((6,)),
        ],
    )
    below, above = shifted(upward, GY, 1), shifted(downward, GY, -1)
    deep, three, upward, downward = call(
        deepen_kernel, "deepen",
        [((512, 128), F32), ((48, 128), F32), ((176, 128), F32), ((240, 128), F32)],
        fields, marks, below, above,
    )
    below, above = shifted(upward, "gx", 1), shifted(downward, "gx", -1)
    main, low, high = call(
        assemble_kernel, "assemble", [((896, 128), F32), ((8, 896), F32), ((8, 896), F32)], deep, below, above
    )
    from_above, from_below = shifted(low, "gz", -1), shifted(high, "gz", 1)
    plane_weights, z_high, z_low = call(
        tables_kernel, "tables", [((32, COLS), F32), ((256, COLS), BF16), ((256, COLS), BF16)], three, below, above
    )
    tables = (plane_weights, z_high, z_low)
    scale, start = call(
        setup_kernel, "setup", [((ROWS, LANES), F32), ((8, 128), F32)],
        main, from_above, from_below, *tables, aux,
        scratch=[pltpu.VMEM((896, LANES), F32)],
    )

    def spread(vector):
        below, above = shifted(vector, GY, 1), shifted(vector, GY, -1)
        three = jnp.concatenate([vector, below, above], axis=0)
        below_three, above_three = shifted(three, "gx", 1), shifted(three, "gx", -1)
        (moved,) = call(
            own_spread_kernel, "own_spread", [((3 * INNER, LANES), F32)], vector, below, above, *tables,
            scratch=[pltpu.VMEM((3 * INNER, 768), BF16)] * 2,
        )
        velocity, low, high = call(
            spread_kernel, "spread", [((3 * INNER, LANES), F32), ((16, 256), F32), ((16, 256), F32)],
            moved, below_three, above_three, *tables, scale,
            scratch=[pltpu.VMEM((192, 768), BF16)] * 4 + [pltpu.VMEM((3 * ROWS, LANES), F32), pltpu.VMEM((256, 128), F32)],
        )
        return velocity, shifted(low, "gz", -1), shifted(high, "gz", 1)

    vectors = [start]
    for step in range(2):
        (image,) = call(
            image_kernel, "image", [((8, 128), F32)],
            *spread(vectors[-1]), *tables, aux, vectors[-1],
        )
        vectors.append(image)
    (sums,) = call(
        last_kernel, "last", [((256, 128), F32)],
        *spread(vectors[-1]), *tables, aux, *vectors,
    )
    gathered = lax.all_to_all(sums, GX_GY_GZ, 0, 0, tiled=True)
    (forces,) = call(finish_kernel, "finish", [((3, MARKERS), F32)], gathered, *vectors)
    return forces


def solution(mesh):
    finer = Mesh(
        mesh.devices.reshape(mesh.shape["gx"], 4, 2, mesh.shape["gz"]), ("gx", "gy_0", "gy_1", "gz")
    )
    return jax.shard_map(
        body,
        mesh=finer,
        in_specs=(
            P("gx", GY, "gz"),
            P(None, "gx", GY, "gz"),
            P(None, GX_GY_GZ),
            P(None, GX_GY_GZ),
            P(None, GX_GY_GZ),
            P(GX_GY_GZ),
            P(GX_GY_GZ),
        ),
        out_specs=P(None, GX_GY_GZ),
        check_vma=False,
    )
```

```python
import jax
import jax.numpy as jnp
from jax import lax
from jax.experimental import pallas as pl
from jax.experimental.pallas import tpu as pltpu
from jax.sharding import Mesh
from jax.sharding import PartitionSpec as P

GY = ("gy_0", "gy_1")
GX_GY_GZ = ("gx", "gy_0", "gy_1", "gz")

PLANES = 13
YPAD = 16
ROWS = PLANES * YPAD
INNER = 11 * YPAD
LANES = 256
DEEP = 16
REACH = 12
MARKERS = 256
FIRST = 3 * MARKERS
STATIC = FIRST + 3 * 128
COLS = STATIC + 3 * 384
F32 = jnp.float32
BF16 = jnp.bfloat16
PARAMS = pltpu.CompilerParams(vmem_limit_bytes=12 * 1024 * 1024)


def shifted(shard, axis, by):
    length = lax.axis_size(axis)
    return lax.ppermute(shard, axis, [(i, (i + by) % length) for i in range(length)])


def halves(value):
    high = value.astype(BF16)
    return high, (value - high.astype(F32)).astype(BF16)


def transposed_dot(left, right):
    return lax.dot_general(left, right, (((1,), (1,)), ((), ())), preferred_element_type=F32)


def plain_dot(left, right):
    return lax.dot_general(left, right, (((1,), (0,)), ((), ())), preferred_element_type=F32)


def delta_rows(extent, cell, fraction):
    step = lax.broadcasted_iota(jnp.int32, (extent, cell.shape[1]), 0).astype(F32) - cell
    radius = jnp.abs(step - fraction)
    near = (step == 0.0) | (step == 1.0)
    far = (step == -1.0) | (step == 2.0)
    inner = (3.0 - 2.0 * radius + jnp.sqrt(jnp.maximum(1.0 + 4.0 * radius - 4.0 * radius * radius, 0.0))) / 8.0
    outer = (5.0 - 2.0 * radius - jnp.sqrt(jnp.maximum(-7.0 + 12.0 * radius - 4.0 * radius * radius, 0.0))) / 8.0
    return jnp.where(near, inner, jnp.where(far, outer, 0.0))


def pack_kernel(
    density_in, base_in, cells_in, offsets_in, target_in, stiffness_in, counts, fields, own, to_above, to_below,
    density, base, cells, offsets, target, stiffness, arrived,
):
    sources = (density_in, base_in, cells_in, offsets_in, target_in, stiffness_in)
    places = (density, base, cells, offsets, target, stiffness)
    copies = [pltpu.make_async_copy(a, b, arrived.at[i]) for i, (a, b) in enumerate(zip(sources, places))]
    for copy in copies:
        copy.start()
    for copy in copies:
        copy.wait()
    for plane in range(8):
        for field in range(4):
            piece = density[plane] if field == 3 else base[field, plane]
            fields[(field * 8 + plane) * 8 : (field * 8 + plane) * 8 + 8, :] = piece
    for block in range(2):
        turned = fields[block * 128 : block * 128 + 128, :].T
        to_below[block * 16 : block * 16 + 16, :] = turned[0:DEEP]
        to_above[block * 16 : block * 16 + 16, :] = turned[128 - DEEP : 128]
    lane = lax.broadcasted_iota(jnp.int32, (1, MARKERS), 1)
    live = jnp.where(lane < counts[0], 1.0, 0.0).astype(F32)
    inside = [(cells[k : k + 1, :] & (7, 7, 127)[k]).astype(F32) for k in range(3)]
    data = inside + [offsets[k : k + 1, :] for k in range(3)] + [live, stiffness[0:1, :]]
    data += [target[k : k + 1, :] for k in range(3)]
    for k, row in enumerate(data):
        own[2 * k : 2 * k + 1, :] = row[:, 0:128]
        own[2 * k + 1 : 2 * k + 2, :] = row[:, 128:256]
    own[22:24, :] = jnp.zeros((2, 128), F32)
    table = jnp.concatenate(data + [jnp.zeros((5, MARKERS), F32)], axis=0)
    table_high = table.astype(BF16)
    rest = table - table_high.astype(F32)
    table_mid = rest.astype(BF16)
    table_low = (rest - table_mid.astype(F32)).astype(BF16)
    upper = jnp.where(inside[2] >= 128.0 - REACH, live, 0.0)
    lower = jnp.where(inside[2] < 1.0 * REACH, live, 0.0)
    flags = jnp.concatenate([upper, lower, jnp.zeros((14, MARKERS), F32)], axis=0).astype(BF16)
    earlier = lax.broadcasted_iota(jnp.int32, (MARKERS, MARKERS), 0) < lax.broadcasted_iota(
        jnp.int32, (MARKERS, MARKERS), 1
    )
    ranks = plain_dot(flags, jnp.where(earlier, 1.0, 0.0).astype(BF16)).astype(jnp.int32)
    slot = lax.broadcasted_iota(jnp.int32, (512, MARKERS), 0)
    lane = lax.broadcasted_iota(jnp.int32, (1, 128), 1)
    for at, (flag, out, shift) in enumerate(((upper, to_above, -128.0), (lower, to_below, 128.0))):
        rank = ranks[at : at + 1, :]
        goal = ((rank >> 6) << 7) + (rank & 63) + 64 * at
        chosen = jnp.where((slot == goal) & (flag > 0.0), 1.0, 0.0).astype(BF16)
        moved = transposed_dot(table_high, chosen) + transposed_dot(table_mid, chosen)
        moved = moved + transposed_dot(table_low, chosen)
        number = jnp.broadcast_to(jnp.sum(flag, axis=1, keepdims=True), (1, 128))
        number = jnp.where((lane < 64) == (at == 0), number, 0.0)
        for block in range(4):
            columns = slice(block * 128, block * 128 + 128)
            for k in range(11):
                row = moved[k : k + 1, columns]
                if k == 2:
                    row = row + shift * moved[6:7, columns]
                out[32 + 4 * k + block : 33 + 4 * k + block, :] = row
            out[76 + block : 77 + block, :] = number


def deepen_z_kernel(fields, own, below, above, wide, marks, aux, upward, downward):
    lane = lax.broadcasted_iota(jnp.int32, (128, 128), 1)
    packed = jnp.zeros((64, 128), F32)
    lane64 = lax.broadcasted_iota(jnp.int32, (64, 128), 1)
    for block in range(2):
        edge = jnp.concatenate(
            [below[block * 16 : block * 16 + 16, :], above[block * 16 : block * 16 + 16, :], jnp.zeros((96, 128), F32)],
            axis=0,
        ).T
        turned = pltpu.roll(fields[block * 128 : block * 128 + 128, :], DEEP, 1)
        wide[block * 128 : block * 128 + 128, :] = jnp.where(lane < DEEP, edge, turned)
        beyond = jnp.where(lane < DEEP, turned, edge)
        for half in range(2):
            field = 2 * block + half
            piece = beyond[half * 64 : half * 64 + 64]
            piece = pltpu.roll(piece, 32 * field, 1) if field else piece
            packed = jnp.where((lane64 >= 32 * field) & (lane64 < 32 * field + 32), piece, packed)
    wide[256:320, :] = packed
    for at in range(40):
        upward[at * 2 : at * 2 + 2, :] = wide[at * 8 + 6 : at * 8 + 8, :]
        downward[at * 3 : at * 3 + 3, :] = wide[at * 8 : at * 8 + 3, :]
    halo = below[32:80, :] + above[32:80, :]
    marks[0:16, :] = own[0:16, :]
    marks[16:40, :] = halo[0:24]
    marks[40:48, :] = jnp.broadcast_to(halo[44:45], (8, 128))
    upward[80:128, :] = marks[...]
    downward[120:168, :] = marks[...]
    aux[...] = jnp.zeros((72, 128), F32)
    for kind in range(3):
        for c in range(3):
            k = 6 + kind if kind < 2 else 8 + c
            aux[24 * kind + 2 * c : 24 * kind + 2 * c + 2, :] = own[2 * k : 2 * k + 2, :]
            for block in range(4):
                row = 24 * kind + 8 + 3 * block + c
                aux[row : row + 1, :] = halo[4 * k + block : 4 * k + block + 1]


def deepen_y_kernel(wide, marks, below, above, deep, three, upward, downward):
    for at in range(40):
        row = at * YPAD
        deep[row : row + 2, :] = below[at * 2 : at * 2 + 2, :]
        deep[row + 2 : row + 10, :] = wide[at * 8 : at * 8 + 8, :]
        deep[row + 10 : row + 13, :] = above[at * 3 : at * 3 + 3, :]
        deep[row + 13 : row + 16, :] = jnp.ones((3, 128), F32)
    for c in range(3):
        upward[c * 16 : c * 16 + 16, :] = deep[c * 128 + 112 : c * 128 + 128, :]
        downward[c * 32 : c * 32 + 32, :] = deep[c * 128 : c * 128 + 32, :]
    for at in range(2):
        row = (3 + at) * 128
        upward[48 + at * 32 : 80 + at * 32, :] = deep[row + 96 : row + 128, :]
        downward[96 + at * 48 : 144 + at * 48, :] = deep[row : row + 48, :]
    three[0:48, :] = marks[...]
    three[48:96, :] = below[80:128, :]
    three[96:144, :] = above[120:168, :]
    upward[112:256, :] = three[...]
    downward[192:336, :] = three[...]


def blocks_used(refs):
    most = jnp.max(jnp.concatenate([ref[first + 40 + 48 * part : first + 41 + 48 * part, :] for ref, first in refs for part in range(3)], axis=0))
    return (most.astype(jnp.int32) + 63) >> 6


def trips(used):
    return jnp.max(used[0:1, :])


def fill_tables(ref, first, along_x, used, plane_weights, z_high, z_low):
    def fill(read, along_y, place):
        plane_weights[0:16, place] = delta_rows(16, read(0) + (along_x + 2.0), read(3))
        plane_weights[16:32, place] = delta_rows(16, read(1) + (along_y + 2.0), read(4))
        high, rest = halves(delta_rows(160, read(2) + 16.0, read(5)))
        z_high[0:160, place] = high
        z_low[0:160, place] = rest

    for part, along_y in enumerate((0.0, -8.0, 8.0)):
        top = first + 48 * part
        for half in range(2):
            column = part * 256 + half * 128
            fill(lambda k: ref[top + 2 * k + half : top + 2 * k + half + 1, :], along_y, slice(column, column + 128))
        column = FIRST + part * 128
        fill(lambda k: ref[top + 16 + 4 * k : top + 17 + 4 * k, :], along_y, slice(column, column + 128))

    def further(block, carry):
        for part, along_y in enumerate((0.0, -8.0, 8.0)):
            top = first + 48 * part + 16 + block
            column = pl.multiple_of(STATIC + (block - 1) * 384 + part * 128, 128)
            fill(lambda k: ref[pl.ds(top + 4 * k, 1), :], along_y, pl.ds(column, 128))
        return carry

    lax.fori_loop(1, used, further, 0)
    z_high[160:256, :] = jnp.zeros((96, COLS), BF16)
    z_low[160:256, :] = jnp.zeros((96, COLS), BF16)


def own_tables_kernel(three, plane_weights, z_high, z_low, used):
    count = blocks_used([(three, 0)])
    used[...] = jnp.full((8, 128), count, jnp.int32)
    fill_tables(three, 0, 0.0, count, plane_weights, z_high, z_low)


def side_tables_kernel(below, above, b_weights, b_high, b_low, a_weights, a_high, a_low, used):
    count = blocks_used([(below, 112), (above, 192)])
    used[...] = jnp.full((8, 128), count, jnp.int32)
    fill_tables(below, 112, -8.0, count, b_weights, b_high, b_low)
    fill_tables(above, 192, 8.0, count, a_weights, a_high, a_low)


def interpolate(velocity_high, velocity_low, plane_weights, z_high, z_low, used, image):
    def lines(place):
        partial = plain_dot(velocity_high[...], z_high[:, place]) + plain_dot(velocity_low[...], z_high[:, place])
        partial = partial + plain_dot(velocity_high[...], z_low[:, place])
        result = []
        for c in range(3):
            total = partial[c * INNER : c * INNER + YPAD] * plane_weights[1:2, place]
            for plane in range(1, 11):
                row = c * INNER + plane * YPAD
                total = total + partial[row : row + YPAD] * plane_weights[plane + 1 : plane + 2, place]
            result.append(jnp.sum(total * plane_weights[16:32, place], axis=0, keepdims=True))
        return result

    image[...] = jnp.zeros((24, 128), F32)
    for c, line in enumerate(lines(slice(0, MARKERS))):
        image[2 * c : 2 * c + 1, :] = line[:, 0:128]
        image[2 * c + 1 : 2 * c + 2, :] = line[:, 128:256]
    for c, line in enumerate(lines(slice(FIRST, FIRST + 128))):
        image[8 + c : 9 + c, :] = line

    def further(block, carry):
        for c, line in enumerate(lines(pl.ds(pl.multiple_of(STATIC + (block - 1) * 384, 128), 128))):
            image[pl.ds(8 + 3 * block + c, 1), :] = line
        return carry

    lax.fori_loop(1, used, further, 0)


def setup_kernel(deep, below, above, plane_weights, z_high, z_low, aux, used, scale, start, velocity_high, velocity_low, image):
    lane = lax.broadcasted_iota(jnp.int32, (YPAD, 128), 1)
    for plane in range(PLANES):
        at = plane * YPAD

        def piece(field):
            if plane < 2:
                row = field * 16 if field < 3 else 48 + (field - 3) * 32 + plane * 16
                return below[row : row + 16, :]
            if plane < 10:
                row = field * 128 + (plane - 2) * 16
                return deep[row : row + 16, :]
            row = field * 32 if field < 3 else 96 + (field - 3) * 48
            row += (plane - 10) * 16
            return above[row : row + 16, :]

        packed = piece(4)
        scale[at : at + YPAD, 0:128] = lax.rsqrt(piece(3))
        scale[at : at + YPAD, 128:256] = lax.rsqrt(jnp.where(lane < 32, pltpu.roll(packed, 32, 1), 1.0))
        if 1 <= plane <= 11:
            for c in range(3):
                row = c * INNER + at - YPAD
                top, rest = halves(piece(c))
                velocity_high[row : row + YPAD, 0:128] = top
                velocity_low[row : row + YPAD, 0:128] = rest
                beyond = pltpu.roll(packed, 128 - 32 * c, 1) if c else packed
                top, rest = halves(jnp.where(lane < 32, beyond, 0.0))
                velocity_high[row : row + YPAD, 128:256] = top
                velocity_low[row : row + YPAD, 128:256] = rest
    interpolate(velocity_high, velocity_low, plane_weights, z_high, z_low, trips(used), image)
    start[...] = aux[0:24, :] * (aux[48:72, :] - image[...])


def fill_tile(rows, planes, plane_weights, weight, left_high, left_low, place):
    along_y = plane_weights[16:32, weight]
    vector = [row * along_y for row in rows]
    for at, plane in enumerate(planes):
        along_x = plane_weights[plane : plane + 1, weight]
        for c in range(3):
            top, rest = halves(vector[c] * along_x)
            row = (c * len(planes) + at) * YPAD
            left_high[row : row + YPAD, place] = top
            left_low[row : row + YPAD, place] = rest


def spread_columns(left_high, left_low, z_high, z_low, left, right):
    total = transposed_dot(left_high[:, left], z_high[:, right]) + transposed_dot(left_low[:, left], z_high[:, right])
    return total + transposed_dot(left_high[:, left], z_low[:, right])


def spread_group(refs, planes, plane_weights, z_high, z_low, used, left_high, left_low, total):
    for part, (ref, first) in enumerate(refs):
        for half in range(2):
            place = slice(part * 256 + half * 128, part * 256 + half * 128 + 128)
            rows = [ref[first + 2 * c + half : first + 2 * c + half + 1, :] for c in range(3)]
            fill_tile(rows, planes, plane_weights, place, left_high, left_low, place)
        place = slice(FIRST + part * 128, FIRST + part * 128 + 128)
        rows = [ref[first + 8 + c : first + 9 + c, :] for c in range(3)]
        fill_tile(rows, planes, plane_weights, place, left_high, left_low, place)
    whole = slice(0, STATIC)
    total[...] = spread_columns(left_high, left_low, z_high, z_low, whole, whole)

    def further(block, carry):
        for part, (ref, first) in enumerate(refs):
            column = pl.multiple_of(STATIC + (block - 1) * 384 + part * 128, 128)
            rows = [ref[pl.ds(first + 8 + 3 * block + c, 1), :] for c in range(3)]
            place = slice(part * 128, part * 128 + 128)
            fill_tile(rows, planes, plane_weights, pl.ds(column, 128), left_high, left_low, place)
        right = pl.ds(pl.multiple_of(STATIC + (block - 1) * 384, 128), 384)
        total[...] += spread_columns(left_high, left_low, z_high, z_low, slice(0, 384), right)
        return carry

    lax.fori_loop(1, used, further, 0)


def own_spread_kernel(own, below, above, plane_weights, z_high, z_low, used, moved, left_high, left_low):
    refs = [(own, 0), (below, 0), (above, 0)]
    spread_group(refs, range(1, 12), plane_weights, z_high, z_low, trips(used), left_high, left_low, moved)


def apply_image(
    moved, below, above, own_tables, own_used, side_tables, side_used, scale, aux, vector,
    left_high, left_low, first, final, field, velocity_high, velocity_low, image,
):
    refs = [[(ref, 24 * part) for part in range(3)] for ref in (below, above)]
    spread_group(refs[0], range(0, 4), *side_tables[0:3], trips(side_used), left_high.at[0], left_low.at[0], first)
    spread_group(refs[1], range(9, 13), *side_tables[3:6], trips(side_used), left_high.at[1], left_low.at[1], final)
    for c in range(3):
        for plane in range(PLANES):
            parts = []
            if 1 <= plane <= 11:
                row = c * INNER + (plane - 1) * YPAD
                parts.append(moved[row : row + YPAD, :])
            if plane < 4:
                row = c * 64 + plane * YPAD
                parts.append(first[row : row + YPAD, :])
            if plane >= 9:
                row = c * 64 + (plane - 9) * YPAD
                parts.append(final[row : row + YPAD, :])
            total = parts[0] if len(parts) == 1 else parts[0] + parts[1]
            row = c * ROWS + plane * YPAD
            field[row : row + YPAD, :] = total * scale[plane * YPAD : plane * YPAD + YPAD, :]
    axial, diagonal = 1.0 / 6.0, 1.0 / 12.0
    up_y = lambda a: pltpu.roll(a, 1, 0)
    down_y = lambda a: pltpu.roll(a, YPAD - 1, 0)
    up_z = lambda a: pltpu.roll(a, 1, 1)
    down_z = lambda a: pltpu.roll(a, LANES - 1, 1)
    onward = [None] * PLANES
    back = [None] * PLANES
    still = [None] * PLANES
    for plane in range(PLANES):
        gx, gy, gz = (field[c * ROWS + plane * YPAD : c * ROWS + plane * YPAD + YPAD, :] for c in range(3))
        hx, hy, hz = gx * diagonal, gy * diagonal, gz * diagonal
        sum_xy, dif_xy = hx + hy, hx - hy
        zx_up, zy_up, zz_up = up_z(hx), up_z(hy), up_z(hz)
        zx_dn, zy_dn, zz_dn = down_z(hx), down_z(hy), down_z(hz)
        xz_sum_up, xz_sum_dn, xz_dif_up, xz_dif_dn = zx_up + zz_up, zx_dn + zz_dn, zx_up - zz_up, zx_dn - zz_dn
        xy_sum_up, xy_sum_dn, xy_dif_up, xy_dif_dn = up_y(sum_xy), down_y(sum_xy), up_y(dif_xy), down_y(dif_xy)
        ax = gx * axial
        onward[plane] = (
            ax + ((xy_sum_up + xy_dif_dn) + (xz_sum_up + xz_dif_dn)),
            xy_sum_up - xy_dif_dn,
            xz_sum_up - xz_dif_dn,
        )
        back[plane] = (
            ax + ((xy_sum_dn + xy_dif_up) + (xz_sum_dn + xz_dif_up)),
            xy_sum_dn - xy_dif_up,
            xz_sum_dn - xz_dif_up,
        )
        yz_same = up_y(zy_up + zz_up)
        yz_same_dn = down_y(zy_dn + zz_dn)
        yz_cross = up_y(zy_dn - zz_dn)
        yz_cross_dn = down_y(zy_up - zz_up)
        same, cross = yz_same + yz_same_dn, yz_cross + yz_cross_dn
        still[plane] = (
            gx,
            gy + ((up_y(hy) + down_y(hy)) * 2.0 + (same + cross)),
            gz + ((zz_up + zz_dn) * 2.0 + (same - cross)),
        )
        if plane >= 2:
            out = plane - 1
            factor = scale[out * YPAD : out * YPAD + YPAD, :] * 0.5
            first = (out - 1) * YPAD
            for c in range(3):
                value = (still[out][c] + (onward[out - 1][c] + back[out + 1][c])) * factor
                top, rest = halves(value)
                row = c * INNER + first
                velocity_high[row : row + YPAD, :] = top
                velocity_low[row : row + YPAD, :] = rest
    interpolate(velocity_high, velocity_low, *own_tables, trips(own_used), image)
    return aux[0:24, :] * (image[...] + aux[24:48, :] * vector[...])


def image_kernel(
    moved, below, above, w, h, l, own_used, bw, bh, bl, aw, ah, al, side_used, scale, aux, vector, result, *scratch
):
    result[...] = apply_image(
        moved, below, above, (w, h, l), own_used, (bw, bh, bl, aw, ah, al), side_used, scale, aux, vector, *scratch
    )


def two_sum(a, b):
    total = a + b
    part = total - a
    return total, (a - (total - part)) + (b - part)


def fast_two_sum(a, b):
    total = a + b
    return total, b - (total - a)


def split(a):
    scaled = a * 4097.0
    high = scaled - (scaled - a)
    return high, a - high


def two_product(a, b):
    product = a * b
    a_high, a_low = split(a)
    b_high, b_low = split(b)
    return product, ((a_high * b_high - product) + a_high * b_low + a_low * b_high) + a_low * b_low


def pair_add(a, b):
    head, tail = two_sum(a[0], b[0])
    return fast_two_sum(head, tail + (a[1] + b[1]))


def pair_negative(a):
    return (-a[0], -a[1])


def pair_multiply(a, b):
    head, tail = two_product(a[0], b[0])
    return fast_two_sum(head, tail + (a[0] * b[1] + a[1] * b[0]))


def pair_divide(a, b):
    first = a[0] / b[0]
    rest = pair_add(a, pair_negative(pair_multiply((first, jnp.zeros_like(first)), b)))
    return fast_two_sum(first, rest[0] / b[0])


ENTRIES = ((0, 0), (0, 1), (0, 2), (0, 3), (1, 1), (1, 2), (1, 3), (2, 2), (2, 3))


def last_kernel(
    moved, below, above, w, h, l, own_used, bw, bh, bl, aw, ah, al, side_used, scale, aux, third, first, second, sums,
    *scratch
):
    fourth = apply_image(
        moved, below, above, (w, h, l), own_used, (bw, bh, bl, aw, ah, al), side_used, scale, aux, third, *scratch
    )
    vectors = [first[0:8, :], second[0:8, :], third[0:8, :], fourth[0:8]]
    lane = lax.broadcasted_iota(jnp.int32, (8, 128), 1)
    packed = jnp.zeros((8, 128), F32)
    for at, (i, j) in enumerate(ENTRIES):
        value = two_product(vectors[i], vectors[j])
        for axis, steps in ((0, (4, 2, 1)), (1, (64, 32, 16, 8, 4, 2, 1))):
            for step in steps:
                value = pair_add(value, (pltpu.roll(value[0], step, axis), pltpu.roll(value[1], step, axis)))
        packed = jnp.where(lane == at, value[0], jnp.where(lane == 16 + at, value[1], packed))
    for block in range(sums.shape[0] // 8):
        sums[block * 8 : block * 8 + 8, :] = packed


def finish_kernel(gathered, first, second, third, forces):
    a = gathered[...]
    count = a.shape[0]
    value = (a, pltpu.roll(a, 112, 1))
    while count > 8:
        count //= 2
        value = pair_add(
            (value[0][0:count], value[1][0:count]), (value[0][count : 2 * count], value[1][count : 2 * count])
        )
    for step in (4, 2, 1):
        value = pair_add(value, (pltpu.roll(value[0], step, 0), pltpu.roll(value[1], step, 0)))
    lane = lax.broadcasted_iota(jnp.int32, (8, 128), 1)
    gram = {}
    for at, (i, j) in enumerate(ENTRIES):
        entry = tuple(
            jnp.broadcast_to(jnp.sum(jnp.where(lane == at, v, 0.0), axis=1, keepdims=True), (8, 128)) for v in value
        )
        gram[i, j] = entry
        gram[j, i] = entry
    add, times = pair_add, pair_multiply
    minus = lambda a, b: pair_add(a, pair_negative(b))

    def form(left, right, shift):
        total = None
        for i, a in enumerate(left):
            for j, b in enumerate(right):
                term = times(times(a, b), gram[i, j + shift])
                total = term if total is None else add(total, term)
        return total

    one = (jnp.ones((8, 128), F32), jnp.zeros((8, 128), F32))
    alpha0 = pair_divide(gram[0, 0], gram[0, 1])
    residual = [one, pair_negative(alpha0)]
    norm1 = form(residual, residual, 0)
    beta0 = pair_divide(norm1, gram[0, 0])
    along1 = [add(one, beta0), pair_negative(alpha0)]
    alpha1 = pair_divide(norm1, form(along1, along1, 1))
    residual = [one, minus(residual[1], times(alpha1, along1[0])), pair_negative(times(alpha1, along1[1]))]
    norm2 = form(residual, residual, 0)
    beta1 = pair_divide(norm2, norm1)
    along2 = [add(one, times(beta1, along1[0])), add(residual[1], times(beta1, along1[1])), residual[2]]
    alpha2 = pair_divide(norm2, form(along2, along2, 1))
    weight0 = add(alpha0, add(times(alpha1, along1[0]), times(alpha2, along2[0])))
    weight1 = add(times(alpha1, along1[1]), times(alpha2, along2[1]))
    weight2 = times(alpha2, along2[2])
    total = weight0[0] * first[0:8, :] + (weight1[0] * second[0:8, :] + weight2[0] * third[0:8, :])
    for c in range(3):
        forces[c : c + 1, 0:128] = total[2 * c : 2 * c + 1, :]
        forces[c : c + 1, 128:256] = total[2 * c + 1 : 2 * c + 2, :]


def call(kernel, name, outs, *operands, memory=None, scratch=()):
    spec = lambda space: pl.BlockSpec(memory_space=space)
    memory = memory or [pltpu.VMEM] * len(operands)
    return pl.pallas_call(
        kernel,
        name=name,
        out_shape=[jax.ShapeDtypeStruct(shape, kind) for shape, kind in outs],
        in_specs=[spec(space) for space in memory],
        out_specs=[spec(pltpu.VMEM)] * len(outs),
        scratch_shapes=list(scratch),
        compiler_params=PARAMS,
    )(*operands)


def body(density, base_velocity, cells, offsets, target, stiffness, counts):
    rows = lambda n: ((n, 128), F32)
    vmem, smem, hbm = pltpu.VMEM, pltpu.SMEM, pltpu.HBM
    table_shapes = [((32, COLS), F32), ((256, COLS), BF16), ((256, COLS), BF16)]
    used_shape = [((8, 128), jnp.int32)]
    arguments = (density, base_velocity, cells, offsets, target, stiffness.reshape(1, MARKERS))
    fields, own, to_above, to_below = call(
        pack_kernel, "pack", [rows(256), rows(24), rows(80), rows(80)],
        *(pltpu.with_memory_space_constraint(a, hbm) for a in arguments), counts,
        memory=[hbm] * 6 + [smem],
        scratch=[
            vmem((8, 8, 128), F32), vmem((3, 8, 8, 128), F32), vmem((3, MARKERS), jnp.int32),
            vmem((3, MARKERS), F32), vmem((3, MARKERS), F32), vmem((1, MARKERS), F32),
            pltpu.SemaphoreType.DMA((6,)),
        ],
    )
    below, above = shifted(to_above, "gz", 1), shifted(to_below, "gz", -1)
    wide, marks, aux, upward, downward = call(
        deepen_z_kernel, "deepen_z", [rows(320), rows(48), rows(72), rows(128), rows(168)], fields, own, below, above
    )
    below, above = shifted(upward, GY, 1), shifted(downward, GY, -1)
    deep, three, upward, downward = call(
        deepen_y_kernel, "deepen_y", [rows(640), rows(144), rows(256), rows(336)], wide, marks, below, above
    )
    below, above = shifted(upward, "gx", 1), shifted(downward, "gx", -1)
    own_tables = call(
        own_tables_kernel, "own_tables", table_shapes + used_shape, three
    )
    side_tables = call(
        side_tables_kernel, "side_tables", table_shapes * 2 + used_shape, below, above
    )
    velocity_scratch = [vmem((3 * INNER, LANES), BF16)] * 2 + [vmem((24, 128), F32)]
    scale, start = call(
        setup_kernel, "setup", [((ROWS, LANES), F32), rows(24)], deep, below, above, *own_tables[0:3], aux, own_tables[3],
        scratch=velocity_scratch,
    )

    def image_of(kernel, name, outs, vector, *others):
        below, above = shifted(vector, GY, 1), shifted(vector, GY, -1)
        three = jnp.concatenate([vector, below, above], axis=0)
        below_three, above_three = shifted(three, "gx", 1), shifted(three, "gx", -1)
        (moved,) = call(
            own_spread_kernel, "own_spread", [((3 * INNER, LANES), F32)], vector, below, above, *own_tables,
            scratch=[vmem((3 * INNER, STATIC), BF16)] * 2,
        )
        (result,) = call(
            kernel, name, outs, moved, below_three, above_three, *own_tables, *side_tables, scale, aux, vector, *others,
            scratch=[vmem((2, 192, STATIC), BF16)] * 2 + [vmem((192, LANES), F32)] * 2
            + [vmem((3 * ROWS, LANES), F32)] + velocity_scratch,
        )
        return result

    second = image_of(image_kernel, "image", [rows(24)], start)
    third = image_of(image_kernel, "image", [rows(24)], second)
    sums = image_of(last_kernel, "last", [rows(256)], third, start, second)
    gathered = lax.all_to_all(sums, GX_GY_GZ, 0, 0, tiled=True)
    (forces,) = call(finish_kernel, "finish", [((3, MARKERS), F32)], gathered, start, second, third)
    return forces


def solution(mesh):
    finer = Mesh(
        mesh.devices.reshape(mesh.shape["gx"], 4, 2, mesh.shape["gz"]), ("gx", "gy_0", "gy_1", "gz")
    )
    return jax.shard_map(
        body,
        mesh=finer,
        in_specs=(
            P("gx", GY, "gz"),
            P(None, "gx", GY, "gz"),
            P(None, GX_GY_GZ),
            P(None, GX_GY_GZ),
            P(None, GX_GY_GZ),
            P(GX_GY_GZ),
            P(GX_GY_GZ),
        ),
        out_specs=P(None, GX_GY_GZ),
        check_vma=False,
    )
```

```python
import jax
import jax.numpy as jnp
from jax import lax
from jax.experimental import pallas as pl
from jax.experimental.pallas import tpu as pltpu
from jax.sharding import Mesh
from jax.sharding import PartitionSpec as P

GY = ("gy_0", "gy_1")
GX_GY_GZ = ("gx", "gy_0", "gy_1", "gz")

PLANES = 13
YPAD = 16
ROWS = PLANES * YPAD
INNER = 11 * YPAD
LANES = 256
DEEP = 16
REACH = 12
MARKERS = 256
FIRST = 3 * MARKERS
STATIC = FIRST + 3 * 128
COLS = STATIC + 3 * 384
F32 = jnp.float32
BF16 = jnp.bfloat16
PARAMS = pltpu.CompilerParams(vmem_limit_bytes=12 * 1024 * 1024)


def shifted(shard, axis, by):
    length = lax.axis_size(axis)
    return lax.ppermute(shard, axis, [(i, (i + by) % length) for i in range(length)])


def halves(value):
    high = value.astype(BF16)
    return high, (value - high.astype(F32)).astype(BF16)


def transposed_dot(left, right):
    return lax.dot_general(left, right, (((1,), (1,)), ((), ())), preferred_element_type=F32)


def plain_dot(left, right):
    return lax.dot_general(left, right, (((1,), (0,)), ((), ())), preferred_element_type=F32)


def delta_weights(fraction):
    def inner(radius):
        return (3.0 - 2.0 * radius + jnp.sqrt(jnp.maximum(1.0 + 4.0 * radius - 4.0 * radius * radius, 0.0))) / 8.0

    def outer(radius):
        return (5.0 - 2.0 * radius - jnp.sqrt(jnp.maximum(-7.0 + 12.0 * radius - 4.0 * radius * radius, 0.0))) / 8.0

    return [outer(1.0 + fraction), inner(fraction), inner(1.0 - fraction), outer(2.0 - fraction)]


def delta_rows(extent, cell, weights, at):
    step = lax.broadcasted_iota(jnp.int32, (extent, cell.shape[1]), 0).astype(F32) - cell
    value = jnp.zeros_like(step)
    for place, weight in zip((-1.0, 0.0, 1.0, 2.0), weights):
        value = jnp.where(step == place, weight[at : at + 1], value)
    return value


def pack_kernel(
    density_in, base_in, cells_in, offsets_in, target_in, stiffness_in, counts, fields, own, to_above, to_below,
    density, base, cells, offsets, target, stiffness, arrived,
):
    sources = (density_in, base_in, cells_in, offsets_in, target_in, stiffness_in)
    places = (density, base, cells, offsets, target, stiffness)
    copies = [pltpu.make_async_copy(a, b, arrived.at[i]) for i, (a, b) in enumerate(zip(sources, places))]
    for copy in copies:
        copy.start()
    for copy in copies:
        copy.wait()
    for plane in range(8):
        for field in range(4):
            piece = density[plane] if field == 3 else base[field, plane]
            fields[(field * 8 + plane) * 8 : (field * 8 + plane) * 8 + 8, :] = piece
    for block in range(2):
        turned = fields[block * 128 : block * 128 + 128, :].T
        to_below[block * 16 : block * 16 + 16, :] = turned[0:DEEP]
        to_above[block * 16 : block * 16 + 16, :] = turned[128 - DEEP : 128]
    lane = lax.broadcasted_iota(jnp.int32, (1, MARKERS), 1)
    live = jnp.where(lane < counts[0], 1.0, 0.0).astype(F32)
    inside = [(cells[k : k + 1, :] & (7, 7, 127)[k]).astype(F32) for k in range(3)]
    data = inside + [offsets[k : k + 1, :] for k in range(3)] + [live, stiffness[0:1, :]]
    data += [target[k : k + 1, :] for k in range(3)]
    for k, row in enumerate(data):
        own[2 * k : 2 * k + 1, :] = row[:, 0:128]
        own[2 * k + 1 : 2 * k + 2, :] = row[:, 128:256]
    own[22:24, :] = jnp.zeros((2, 128), F32)
    table = jnp.concatenate(data + [jnp.zeros((5, MARKERS), F32)], axis=0)
    table_high = table.astype(BF16)
    rest = table - table_high.astype(F32)
    table_mid = rest.astype(BF16)
    table_low = (rest - table_mid.astype(F32)).astype(BF16)
    upper = jnp.where(inside[2] >= 128.0 - REACH, live, 0.0)
    lower = jnp.where(inside[2] < 1.0 * REACH, live, 0.0)
    flags = jnp.concatenate([upper, lower, jnp.zeros((14, MARKERS), F32)], axis=0).astype(BF16)
    earlier = lax.broadcasted_iota(jnp.int32, (MARKERS, MARKERS), 0) < lax.broadcasted_iota(
        jnp.int32, (MARKERS, MARKERS), 1
    )
    ranks = plain_dot(flags, jnp.where(earlier, 1.0, 0.0).astype(BF16)).astype(jnp.int32)
    slot = lax.broadcasted_iota(jnp.int32, (512, MARKERS), 0)
    lane = lax.broadcasted_iota(jnp.int32, (1, 128), 1)
    for at, (flag, out, shift) in enumerate(((upper, to_above, -128.0), (lower, to_below, 128.0))):
        rank = ranks[at : at + 1, :]
        goal = ((rank >> 6) << 7) + (rank & 63) + 64 * at
        chosen = jnp.where((slot == goal) & (flag > 0.0), 1.0, 0.0).astype(BF16)
        moved = transposed_dot(table_high, chosen) + transposed_dot(table_mid, chosen)
        moved = moved + transposed_dot(table_low, chosen)
        number = jnp.broadcast_to(jnp.sum(flag, axis=1, keepdims=True), (1, 128))
        number = jnp.where((lane < 64) == (at == 0), number, 0.0)
        for block in range(4):
            columns = slice(block * 128, block * 128 + 128)
            for k in range(11):
                row = moved[k : k + 1, columns]
                if k == 2:
                    row = row + shift * moved[6:7, columns]
                out[32 + 4 * k + block : 33 + 4 * k + block, :] = row
            out[76 + block : 77 + block, :] = number


def deepen_z_kernel(fields, own, below, above, wide, marks, aux, upward, downward):
    lane = lax.broadcasted_iota(jnp.int32, (128, 128), 1)
    packed = jnp.zeros((64, 128), F32)
    lane64 = lax.broadcasted_iota(jnp.int32, (64, 128), 1)
    for block in range(2):
        edge = jnp.concatenate(
            [below[block * 16 : block * 16 + 16, :], above[block * 16 : block * 16 + 16, :], jnp.zeros((96, 128), F32)],
            axis=0,
        ).T
        turned = pltpu.roll(fields[block * 128 : block * 128 + 128, :], DEEP, 1)
        wide[block * 128 : block * 128 + 128, :] = jnp.where(lane < DEEP, edge, turned)
        beyond = jnp.where(lane < DEEP, turned, edge)
        for half in range(2):
            field = 2 * block + half
            piece = beyond[half * 64 : half * 64 + 64]
            piece = pltpu.roll(piece, 32 * field, 1) if field else piece
            packed = jnp.where((lane64 >= 32 * field) & (lane64 < 32 * field + 32), piece, packed)
    wide[256:320, :] = packed
    for at in range(24):
        upward[at : at + 1, :] = wide[at * 8 + 7 : at * 8 + 8, :]
        downward[at * 2 : at * 2 + 2, :] = wide[at * 8 : at * 8 + 2, :]
    for at in range(16):
        row = 192 + at * 8
        upward[24 + at * 2 : 26 + at * 2, :] = wide[row + 6 : row + 8, :]
        downward[48 + at * 3 : 51 + at * 3, :] = wide[row : row + 3, :]
    halo = below[32:80, :] + above[32:80, :]
    marks[0:12, :] = own[0:12, :]
    marks[12:36, :] = halo[0:24]
    marks[36:40, :] = jnp.broadcast_to(halo[44:45], (4, 128))
    upward[56:96, :] = marks[...]
    downward[96:136, :] = marks[...]
    aux[...] = jnp.zeros((72, 128), F32)
    for kind in range(3):
        for c in range(3):
            k = 6 + kind if kind < 2 else 8 + c
            aux[24 * kind + 2 * c : 24 * kind + 2 * c + 2, :] = own[2 * k : 2 * k + 2, :]
            for block in range(4):
                row = 24 * kind + 8 + 3 * block + c
                aux[row : row + 1, :] = halo[4 * k + block : 4 * k + block + 1]


def deepen_y_kernel(wide, marks, below, above, deep, three, upward, downward):
    for at in range(40):
        row = at * YPAD
        deep[row + 2 : row + 10, :] = wide[at * 8 : at * 8 + 8, :]
        if at < 24:
            deep[row : row + 1, :] = jnp.ones((1, 128), F32)
            deep[row + 1 : row + 2, :] = below[at : at + 1, :]
            deep[row + 10 : row + 12, :] = above[at * 2 : at * 2 + 2, :]
            deep[row + 12 : row + 16, :] = jnp.ones((4, 128), F32)
        else:
            near, far = 24 + (at - 24) * 2, 48 + (at - 24) * 3
            deep[row : row + 2, :] = below[near : near + 2, :]
            deep[row + 10 : row + 13, :] = above[far : far + 3, :]
            deep[row + 13 : row + 16, :] = jnp.ones((3, 128), F32)
    for c in range(3):
        upward[c * 13 : c * 13 + 13, :] = deep[c * 128 + 112 : c * 128 + 125, :]
        for k in range(2):
            row = c * 128 + k * YPAD
            downward[c * 26 + k * 13 : c * 26 + k * 13 + 13, :] = deep[row : row + 13, :]
    for at in range(2):
        row = (3 + at) * 128
        for k in range(3):
            if k < 2:
                upward[39 + at * 26 + k * 13 : 52 + at * 26 + k * 13, :] = deep[row + 96 + k * 16 : row + 109 + k * 16, :]
            downward[78 + at * 39 + k * 13 : 91 + at * 39 + k * 13, :] = deep[row + k * 16 : row + k * 16 + 13, :]
    three[0:40, :] = marks[...]
    three[40:80, :] = below[56:96, :]
    three[80:120, :] = above[96:136, :]
    upward[96:216, :] = three[...]
    downward[160:280, :] = three[...]


def blocks_used(refs):
    most = jnp.max(jnp.concatenate([ref[first + 36 + 40 * part : first + 37 + 40 * part, :] for ref, first in refs for part in range(3)], axis=0))
    return (most.astype(jnp.int32) + 63) >> 6


def trips(used):
    return jnp.max(used[0:1, :])


def fill_tables(ref, first, along_x, used, plane_weights, z_high, z_low):
    def fill(read, along_y, place):
        fractions = jnp.concatenate([read(3), read(4), read(5), jnp.zeros((5, 128), F32)], axis=0)
        weights = delta_weights(fractions)
        plane_weights[0:16, place] = delta_rows(16, read(0) + (along_x + 2.0), weights, 0)
        plane_weights[16:32, place] = delta_rows(16, read(1) + (along_y + 2.0), weights, 1)
        high, rest = halves(delta_rows(160, read(2) + 16.0, weights, 2))
        z_high[0:160, place] = high
        z_low[0:160, place] = rest

    for part, along_y in enumerate((0.0, -8.0, 8.0)):
        top = first + 40 * part
        for half in range(2):
            column = part * 256 + half * 128
            fill(lambda k: ref[top + 2 * k + half : top + 2 * k + half + 1, :], along_y, slice(column, column + 128))
        column = FIRST + part * 128
        fill(lambda k: ref[top + 12 + 4 * k : top + 13 + 4 * k, :], along_y, slice(column, column + 128))

    def further(block, carry):
        for part, along_y in enumerate((0.0, -8.0, 8.0)):
            top = first + 40 * part + 12 + block
            column = pl.multiple_of(STATIC + (block - 1) * 384 + part * 128, 128)
            fill(lambda k: ref[pl.ds(top + 4 * k, 1), :], along_y, pl.ds(column, 128))
        return carry

    lax.fori_loop(1, used, further, 0)
    z_high[160:256, :] = jnp.zeros((96, COLS), BF16)
    z_low[160:256, :] = jnp.zeros((96, COLS), BF16)


def own_tables_kernel(three, plane_weights, z_high, z_low, used):
    count = blocks_used([(three, 0)])
    used[...] = jnp.full((8, 128), count, jnp.int32)
    fill_tables(three, 0, 0.0, count, plane_weights, z_high, z_low)


def side_tables_kernel(below, above, b_weights, b_high, b_low, a_weights, a_high, a_low, used):
    count = blocks_used([(below, 96), (above, 160)])
    used[...] = jnp.full((8, 128), count, jnp.int32)
    fill_tables(below, 96, -8.0, count, b_weights, b_high, b_low)
    fill_tables(above, 160, 8.0, count, a_weights, a_high, a_low)


def interpolate(velocity_high, velocity_low, planes, plane_weights, z_high, z_low, used, image):
    def lines(place):
        partial = plain_dot(velocity_high[...], z_high[:, place]) + plain_dot(velocity_low[...], z_high[:, place])
        partial = partial + plain_dot(velocity_high[...], z_low[:, place])
        result = []
        for c in range(3):
            total = None
            for at, plane in enumerate(planes):
                row = (c * len(planes) + at) * YPAD
                term = partial[row : row + YPAD] * plane_weights[plane : plane + 1, place]
                total = term if total is None else total + term
            result.append(jnp.sum(total * plane_weights[16:32, place], axis=0, keepdims=True))
        return result

    image[...] = jnp.zeros((24, 128), F32)
    for c, line in enumerate(lines(slice(0, MARKERS))):
        image[2 * c : 2 * c + 1, :] = line[:, 0:128]
        image[2 * c + 1 : 2 * c + 2, :] = line[:, 128:256]
    for c, line in enumerate(lines(slice(FIRST, FIRST + 128))):
        image[8 + c : 9 + c, :] = line

    def further(block, carry):
        for c, line in enumerate(lines(pl.ds(pl.multiple_of(STATIC + (block - 1) * 384, 128), 128))):
            image[pl.ds(8 + 3 * block + c, 1), :] = line
        return carry

    lax.fori_loop(1, used, further, 0)


def setup_kernel(deep, below, above, plane_weights, z_high, z_low, aux, used, scale, start, velocity_high, velocity_low, image):
    lane = lax.broadcasted_iota(jnp.int32, (YPAD, 128), 1)
    used_rows = lax.broadcasted_iota(jnp.int32, (YPAD, 128), 0) < 13
    for plane in range(PLANES):
        at = plane * YPAD

        def piece(field):
            if plane < 2:
                row = field * 13 if field < 3 else 39 + (field - 3) * 26 + plane * 13
                return jnp.where(used_rows, below[row : row + 16, :], 1.0)
            if plane < 10:
                row = field * 128 + (plane - 2) * 16
                return deep[row : row + 16, :]
            row = field * 26 if field < 3 else 78 + (field - 3) * 39
            row += (plane - 10) * 13
            return jnp.where(used_rows, above[row : row + 16, :], 1.0)

        packed = piece(4)
        scale[at : at + YPAD, 0:128] = lax.rsqrt(piece(3))
        scale[at : at + YPAD, 128:256] = lax.rsqrt(jnp.where(lane < 32, pltpu.roll(packed, 32, 1), 1.0))
        if 1 <= plane <= 11:
            for c in range(3):
                row = c * INNER + at - YPAD
                top, rest = halves(piece(c))
                velocity_high[row : row + YPAD, 0:128] = top
                velocity_low[row : row + YPAD, 0:128] = rest
                beyond = pltpu.roll(packed, 128 - 32 * c, 1) if c else packed
                top, rest = halves(jnp.where(lane < 32, beyond, 0.0))
                velocity_high[row : row + YPAD, 128:256] = top
                velocity_low[row : row + YPAD, 128:256] = rest
    interpolate(velocity_high, velocity_low, range(1, 12), plane_weights, z_high, z_low, trips(used), image)
    start[...] = aux[0:24, :] * (aux[48:72, :] - image[...])


def fill_tile(rows, planes, plane_weights, weight, left_high, left_low, place):
    along_y = plane_weights[16:32, weight]
    vector = [row * along_y for row in rows]
    for at, plane in enumerate(planes):
        along_x = plane_weights[plane : plane + 1, weight]
        for c in range(3):
            top, rest = halves(vector[c] * along_x)
            row = (c * len(planes) + at) * YPAD
            left_high[row : row + YPAD, place] = top
            left_low[row : row + YPAD, place] = rest


def spread_columns(left_high, left_low, z_high, z_low, left, right):
    total = transposed_dot(left_high[:, left], z_high[:, right]) + transposed_dot(left_low[:, left], z_high[:, right])
    return total + transposed_dot(left_high[:, left], z_low[:, right])


def spread_group(refs, planes, plane_weights, z_high, z_low, used, left_high, left_low, total, begun=None, part0=0):
    count = len(refs)
    for at, (ref, first) in enumerate(refs):
        part = part0 + at
        for half in range(2):
            place = slice(at * 256 + half * 128, at * 256 + half * 128 + 128)
            weight = slice(part * 256 + half * 128, part * 256 + half * 128 + 128)
            rows = [ref[first + 2 * c + half : first + 2 * c + half + 1, :] for c in range(3)]
            fill_tile(rows, planes, plane_weights, weight, left_high, left_low, place)
        place = slice(count * 256 + at * 128, count * 256 + at * 128 + 128)
        weight = slice(FIRST + part * 128, FIRST + part * 128 + 128)
        rows = [ref[first + 8 + c : first + 9 + c, :] for c in range(3)]
        fill_tile(rows, planes, plane_weights, weight, left_high, left_low, place)
    value = spread_columns(
        left_high, left_low, z_high, z_low, slice(0, count * 256), slice(part0 * 256, (part0 + count) * 256)
    )
    value = value + spread_columns(
        left_high, left_low, z_high, z_low, slice(count * 256, count * 384),
        slice(FIRST + part0 * 128, FIRST + (part0 + count) * 128),
    )
    total[...] = value if begun is None else value + begun[...]

    def further(block, carry):
        for at, (ref, first) in enumerate(refs):
            column = pl.multiple_of(STATIC + (block - 1) * 384 + (part0 + at) * 128, 128)
            rows = [ref[pl.ds(first + 8 + 3 * block + c, 1), :] for c in range(3)]
            place = slice(at * 128, at * 128 + 128)
            fill_tile(rows, planes, plane_weights, pl.ds(column, 128), left_high, left_low, place)
        right = pl.ds(pl.multiple_of(STATIC + (block - 1) * 384 + part0 * 128, 128), count * 128)
        total[...] += spread_columns(left_high, left_low, z_high, z_low, slice(0, count * 128), right)
        return carry

    lax.fori_loop(1, used, further, 0)


def respond(moved, planes, outs, scale, velocity_high, velocity_low):
    axial, diagonal = 1.0 / 6.0, 1.0 / 12.0
    up_y = lambda a: pltpu.roll(a, 1, 0)
    down_y = lambda a: pltpu.roll(a, YPAD - 1, 0)
    up_z = lambda a: pltpu.roll(a, 1, 1)
    down_z = lambda a: pltpu.roll(a, LANES - 1, 1)
    onward, back, still = {}, {}, {}
    for at, plane in enumerate(planes):
        factor = scale[plane * YPAD : plane * YPAD + YPAD, :]
        rows = [(c * len(planes) + at) * YPAD for c in range(3)]
        gx, gy, gz = (moved[row : row + YPAD, :] * factor for row in rows)
        hx, hy, hz = gx * diagonal, gy * diagonal, gz * diagonal
        sum_xy, dif_xy = hx + hy, hx - hy
        zx_up, zy_up, zz_up = up_z(hx), up_z(hy), up_z(hz)
        zx_dn, zy_dn, zz_dn = down_z(hx), down_z(hy), down_z(hz)
        xz_sum_up, xz_sum_dn, xz_dif_up, xz_dif_dn = zx_up + zz_up, zx_dn + zz_dn, zx_up - zz_up, zx_dn - zz_dn
        xy_sum_up, xy_sum_dn, xy_dif_up, xy_dif_dn = up_y(sum_xy), down_y(sum_xy), up_y(dif_xy), down_y(dif_xy)
        ax = gx * axial
        onward[plane] = (
            ax + ((xy_sum_up + xy_dif_dn) + (xz_sum_up + xz_dif_dn)),
            xy_sum_up - xy_dif_dn,
            xz_sum_up - xz_dif_dn,
        )
        back[plane] = (
            ax + ((xy_sum_dn + xy_dif_up) + (xz_sum_dn + xz_dif_up)),
            xy_sum_dn - xy_dif_up,
            xz_sum_dn - xz_dif_up,
        )
        yz_same = up_y(zy_up + zz_up)
        yz_same_dn = down_y(zy_dn + zz_dn)
        yz_cross = up_y(zy_dn - zz_dn)
        yz_cross_dn = down_y(zy_up - zz_up)
        same, cross = yz_same + yz_same_dn, yz_cross + yz_cross_dn
        still[plane] = (
            gx,
            gy + ((up_y(hy) + down_y(hy)) * 2.0 + (same + cross)),
            gz + ((zz_up + zz_dn) * 2.0 + (same - cross)),
        )
        for place, out in enumerate(outs):
            if min(out + 1, planes[-1]) != plane:
                continue
            factor = scale[out * YPAD : out * YPAD + YPAD, :] * 0.5
            for c in range(3):
                parts = [group[at][c] for group, at in ((onward, out - 1), (still, out), (back, out + 1)) if at in group]
                total = parts[0]
                for part in parts[1:]:
                    total = total + part
                top, rest = halves(total * factor)
                row = (c * len(outs) + place) * YPAD
                velocity_high[row : row + YPAD, :] = top
                velocity_low[row : row + YPAD, :] = rest


def own_spread(own, plane_weights, z_high, z_low, used, total, left_high, left_low):
    spread_group([(own, 0)], range(1, 12), plane_weights, z_high, z_low, trips(used), left_high, left_low, total)


def own_image(
    begun, below, above, plane_weights, z_high, z_low, used, scale, result, left_high, left_low, moved, velocity_high,
    velocity_low,
):
    refs = [(below, 0), (above, 0)]
    planes = range(1, 12)
    count = trips(used)
    spread_group(refs, planes, plane_weights, z_high, z_low, count, left_high, left_low, moved, begun, 1)
    respond(moved, planes, planes, scale, velocity_high, velocity_low)
    interpolate(velocity_high, velocity_low, planes, plane_weights, z_high, z_low, count, result)


def side_image(
    below, begun, three, own_tables, own_used, side_tables, used, scale, left_high, left_low, moved, velocity_high,
    velocity_low, image,
):
    planes, outs = (range(0, 4), range(1, 5)) if below else (range(9, 13), range(8, 12))
    refs = [(three, 24 * part) for part in range(3)]
    spread_group(refs, planes, *side_tables, trips(used), left_high, left_low, moved)
    respond(moved, planes, outs, scale, velocity_high, velocity_low)
    interpolate(velocity_high, velocity_low, outs, *own_tables, trips(own_used), image)
    return begun[...] + image[...]


def below_kernel(begun, three, w, h, l, own_used, sw, sh, sl, used, scale, result, *scratch):
    result[...] = side_image(True, begun, three, (w, h, l), own_used, (sw, sh, sl), used, scale, *scratch)


def above_image(begun, three, w, h, l, own_used, sw, sh, sl, used, scale, aux, vector, *scratch):
    image = side_image(False, begun, three, (w, h, l), own_used, (sw, sh, sl), used, scale, *scratch)
    return aux[0:24, :] * (image + aux[24:48, :] * vector[...])


def above_kernel(begun, three, w, h, l, own_used, sw, sh, sl, used, scale, aux, vector, result, *scratch):
    result[...] = above_image(begun, three, w, h, l, own_used, sw, sh, sl, used, scale, aux, vector, *scratch)


def two_sum(a, b):
    total = a + b
    part = total - a
    return total, (a - (total - part)) + (b - part)


def fast_two_sum(a, b):
    total = a + b
    return total, b - (total - a)


def split(a):
    scaled = a * 4097.0
    high = scaled - (scaled - a)
    return high, a - high


def two_product(a, b):
    product = a * b
    a_high, a_low = split(a)
    b_high, b_low = split(b)
    return product, ((a_high * b_high - product) + a_high * b_low + a_low * b_high) + a_low * b_low


def pair_add(a, b):
    head, tail = two_sum(a[0], b[0])
    return fast_two_sum(head, tail + (a[1] + b[1]))


def pair_negative(a):
    return (-a[0], -a[1])


def pair_multiply(a, b):
    head, tail = two_product(a[0], b[0])
    return fast_two_sum(head, tail + (a[0] * b[1] + a[1] * b[0]))


def pair_divide(a, b):
    first = a[0] / b[0]
    rest = pair_add(a, pair_negative(pair_multiply((first, jnp.zeros_like(first)), b)))
    return fast_two_sum(first, rest[0] / b[0])


ENTRIES = ((0, 0), (0, 1), (0, 2), (0, 3), (1, 1), (1, 2), (1, 3), (2, 2), (2, 3))


def gram_lanes(vectors, entries, packed):
    lane = lax.broadcasted_iota(jnp.int32, (8, 128), 1)
    for at, (i, j) in enumerate(ENTRIES):
        if (i, j) not in entries:
            continue
        value = two_product(vectors[i], vectors[j])
        for axis, steps in ((0, (4, 2, 1)), (1, (64, 32, 16, 8, 4, 2, 1))):
            for step in steps:
                value = pair_add(value, (pltpu.roll(value[0], step, axis), pltpu.roll(value[1], step, axis)))
        packed = jnp.where(lane == at, value[0], jnp.where(lane == 16 + at, value[1], packed))
    return packed


EARLY = tuple(entry for entry in ENTRIES if entry[1] < 3)
LATE = tuple(entry for entry in ENTRIES if entry[1] == 3)


def own_spread_last(own, w, h, l, used, first, second, total, early, *scratch):
    own_spread(own, w, h, l, used, total, *scratch)
    early[...] = gram_lanes([first[0:8, :], second[0:8, :], own[0:8, :]], EARLY, jnp.zeros((8, 128), F32))


def last_kernel(
    begun, three, w, h, l, own_used, sw, sh, sl, used, scale, aux, third, first, second, early, sums, *scratch
):
    fourth = above_image(begun, three, w, h, l, own_used, sw, sh, sl, used, scale, aux, third, *scratch)
    vectors = [first[0:8, :], second[0:8, :], third[0:8, :], fourth[0:8]]
    packed = gram_lanes(vectors, LATE, early[...])
    for block in range(sums.shape[0] // 8):
        sums[block * 8 : block * 8 + 8, :] = packed


def finish_kernel(gathered, first, second, third, forces):
    a = gathered[...]
    count = a.shape[0]
    value = (a, pltpu.roll(a, 112, 1))
    while count > 8:
        count //= 2
        value = pair_add(
            (value[0][0:count], value[1][0:count]), (value[0][count : 2 * count], value[1][count : 2 * count])
        )
    for step in (4, 2, 1):
        value = pair_add(value, (pltpu.roll(value[0], step, 0), pltpu.roll(value[1], step, 0)))
    lane = lax.broadcasted_iota(jnp.int32, (8, 128), 1)
    gram = {}
    for at, (i, j) in enumerate(ENTRIES):
        entry = tuple(
            jnp.broadcast_to(jnp.sum(jnp.where(lane == at, v, 0.0), axis=1, keepdims=True), (8, 128)) for v in value
        )
        gram[i, j] = entry
        gram[j, i] = entry
    add, times = pair_add, pair_multiply
    minus = lambda a, b: pair_add(a, pair_negative(b))

    def form(left, right, shift):
        total = None
        for i, a in enumerate(left):
            for j, b in enumerate(right):
                term = times(times(a, b), gram[i, j + shift])
                total = term if total is None else add(total, term)
        return total

    one = (jnp.ones((8, 128), F32), jnp.zeros((8, 128), F32))
    alpha0 = pair_divide(gram[0, 0], gram[0, 1])
    residual = [one, pair_negative(alpha0)]
    norm1 = form(residual, residual, 0)
    beta0 = pair_divide(norm1, gram[0, 0])
    along1 = [add(one, beta0), pair_negative(alpha0)]
    alpha1 = pair_divide(norm1, form(along1, along1, 1))
    residual = [one, minus(residual[1], times(alpha1, along1[0])), pair_negative(times(alpha1, along1[1]))]
    norm2 = form(residual, residual, 0)
    beta1 = pair_divide(norm2, norm1)
    along2 = [add(one, times(beta1, along1[0])), add(residual[1], times(beta1, along1[1])), residual[2]]
    alpha2 = pair_divide(norm2, form(along2, along2, 1))
    weight0 = add(alpha0, add(times(alpha1, along1[0]), times(alpha2, along2[0])))
    weight1 = add(times(alpha1, along1[1]), times(alpha2, along2[1]))
    weight2 = times(alpha2, along2[2])
    total = weight0[0] * first[0:8, :] + (weight1[0] * second[0:8, :] + weight2[0] * third[0:8, :])
    for c in range(3):
        forces[c : c + 1, 0:128] = total[2 * c : 2 * c + 1, :]
        forces[c : c + 1, 128:256] = total[2 * c + 1 : 2 * c + 2, :]


def call(kernel, name, outs, *operands, memory=None, scratch=()):
    spec = lambda space: pl.BlockSpec(memory_space=space)
    memory = memory or [pltpu.VMEM] * len(operands)
    return pl.pallas_call(
        kernel,
        name=name,
        out_shape=[jax.ShapeDtypeStruct(shape, kind) for shape, kind in outs],
        in_specs=[spec(space) for space in memory],
        out_specs=[spec(pltpu.VMEM)] * len(outs),
        scratch_shapes=list(scratch),
        compiler_params=PARAMS,
    )(*operands)


def body(density, base_velocity, cells, offsets, target, stiffness, counts):
    rows = lambda n: ((n, 128), F32)
    vmem, smem, hbm = pltpu.VMEM, pltpu.SMEM, pltpu.HBM
    table_shapes = [((32, COLS), F32), ((256, COLS), BF16), ((256, COLS), BF16)]
    used_shape = [((8, 128), jnp.int32)]
    arguments = (density, base_velocity, cells, offsets, target, stiffness.reshape(1, MARKERS))
    fields, own, to_above, to_below = call(
        pack_kernel, "pack", [rows(256), rows(24), rows(80), rows(80)],
        *(pltpu.with_memory_space_constraint(a, hbm) for a in arguments), counts,
        memory=[hbm] * 6 + [smem],
        scratch=[
            vmem((8, 8, 128), F32), vmem((3, 8, 8, 128), F32), vmem((3, MARKERS), jnp.int32),
            vmem((3, MARKERS), F32), vmem((3, MARKERS), F32), vmem((1, MARKERS), F32),
            pltpu.SemaphoreType.DMA((6,)),
        ],
    )
    below, above = shifted(to_above, "gz", 1), shifted(to_below, "gz", -1)
    wide, marks, aux, upward, downward = call(
        deepen_z_kernel, "deepen_z", [rows(320), rows(40), rows(72), rows(96), rows(136)], fields, own, below, above
    )
    below, above = shifted(upward, GY, 1), shifted(downward, GY, -1)
    deep, three, upward, downward = call(
        deepen_y_kernel, "deepen_y", [rows(640), rows(120), rows(216), rows(280)], wide, marks, below, above
    )
    below, above = shifted(upward, "gx", 1), shifted(downward, "gx", -1)
    own_tables = call(
        own_tables_kernel, "own_tables", table_shapes + used_shape, three
    )
    side_tables = call(
        side_tables_kernel, "side_tables", table_shapes * 2 + used_shape, below, above
    )
    velocity_scratch = [vmem((3 * INNER, LANES), BF16)] * 2
    image_scratch = vmem((24, 128), F32)
    scale, start = call(
        setup_kernel, "setup", [((ROWS, LANES), F32), rows(24)], deep, below, above, *own_tables[0:3], aux, own_tables[3],
        scratch=velocity_scratch + [image_scratch],
    )

    def image_of(last, vector, *others):
        below, above = shifted(vector, GY, 1), shifted(vector, GY, -1)
        begun = call(
            own_spread_last if last else own_spread, "own_spread",
            [((3 * INNER, LANES), F32)] + ([rows(8)] if last else []), vector, *own_tables, *others,
            scratch=[vmem((3 * INNER, 384), BF16)] * 2,
        )
        held = list(begun) + (list(side_tables) if vector is start else [])
        three = lax.optimization_barrier((jnp.concatenate([vector, below, above], axis=0), *held))[0]
        below_three, above_three = shifted(three, "gx", 1), shifted(three, "gx", -1)
        (own_part,) = call(
            own_image, "own_image", [rows(24)], begun[0], below, above, *own_tables, scale,
            scratch=[vmem((3 * INNER, 768), BF16)] * 2 + [vmem((3 * INNER, LANES), F32)] + velocity_scratch,
        )
        side_scratch = [vmem((192, STATIC), BF16)] * 2 + [vmem((192, LANES), F32)]
        side_scratch += [vmem((192, LANES), BF16)] * 2 + [image_scratch]
        (part,) = call(
            below_kernel, "below", [rows(24)], own_part, below_three, *own_tables, *side_tables[0:3], side_tables[6], scale,
            scratch=side_scratch,
        )
        (result,) = call(
            last_kernel if last else above_kernel, "above", [rows(256 if last else 24)],
            part, above_three, *own_tables, *side_tables[3:7], scale, aux, vector, *others, *begun[1:],
            scratch=side_scratch,
        )
        return result

    second = image_of(False, start)
    third = image_of(False, second)
    sums = image_of(True, third, start, second)
    gathered = lax.all_to_all(sums, GX_GY_GZ, 0, 0, tiled=True)
    (forces,) = call(finish_kernel, "finish", [((3, MARKERS), F32)], gathered, start, second, third)
    return forces


def solution(mesh):
    finer = Mesh(
        mesh.devices.reshape(mesh.shape["gx"], 4, 2, mesh.shape["gz"]), ("gx", "gy_0", "gy_1", "gz")
    )
    return jax.shard_map(
        body,
        mesh=finer,
        in_specs=(
            P("gx", GY, "gz"),
            P(None, "gx", GY, "gz"),
            P(None, GX_GY_GZ),
            P(None, GX_GY_GZ),
            P(None, GX_GY_GZ),
            P(GX_GY_GZ),
            P(GX_GY_GZ),
        ),
        out_specs=P(None, GX_GY_GZ),
        check_vma=False,
    )
```

```python
import jax
import jax.numpy as jnp
from jax import lax
from jax.experimental import pallas as pl
from jax.experimental.pallas import tpu as pltpu
from jax.sharding import Mesh
from jax.sharding import PartitionSpec as P

GY = ("gy_0", "gy_1")
GX_GY_GZ = ("gx", "gy_0", "gy_1", "gz")

PLANES = 13
YPAD = 16
ROWS = PLANES * YPAD
INNER = 11 * YPAD
LANES = 256
DEEP = 16
REACH = 12
MARKERS = 256
FIRST = 3 * MARKERS
STATIC = FIRST + 3 * 128
COLS = STATIC + 3 * 384
F32 = jnp.float32
BF16 = jnp.bfloat16
PARAMS = pltpu.CompilerParams(vmem_limit_bytes=12 * 1024 * 1024)


def shifted(shard, axis, by):
    length = lax.axis_size(axis)
    return lax.ppermute(shard, axis, [(i, (i + by) % length) for i in range(length)])


def swapped_y(to_apart, to_near):
    length = lax.axis_size(GY)
    apart = lax.ppermute(to_apart, GY, [(i, (i + 1 if i % 2 else i - 1) % length) for i in range(length)])
    return apart, lax.ppermute(to_near, GY, [(i, i ^ 1) for i in range(length)])


def apart_is_below():
    return lax.axis_index("gy_1") == 0


def halves(value):
    high = value.astype(BF16)
    return high, (value - high.astype(F32)).astype(BF16)


def transposed_dot(left, right):
    return lax.dot_general(left, right, (((1,), (1,)), ((), ())), preferred_element_type=F32)


def plain_dot(left, right):
    return lax.dot_general(left, right, (((1,), (0,)), ((), ())), preferred_element_type=F32)


def delta_weights(fraction):
    def inner(radius):
        return (3.0 - 2.0 * radius + jnp.sqrt(jnp.maximum(1.0 + 4.0 * radius - 4.0 * radius * radius, 0.0))) / 8.0

    def outer(radius):
        return (5.0 - 2.0 * radius - jnp.sqrt(jnp.maximum(-7.0 + 12.0 * radius - 4.0 * radius * radius, 0.0))) / 8.0

    return [outer(1.0 + fraction), inner(fraction), inner(1.0 - fraction), outer(2.0 - fraction)]


def delta_rows(extent, cell, weights, at):
    step = lax.broadcasted_iota(jnp.int32, (extent, cell.shape[1]), 0).astype(F32) - cell
    value = jnp.zeros_like(step)
    for place, weight in zip((-1.0, 0.0, 1.0, 2.0), weights):
        value = jnp.where(step == place, weight[at : at + 1], value)
    return value


def pack_kernel(
    density_in, base_in, cells_in, offsets_in, target_in, stiffness_in, counts, fields, own, to_above, to_below,
    density, base, cells, offsets, target, stiffness, arrived,
):
    sources = (density_in, base_in, cells_in, offsets_in, target_in, stiffness_in)
    places = (density, base, cells, offsets, target, stiffness)
    copies = [pltpu.make_async_copy(a, b, arrived.at[i]) for i, (a, b) in enumerate(zip(sources, places))]
    for copy in copies:
        copy.start()
    for copy in copies:
        copy.wait()
    for plane in range(8):
        for field in range(4):
            piece = density[plane] if field == 3 else base[field, plane]
            fields[(field * 8 + plane) * 8 : (field * 8 + plane) * 8 + 8, :] = piece
    for block in range(2):
        turned = fields[block * 128 : block * 128 + 128, :].T
        to_below[block * 16 : block * 16 + 16, :] = turned[0:DEEP]
        to_above[block * 16 : block * 16 + 16, :] = turned[128 - DEEP : 128]
    lane = lax.broadcasted_iota(jnp.int32, (1, MARKERS), 1)
    live = jnp.where(lane < counts[0], 1.0, 0.0).astype(F32)
    inside = [(cells[k : k + 1, :] & (7, 7, 127)[k]).astype(F32) for k in range(3)]
    data = inside + [offsets[k : k + 1, :] for k in range(3)] + [live, stiffness[0:1, :]]
    data += [target[k : k + 1, :] for k in range(3)]
    for k, row in enumerate(data):
        own[2 * k : 2 * k + 1, :] = row[:, 0:128]
        own[2 * k + 1 : 2 * k + 2, :] = row[:, 128:256]
    own[22:24, :] = jnp.zeros((2, 128), F32)
    table = jnp.concatenate(data + [jnp.zeros((5, MARKERS), F32)], axis=0)
    table_high = table.astype(BF16)
    rest = table - table_high.astype(F32)
    table_mid = rest.astype(BF16)
    table_low = (rest - table_mid.astype(F32)).astype(BF16)
    upper = jnp.where(inside[2] >= 128.0 - REACH, live, 0.0)
    lower = jnp.where(inside[2] < 1.0 * REACH, live, 0.0)
    flags = jnp.concatenate([upper, lower, jnp.zeros((14, MARKERS), F32)], axis=0).astype(BF16)
    earlier = lax.broadcasted_iota(jnp.int32, (MARKERS, MARKERS), 0) < lax.broadcasted_iota(
        jnp.int32, (MARKERS, MARKERS), 1
    )
    ranks = plain_dot(flags, jnp.where(earlier, 1.0, 0.0).astype(BF16)).astype(jnp.int32)
    slot = lax.broadcasted_iota(jnp.int32, (512, MARKERS), 0)
    lane = lax.broadcasted_iota(jnp.int32, (1, 128), 1)
    for at, (flag, out, shift) in enumerate(((upper, to_above, -128.0), (lower, to_below, 128.0))):
        rank = ranks[at : at + 1, :]
        goal = ((rank >> 6) << 7) + (rank & 63) + 64 * at
        chosen = jnp.where((slot == goal) & (flag > 0.0), 1.0, 0.0).astype(BF16)
        moved = transposed_dot(table_high, chosen) + transposed_dot(table_mid, chosen)
        moved = moved + transposed_dot(table_low, chosen)
        number = jnp.broadcast_to(jnp.sum(flag, axis=1, keepdims=True), (1, 128))
        number = jnp.where((lane < 64) == (at == 0), number, 0.0)
        for block in range(4):
            columns = slice(block * 128, block * 128 + 128)
            for k in range(11):
                row = moved[k : k + 1, columns]
                if k == 2:
                    row = row + shift * moved[6:7, columns]
                out[32 + 4 * k + block : 33 + 4 * k + block, :] = row
            out[76 + block : 77 + block, :] = number


def deepen_z_kernel(fields, own, below, above, wide, marks, aux, to_apart, to_near, upward, downward):
    lane = lax.broadcasted_iota(jnp.int32, (128, 128), 1)
    packed = jnp.zeros((64, 128), F32)
    lane64 = lax.broadcasted_iota(jnp.int32, (64, 128), 1)
    for block in range(2):
        edge = jnp.concatenate(
            [below[block * 16 : block * 16 + 16, :], above[block * 16 : block * 16 + 16, :], jnp.zeros((96, 128), F32)],
            axis=0,
        ).T
        turned = pltpu.roll(fields[block * 128 : block * 128 + 128, :], DEEP, 1)
        wide[block * 128 : block * 128 + 128, :] = jnp.where(lane < DEEP, edge, turned)
        beyond = jnp.where(lane < DEEP, turned, edge)
        for half in range(2):
            field = 2 * block + half
            piece = beyond[half * 64 : half * 64 + 64]
            piece = pltpu.roll(piece, 32 * field, 1) if field else piece
            packed = jnp.where((lane64 >= 32 * field) & (lane64 < 32 * field + 32), piece, packed)
    wide[256:320, :] = packed
    for at in range(24):
        upward[at : at + 1, :] = wide[at * 8 + 7 : at * 8 + 8, :]
        downward[at * 2 : at * 2 + 2, :] = wide[at * 8 : at * 8 + 2, :]
    for at in range(16):
        row = 192 + at * 8
        upward[24 + at * 2 : 26 + at * 2, :] = wide[row + 6 : row + 8, :]
        downward[48 + at * 3 : 51 + at * 3, :] = wide[row : row + 3, :]
    halo = below[32:80, :] + above[32:80, :]
    marks[0:12, :] = own[0:12, :]
    marks[12:36, :] = halo[0:24]
    marks[36:40, :] = jnp.broadcast_to(halo[44:45], (4, 128))
    upward[56:96, :] = marks[...]
    downward[96:136, :] = marks[...]
    upward[96:136, :] = jnp.zeros((40, 128), F32)
    order = apart_is_below()
    to_apart[...] = jnp.where(order, downward[...], upward[...])
    to_near[...] = jnp.where(order, upward[...], downward[...])
    aux[...] = jnp.zeros((72, 128), F32)
    for kind in range(3):
        for c in range(3):
            k = 6 + kind if kind < 2 else 8 + c
            aux[24 * kind + 2 * c : 24 * kind + 2 * c + 2, :] = own[2 * k : 2 * k + 2, :]
            for block in range(4):
                row = 24 * kind + 8 + 3 * block + c
                aux[row : row + 1, :] = halo[4 * k + block : 4 * k + block + 1]


def deepen_y_kernel(wide, marks, apart, near, deep, three, upward, downward, below, above):
    order = apart_is_below()
    below[...] = jnp.where(order, apart[...], near[...])
    above[...] = jnp.where(order, near[...], apart[...])
    for at in range(40):
        row = at * YPAD
        deep[row + 2 : row + 10, :] = wide[at * 8 : at * 8 + 8, :]
        if at < 24:
            deep[row : row + 1, :] = jnp.ones((1, 128), F32)
            deep[row + 1 : row + 2, :] = below[at : at + 1, :]
            deep[row + 10 : row + 12, :] = above[at * 2 : at * 2 + 2, :]
            deep[row + 12 : row + 16, :] = jnp.ones((4, 128), F32)
        else:
            near, far = 24 + (at - 24) * 2, 48 + (at - 24) * 3
            deep[row : row + 2, :] = below[near : near + 2, :]
            deep[row + 10 : row + 13, :] = above[far : far + 3, :]
            deep[row + 13 : row + 16, :] = jnp.ones((3, 128), F32)
    for c in range(3):
        upward[c * 13 : c * 13 + 13, :] = deep[c * 128 + 112 : c * 128 + 125, :]
        for k in range(2):
            row = c * 128 + k * YPAD
            downward[c * 26 + k * 13 : c * 26 + k * 13 + 13, :] = deep[row : row + 13, :]
    for at in range(2):
        row = (3 + at) * 128
        for k in range(3):
            if k < 2:
                upward[39 + at * 26 + k * 13 : 52 + at * 26 + k * 13, :] = deep[row + 96 + k * 16 : row + 109 + k * 16, :]
            downward[78 + at * 39 + k * 13 : 91 + at * 39 + k * 13, :] = deep[row + k * 16 : row + k * 16 + 13, :]
    three[0:40, :] = marks[...]
    three[40:80, :] = jnp.where(order, below[56:96, :], above[96:136, :])
    three[80:120, :] = jnp.where(order, above[96:136, :], below[56:96, :])
    upward[96:216, :] = three[...]
    downward[160:280, :] = three[...]


def blocks_used(refs):
    most = jnp.max(jnp.concatenate([ref[first + 36 + 40 * part : first + 37 + 40 * part, :] for ref, first in refs for part in range(3)], axis=0))
    return (most.astype(jnp.int32) + 63) >> 6


def trips(used):
    return jnp.max(used[0:1, :])


def fill_tables(ref, first, along_x, used, plane_weights, z_high, z_low):
    apart = jnp.where(apart_is_below(), -8.0, 8.0).astype(F32)

    def fill(read, along_y, place):
        fractions = jnp.concatenate([read(3), read(4), read(5), jnp.zeros((5, 128), F32)], axis=0)
        weights = delta_weights(fractions)
        plane_weights[0:16, place] = delta_rows(16, read(0) + (along_x + 2.0), weights, 0)
        plane_weights[16:32, place] = delta_rows(16, read(1) + (along_y + 2.0), weights, 1)
        high, rest = halves(delta_rows(160, read(2) + 16.0, weights, 2))
        z_high[0:160, place] = high
        z_low[0:160, place] = rest

    for part, along_y in enumerate((0.0, apart, -apart)):
        top = first + 40 * part
        for half in range(2):
            column = part * 256 + half * 128
            fill(lambda k: ref[top + 2 * k + half : top + 2 * k + half + 1, :], along_y, slice(column, column + 128))
        column = FIRST + part * 128
        fill(lambda k: ref[top + 12 + 4 * k : top + 13 + 4 * k, :], along_y, slice(column, column + 128))

    def further(block, carry):
        for part, along_y in enumerate((0.0, apart, -apart)):
            top = first + 40 * part + 12 + block
            column = pl.multiple_of(STATIC + (block - 1) * 384 + part * 128, 128)
            fill(lambda k: ref[pl.ds(top + 4 * k, 1), :], along_y, pl.ds(column, 128))
        return carry

    lax.fori_loop(1, used, further, 0)
    z_high[160:256, :] = jnp.zeros((96, COLS), BF16)
    z_low[160:256, :] = jnp.zeros((96, COLS), BF16)


def own_tables_kernel(three, plane_weights, z_high, z_low, used):
    count = blocks_used([(three, 0)])
    used[...] = jnp.full((8, 128), count, jnp.int32)
    fill_tables(three, 0, 0.0, count, plane_weights, z_high, z_low)


def side_tables_kernel(below, above, b_weights, b_high, b_low, a_weights, a_high, a_low, used):
    count = blocks_used([(below, 96), (above, 160)])
    used[...] = jnp.full((8, 128), count, jnp.int32)
    fill_tables(below, 96, -8.0, count, b_weights, b_high, b_low)
    fill_tables(above, 160, 8.0, count, a_weights, a_high, a_low)


def interpolate(velocity_high, velocity_low, planes, plane_weights, z_high, z_low, used, image):
    def lines(place):
        partial = plain_dot(velocity_high[...], z_high[:, place]) + plain_dot(velocity_low[...], z_high[:, place])
        partial = partial + plain_dot(velocity_high[...], z_low[:, place])
        result = []
        for c in range(3):
            total = None
            for at, plane in enumerate(planes):
                row = (c * len(planes) + at) * YPAD
                term = partial[row : row + YPAD] * plane_weights[plane : plane + 1, place]
                total = term if total is None else total + term
            result.append(jnp.sum(total * plane_weights[16:32, place], axis=0, keepdims=True))
        return result

    image[...] = jnp.zeros((24, 128), F32)
    for c, line in enumerate(lines(slice(0, MARKERS))):
        image[2 * c : 2 * c + 1, :] = line[:, 0:128]
        image[2 * c + 1 : 2 * c + 2, :] = line[:, 128:256]
    for c, line in enumerate(lines(slice(FIRST, FIRST + 128))):
        image[8 + c : 9 + c, :] = line

    def further(block, carry):
        for c, line in enumerate(lines(pl.ds(pl.multiple_of(STATIC + (block - 1) * 384, 128), 128))):
            image[pl.ds(8 + 3 * block + c, 1), :] = line
        return carry

    lax.fori_loop(1, used, further, 0)


def setup_kernel(deep, below, above, plane_weights, z_high, z_low, aux, used, scale, start, velocity_high, velocity_low, image):
    lane = lax.broadcasted_iota(jnp.int32, (YPAD, 128), 1)
    used_rows = lax.broadcasted_iota(jnp.int32, (YPAD, 128), 0) < 13
    for plane in range(PLANES):
        at = plane * YPAD

        def piece(field):
            if plane < 2:
                row = field * 13 if field < 3 else 39 + (field - 3) * 26 + plane * 13
                return jnp.where(used_rows, below[row : row + 16, :], 1.0)
            if plane < 10:
                row = field * 128 + (plane - 2) * 16
                return deep[row : row + 16, :]
            row = field * 26 if field < 3 else 78 + (field - 3) * 39
            row += (plane - 10) * 13
            return jnp.where(used_rows, above[row : row + 16, :], 1.0)

        packed = piece(4)
        scale[at : at + YPAD, 0:128] = lax.rsqrt(piece(3))
        scale[at : at + YPAD, 128:256] = lax.rsqrt(jnp.where(lane < 32, pltpu.roll(packed, 32, 1), 1.0))
        if 1 <= plane <= 11:
            for c in range(3):
                row = c * INNER + at - YPAD
                top, rest = halves(piece(c))
                velocity_high[row : row + YPAD, 0:128] = top
                velocity_low[row : row + YPAD, 0:128] = rest
                beyond = pltpu.roll(packed, 128 - 32 * c, 1) if c else packed
                top, rest = halves(jnp.where(lane < 32, beyond, 0.0))
                velocity_high[row : row + YPAD, 128:256] = top
                velocity_low[row : row + YPAD, 128:256] = rest
    interpolate(velocity_high, velocity_low, range(1, 12), plane_weights, z_high, z_low, trips(used), image)
    start[...] = aux[0:24, :] * (aux[48:72, :] - image[...])


def fill_tile(rows, planes, plane_weights, weight, left_high, left_low, place):
    along_y = plane_weights[16:32, weight]
    vector = [row * along_y for row in rows]
    for at, plane in enumerate(planes):
        along_x = plane_weights[plane : plane + 1, weight]
        for c in range(3):
            top, rest = halves(vector[c] * along_x)
            row = (c * len(planes) + at) * YPAD
            left_high[row : row + YPAD, place] = top
            left_low[row : row + YPAD, place] = rest


def spread_columns(left_high, left_low, z_high, z_low, left, right):
    total = transposed_dot(left_high[:, left], z_high[:, right]) + transposed_dot(left_low[:, left], z_high[:, right])
    return total + transposed_dot(left_high[:, left], z_low[:, right])


def spread_group(refs, planes, plane_weights, z_high, z_low, used, left_high, left_low, total, begun=None, part0=0):
    count = len(refs)
    for at, (ref, first) in enumerate(refs):
        part = part0 + at
        for half in range(2):
            place = slice(at * 256 + half * 128, at * 256 + half * 128 + 128)
            weight = slice(part * 256 + half * 128, part * 256 + half * 128 + 128)
            rows = [ref[first + 2 * c + half : first + 2 * c + half + 1, :] for c in range(3)]
            fill_tile(rows, planes, plane_weights, weight, left_high, left_low, place)
        place = slice(count * 256 + at * 128, count * 256 + at * 128 + 128)
        weight = slice(FIRST + part * 128, FIRST + part * 128 + 128)
        rows = [ref[first + 8 + c : first + 9 + c, :] for c in range(3)]
        fill_tile(rows, planes, plane_weights, weight, left_high, left_low, place)
    value = spread_columns(
        left_high, left_low, z_high, z_low, slice(0, count * 256), slice(part0 * 256, (part0 + count) * 256)
    )
    value = value + spread_columns(
        left_high, left_low, z_high, z_low, slice(count * 256, count * 384),
        slice(FIRST + part0 * 128, FIRST + (part0 + count) * 128),
    )
    total[...] = value if begun is None else value + begun[...]

    def further(block, carry):
        for at, (ref, first) in enumerate(refs):
            column = pl.multiple_of(STATIC + (block - 1) * 384 + (part0 + at) * 128, 128)
            rows = [ref[pl.ds(first + 8 + 3 * block + c, 1), :] for c in range(3)]
            place = slice(at * 128, at * 128 + 128)
            fill_tile(rows, planes, plane_weights, pl.ds(column, 128), left_high, left_low, place)
        right = pl.ds(pl.multiple_of(STATIC + (block - 1) * 384 + part0 * 128, 128), count * 128)
        total[...] += spread_columns(left_high, left_low, z_high, z_low, slice(0, count * 128), right)
        return carry

    lax.fori_loop(1, used, further, 0)


def respond(moved, planes, outs, scale, velocity_high, velocity_low):
    axial, diagonal = 1.0 / 6.0, 1.0 / 12.0
    up_y = lambda a: pltpu.roll(a, 1, 0)
    down_y = lambda a: pltpu.roll(a, YPAD - 1, 0)
    up_z = lambda a: pltpu.roll(a, 1, 1)
    down_z = lambda a: pltpu.roll(a, LANES - 1, 1)
    onward, back, still = {}, {}, {}
    for at, plane in enumerate(planes):
        factor = scale[plane * YPAD : plane * YPAD + YPAD, :]
        rows = [(c * len(planes) + at) * YPAD for c in range(3)]
        gx, gy, gz = (moved[row : row + YPAD, :] * factor for row in rows)
        hx, hy, hz = gx * diagonal, gy * diagonal, gz * diagonal
        sum_xy, dif_xy = hx + hy, hx - hy
        zx_up, zy_up, zz_up = up_z(hx), up_z(hy), up_z(hz)
        zx_dn, zy_dn, zz_dn = down_z(hx), down_z(hy), down_z(hz)
        xz_sum_up, xz_sum_dn, xz_dif_up, xz_dif_dn = zx_up + zz_up, zx_dn + zz_dn, zx_up - zz_up, zx_dn - zz_dn
        xy_sum_up, xy_sum_dn, xy_dif_up, xy_dif_dn = up_y(sum_xy), down_y(sum_xy), up_y(dif_xy), down_y(dif_xy)
        ax = gx * axial
        onward[plane] = (
            ax + ((xy_sum_up + xy_dif_dn) + (xz_sum_up + xz_dif_dn)),
            xy_sum_up - xy_dif_dn,
            xz_sum_up - xz_dif_dn,
        )
        back[plane] = (
            ax + ((xy_sum_dn + xy_dif_up) + (xz_sum_dn + xz_dif_up)),
            xy_sum_dn - xy_dif_up,
            xz_sum_dn - xz_dif_up,
        )
        yz_same = up_y(zy_up + zz_up)
        yz_same_dn = down_y(zy_dn + zz_dn)
        yz_cross = up_y(zy_dn - zz_dn)
        yz_cross_dn = down_y(zy_up - zz_up)
        same, cross = yz_same + yz_same_dn, yz_cross + yz_cross_dn
        still[plane] = (
            gx,
            gy + ((up_y(hy) + down_y(hy)) * 2.0 + (same + cross)),
            gz + ((zz_up + zz_dn) * 2.0 + (same - cross)),
        )
        for place, out in enumerate(outs):
            if min(out + 1, planes[-1]) != plane:
                continue
            factor = scale[out * YPAD : out * YPAD + YPAD, :] * 0.5
            for c in range(3):
                parts = [group[at][c] for group, at in ((onward, out - 1), (still, out), (back, out + 1)) if at in group]
                total = parts[0]
                for part in parts[1:]:
                    total = total + part
                top, rest = halves(total * factor)
                row = (c * len(outs) + place) * YPAD
                velocity_high[row : row + YPAD, :] = top
                velocity_low[row : row + YPAD, :] = rest


def own_spread(own, plane_weights, z_high, z_low, used, total, left_high, left_low):
    spread_group([(own, 0)], range(1, 12), plane_weights, z_high, z_low, trips(used), left_high, left_low, total)


def own_image(
    begun, apart, near, plane_weights, z_high, z_low, used, scale, result, left_high, left_low, moved, velocity_high,
    velocity_low,
):
    refs = [(apart, 0), (near, 0)]
    planes = range(1, 12)
    count = trips(used)
    spread_group(refs, planes, plane_weights, z_high, z_low, count, left_high, left_low, moved, begun, 1)
    respond(moved, planes, planes, scale, velocity_high, velocity_low)
    interpolate(velocity_high, velocity_low, planes, plane_weights, z_high, z_low, count, result)


def side_image(
    below, begun, three, own_tables, own_used, side_tables, used, scale, left_high, left_low, moved, velocity_high,
    velocity_low, image,
):
    planes, outs = (range(0, 4), range(1, 5)) if below else (range(9, 13), range(8, 12))
    refs = [(three, 24 * part) for part in range(3)]
    spread_group(refs, planes, *side_tables, trips(used), left_high, left_low, moved)
    respond(moved, planes, outs, scale, velocity_high, velocity_low)
    interpolate(velocity_high, velocity_low, outs, *own_tables, trips(own_used), image)
    return begun[...] + image[...]


def below_kernel(begun, three, w, h, l, own_used, sw, sh, sl, used, scale, result, *scratch):
    result[...] = side_image(True, begun, three, (w, h, l), own_used, (sw, sh, sl), used, scale, *scratch)


def above_image(begun, three, w, h, l, own_used, sw, sh, sl, used, scale, aux, vector, *scratch):
    image = side_image(False, begun, three, (w, h, l), own_used, (sw, sh, sl), used, scale, *scratch)
    return aux[0:24, :] * (image + aux[24:48, :] * vector[...])


def above_kernel(begun, three, w, h, l, own_used, sw, sh, sl, used, scale, aux, vector, result, *scratch):
    result[...] = above_image(begun, three, w, h, l, own_used, sw, sh, sl, used, scale, aux, vector, *scratch)


def two_sum(a, b):
    total = a + b
    part = total - a
    return total, (a - (total - part)) + (b - part)


def fast_two_sum(a, b):
    total = a + b
    return total, b - (total - a)


def split(a):
    scaled = a * 4097.0
    high = scaled - (scaled - a)
    return high, a - high


def two_product(a, b):
    product = a * b
    a_high, a_low = split(a)
    b_high, b_low = split(b)
    return product, ((a_high * b_high - product) + a_high * b_low + a_low * b_high) + a_low * b_low


def pair_add(a, b):
    head, tail = two_sum(a[0], b[0])
    return fast_two_sum(head, tail + (a[1] + b[1]))


def pair_negative(a):
    return (-a[0], -a[1])


def pair_multiply(a, b):
    head, tail = two_product(a[0], b[0])
    return fast_two_sum(head, tail + (a[0] * b[1] + a[1] * b[0]))


def pair_divide(a, b):
    first = a[0] / b[0]
    rest = pair_add(a, pair_negative(pair_multiply((first, jnp.zeros_like(first)), b)))
    return fast_two_sum(first, rest[0] / b[0])


ENTRIES = ((0, 0), (0, 1), (0, 2), (0, 3), (1, 1), (1, 2), (1, 3), (2, 2), (2, 3))


def gram_lanes(vectors, entries, packed):
    lane = lax.broadcasted_iota(jnp.int32, (8, 128), 1)
    for at, (i, j) in enumerate(ENTRIES):
        if (i, j) not in entries:
            continue
        value = two_product(vectors[i], vectors[j])
        for axis, steps in ((0, (4, 2, 1)), (1, (64, 32, 16, 8, 4, 2, 1))):
            for step in steps:
                value = pair_add(value, (pltpu.roll(value[0], step, axis), pltpu.roll(value[1], step, axis)))
        packed = jnp.where(lane == at, value[0], jnp.where(lane == 16 + at, value[1], packed))
    return packed


EARLY = tuple(entry for entry in ENTRIES if entry[1] < 3)
LATE = tuple(entry for entry in ENTRIES if entry[1] == 3)


def own_spread_last(own, w, h, l, used, first, second, total, early, *scratch):
    own_spread(own, w, h, l, used, total, *scratch)
    early[...] = gram_lanes([first[0:8, :], second[0:8, :], own[0:8, :]], EARLY, jnp.zeros((8, 128), F32))


def last_kernel(
    begun, three, w, h, l, own_used, sw, sh, sl, used, scale, aux, third, first, second, early, sums, *scratch
):
    fourth = above_image(begun, three, w, h, l, own_used, sw, sh, sl, used, scale, aux, third, *scratch)
    vectors = [first[0:8, :], second[0:8, :], third[0:8, :], fourth[0:8]]
    packed = gram_lanes(vectors, LATE, early[...])
    for block in range(sums.shape[0] // 8):
        sums[block * 8 : block * 8 + 8, :] = packed


def finish_kernel(gathered, first, second, third, forces):
    a = gathered[...]
    count = a.shape[0]
    value = (a, pltpu.roll(a, 112, 1))
    while count > 8:
        count //= 2
        value = pair_add(
            (value[0][0:count], value[1][0:count]), (value[0][count : 2 * count], value[1][count : 2 * count])
        )
    for step in (4, 2, 1):
        value = pair_add(value, (pltpu.roll(value[0], step, 0), pltpu.roll(value[1], step, 0)))
    lane = lax.broadcasted_iota(jnp.int32, (8, 128), 1)
    gram = {}
    for at, (i, j) in enumerate(ENTRIES):
        entry = tuple(
            jnp.broadcast_to(jnp.sum(jnp.where(lane == at, v, 0.0), axis=1, keepdims=True), (8, 128)) for v in value
        )
        gram[i, j] = entry
        gram[j, i] = entry
    add, times = pair_add, pair_multiply
    minus = lambda a, b: pair_add(a, pair_negative(b))

    def form(left, right, shift):
        total = None
        for i, a in enumerate(left):
            for j, b in enumerate(right):
                term = times(times(a, b), gram[i, j + shift])
                total = term if total is None else add(total, term)
        return total

    one = (jnp.ones((8, 128), F32), jnp.zeros((8, 128), F32))
    alpha0 = pair_divide(gram[0, 0], gram[0, 1])
    residual = [one, pair_negative(alpha0)]
    norm1 = form(residual, residual, 0)
    beta0 = pair_divide(norm1, gram[0, 0])
    along1 = [add(one, beta0), pair_negative(alpha0)]
    alpha1 = pair_divide(norm1, form(along1, along1, 1))
    residual = [one, minus(residual[1], times(alpha1, along1[0])), pair_negative(times(alpha1, along1[1]))]
    norm2 = form(residual, residual, 0)
    beta1 = pair_divide(norm2, norm1)
    along2 = [add(one, times(beta1, along1[0])), add(residual[1], times(beta1, along1[1])), residual[2]]
    alpha2 = pair_divide(norm2, form(along2, along2, 1))
    weight0 = add(alpha0, add(times(alpha1, along1[0]), times(alpha2, along2[0])))
    weight1 = add(times(alpha1, along1[1]), times(alpha2, along2[1]))
    weight2 = times(alpha2, along2[2])
    total = weight0[0] * first[0:8, :] + (weight1[0] * second[0:8, :] + weight2[0] * third[0:8, :])
    for c in range(3):
        forces[c : c + 1, 0:128] = total[2 * c : 2 * c + 1, :]
        forces[c : c + 1, 128:256] = total[2 * c + 1 : 2 * c + 2, :]


def call(kernel, name, outs, *operands, memory=None, scratch=()):
    spec = lambda space: pl.BlockSpec(memory_space=space)
    memory = memory or [pltpu.VMEM] * len(operands)
    return pl.pallas_call(
        kernel,
        name=name,
        out_shape=[jax.ShapeDtypeStruct(shape, kind) for shape, kind in outs],
        in_specs=[spec(space) for space in memory],
        out_specs=[spec(pltpu.VMEM)] * len(outs),
        scratch_shapes=list(scratch),
        compiler_params=PARAMS,
    )(*operands)


def body(density, base_velocity, cells, offsets, target, stiffness, counts):
    rows = lambda n: ((n, 128), F32)
    vmem, smem, hbm = pltpu.VMEM, pltpu.SMEM, pltpu.HBM
    table_shapes = [((32, COLS), F32), ((256, COLS), BF16), ((256, COLS), BF16)]
    used_shape = [((8, 128), jnp.int32)]
    arguments = (density, base_velocity, cells, offsets, target, stiffness.reshape(1, MARKERS))
    fields, own, to_above, to_below = call(
        pack_kernel, "pack", [rows(256), rows(24), rows(80), rows(80)],
        *(pltpu.with_memory_space_constraint(a, hbm) for a in arguments), counts,
        memory=[hbm] * 6 + [smem],
        scratch=[
            vmem((8, 8, 128), F32), vmem((3, 8, 8, 128), F32), vmem((3, MARKERS), jnp.int32),
            vmem((3, MARKERS), F32), vmem((3, MARKERS), F32), vmem((1, MARKERS), F32),
            pltpu.SemaphoreType.DMA((6,)),
        ],
    )
    below, above = shifted(to_above, "gz", 1), shifted(to_below, "gz", -1)
    wide, marks, aux, to_apart, to_near = call(
        deepen_z_kernel, "deepen_z", [rows(320), rows(40), rows(72), rows(136), rows(136)], fields, own, below, above,
        scratch=[vmem((136, 128), F32)] * 2,
    )
    apart, near = swapped_y(to_apart, to_near)
    deep, three, upward, downward = call(
        deepen_y_kernel, "deepen_y", [rows(640), rows(120), rows(216), rows(280)], wide, marks, apart, near,
        scratch=[vmem((136, 128), F32)] * 2,
    )
    below, above = shifted(upward, "gx", 1), shifted(downward, "gx", -1)
    own_tables = call(
        own_tables_kernel, "own_tables", table_shapes + used_shape, three
    )
    side_tables = call(
        side_tables_kernel, "side_tables", table_shapes * 2 + used_shape, below, above
    )
    velocity_scratch = [vmem((3 * INNER, LANES), BF16)] * 2
    image_scratch = vmem((24, 128), F32)
    scale, start = call(
        setup_kernel, "setup", [((ROWS, LANES), F32), rows(24)], deep, below, above, *own_tables[0:3], aux, own_tables[3],
        scratch=velocity_scratch + [image_scratch],
    )

    def image_of(last, vector, *others):
        apart, near = swapped_y(vector, vector)
        begun = call(
            own_spread_last if last else own_spread, "own_spread",
            [((3 * INNER, LANES), F32)] + ([rows(8)] if last else []), vector, *own_tables, *others,
            scratch=[vmem((3 * INNER, 384), BF16)] * 2,
        )
        held = list(begun) + (list(side_tables) if vector is start else [])
        three = lax.optimization_barrier((jnp.concatenate([vector, apart, near], axis=0), *held))[0]
        below_three, above_three = shifted(three, "gx", 1), shifted(three, "gx", -1)
        (own_part,) = call(
            own_image, "own_image", [rows(24)], begun[0], apart, near, *own_tables, scale,
            scratch=[vmem((3 * INNER, 768), BF16)] * 2 + [vmem((3 * INNER, LANES), F32)] + velocity_scratch,
        )
        side_scratch = [vmem((192, STATIC), BF16)] * 2 + [vmem((192, LANES), F32)]
        side_scratch += [vmem((192, LANES), BF16)] * 2 + [image_scratch]
        (part,) = call(
            below_kernel, "below", [rows(24)], own_part, below_three, *own_tables, *side_tables[0:3], side_tables[6], scale,
            scratch=side_scratch,
        )
        (result,) = call(
            last_kernel if last else above_kernel, "above", [rows(256 if last else 24)],
            part, above_three, *own_tables, *side_tables[3:7], scale, aux, vector, *others, *begun[1:],
            scratch=side_scratch,
        )
        return result

    second = image_of(False, start)
    third = image_of(False, second)
    sums = image_of(True, third, start, second)
    gathered = lax.all_to_all(sums, GX_GY_GZ, 0, 0, tiled=True)
    (forces,) = call(finish_kernel, "finish", [((3, MARKERS), F32)], gathered, start, second, third)
    return forces


def solution(mesh):
    finer = Mesh(
        mesh.devices.reshape(mesh.shape["gx"], 4, 2, mesh.shape["gz"]), ("gx", "gy_0", "gy_1", "gz")
    )
    return jax.shard_map(
        body,
        mesh=finer,
        in_specs=(
            P("gx", GY, "gz"),
            P(None, "gx", GY, "gz"),
            P(None, GX_GY_GZ),
            P(None, GX_GY_GZ),
            P(None, GX_GY_GZ),
            P(GX_GY_GZ),
            P(GX_GY_GZ),
        ),
        out_specs=P(None, GX_GY_GZ),
        check_vma=False,
    )
```

```python
import jax
import jax.numpy as jnp
from jax import lax
from jax.experimental import pallas as pl
from jax.experimental.pallas import tpu as pltpu
from jax.sharding import Mesh
from jax.sharding import PartitionSpec as P

GY = ("gy_0", "gy_1")
GX_GY_GZ = ("gx", "gy_0", "gy_1", "gz")

PLANES = 13
YPAD = 16
ROWS = PLANES * YPAD
INNER = 11 * YPAD
LANES = 256
DEEP = 16
REACH = 12
MARKERS = 256
FIRST = 3 * MARKERS
STATIC = FIRST + 3 * 128
COLS = STATIC + 3 * 384
F32 = jnp.float32
BF16 = jnp.bfloat16
PARAMS = pltpu.CompilerParams(vmem_limit_bytes=12 * 1024 * 1024)


def shifted(shard, axis, by):
    length = lax.axis_size(axis)
    return lax.ppermute(shard, axis, [(i, (i + by) % length) for i in range(length)])


def swapped_y(to_apart, to_near):
    length = lax.axis_size(GY)
    apart = lax.ppermute(to_apart, GY, [(i, (i + 1 if i % 2 else i - 1) % length) for i in range(length)])
    return apart, lax.ppermute(to_near, GY, [(i, i ^ 1) for i in range(length)])


def swapped_z(to_odd, to_even):
    length = lax.axis_size("gz")
    odd = lax.ppermute(to_odd, "gz", [(i, (i + 1 if i % 2 else i - 1) % length) for i in range(length)])
    return odd, lax.ppermute(to_even, "gz", [(i, i ^ 1) for i in range(length)])


def odd_is_below():
    return lax.rem(lax.axis_index("gz"), 2) == 0


def apart_is_below():
    return lax.axis_index("gy_1") == 0


def halves(value):
    high = value.astype(BF16)
    return high, (value - high.astype(F32)).astype(BF16)


def transposed_dot(left, right):
    return lax.dot_general(left, right, (((1,), (1,)), ((), ())), preferred_element_type=F32)


def plain_dot(left, right):
    return lax.dot_general(left, right, (((1,), (0,)), ((), ())), preferred_element_type=F32)


def delta_weights(fraction):
    def inner(radius):
        return (3.0 - 2.0 * radius + jnp.sqrt(jnp.maximum(1.0 + 4.0 * radius - 4.0 * radius * radius, 0.0))) / 8.0

    def outer(radius):
        return (5.0 - 2.0 * radius - jnp.sqrt(jnp.maximum(-7.0 + 12.0 * radius - 4.0 * radius * radius, 0.0))) / 8.0

    return [outer(1.0 + fraction), inner(fraction), inner(1.0 - fraction), outer(2.0 - fraction)]


def delta_rows(extent, cell, weights, at):
    step = lax.broadcasted_iota(jnp.int32, (extent, cell.shape[1]), 0).astype(F32) - cell
    value = jnp.zeros_like(step)
    for place, weight in zip((-1.0, 0.0, 1.0, 2.0), weights):
        value = jnp.where(step == place, weight[at : at + 1], value)
    return value


def pack_kernel(
    density_in, base_in, cells_in, offsets_in, target_in, stiffness_in, counts, fields, own, to_odd, to_even,
    density, base, cells, offsets, target, stiffness, arrived, to_above, to_below,
):
    sources = (density_in, base_in, cells_in, offsets_in, target_in, stiffness_in)
    places = (density, base, cells, offsets, target, stiffness)
    copies = [pltpu.make_async_copy(a, b, arrived.at[i]) for i, (a, b) in enumerate(zip(sources, places))]
    for copy in copies:
        copy.start()
    for copy in copies:
        copy.wait()
    for plane in range(8):
        for field in range(4):
            piece = density[plane] if field == 3 else base[field, plane]
            fields[(field * 8 + plane) * 8 : (field * 8 + plane) * 8 + 8, :] = piece
    for block in range(2):
        turned = fields[block * 128 : block * 128 + 128, :].T
        to_below[block * 16 : block * 16 + 16, :] = turned[0:DEEP]
        to_above[block * 16 : block * 16 + 16, :] = turned[128 - DEEP : 128]
    lane = lax.broadcasted_iota(jnp.int32, (1, MARKERS), 1)
    live = jnp.where(lane < counts[0], 1.0, 0.0).astype(F32)
    inside = [(cells[k : k + 1, :] & (7, 7, 127)[k]).astype(F32) for k in range(3)]
    data = inside + [offsets[k : k + 1, :] for k in range(3)] + [live, stiffness[0:1, :]]
    data += [target[k : k + 1, :] for k in range(3)]
    for k, row in enumerate(data):
        own[2 * k : 2 * k + 1, :] = row[:, 0:128]
        own[2 * k + 1 : 2 * k + 2, :] = row[:, 128:256]
    own[22:24, :] = jnp.zeros((2, 128), F32)
    table = jnp.concatenate(data + [jnp.zeros((5, MARKERS), F32)], axis=0)
    table_high = table.astype(BF16)
    rest = table - table_high.astype(F32)
    table_mid = rest.astype(BF16)
    table_low = (rest - table_mid.astype(F32)).astype(BF16)
    split_table = jnp.concatenate([table_high, table_mid, table_low], axis=0)
    upper = jnp.where(inside[2] >= 128.0 - REACH, live, 0.0)
    lower = jnp.where(inside[2] < 1.0 * REACH, live, 0.0)
    flags = jnp.concatenate([upper, lower, jnp.zeros((14, MARKERS), F32)], axis=0).astype(BF16)
    earlier = lax.broadcasted_iota(jnp.int32, (MARKERS, MARKERS), 0) < lax.broadcasted_iota(
        jnp.int32, (MARKERS, MARKERS), 1
    )
    ranks = plain_dot(flags, jnp.where(earlier, 1.0, 0.0).astype(BF16)).astype(jnp.int32)
    slot = lax.broadcasted_iota(jnp.int32, (512, MARKERS), 0)
    goal = jnp.where(upper > 0.0, ranks[0:1, :], jnp.where(lower > 0.0, ranks[1:2, :], 1024))
    goal = ((goal >> 6) << 7) + (goal & 63) + jnp.where(lower > 0.0, 64, 0)
    moved = transposed_dot(split_table, jnp.where(slot == goal, 1.0, 0.0).astype(BF16))
    moved = (moved[0:16] + moved[16:32]) + moved[32:48]
    first_half = lax.broadcasted_iota(jnp.int32, (1, 128), 1) < 64
    for flag, out, shift, mine in ((upper, to_above, -128.0, first_half), (lower, to_below, 128.0, ~first_half)):
        number = jnp.broadcast_to(jnp.sum(flag, axis=1, keepdims=True), (1, 128))
        for block in range(4):
            columns = slice(block * 128, block * 128 + 128)
            for k in range(11):
                row = moved[k : k + 1, columns]
                if k == 2:
                    row = row + shift * moved[6:7, columns]
                out[32 + 4 * k + block : 33 + 4 * k + block, :] = jnp.where(mine, row, 0.0)
            out[76 + block : 77 + block, :] = jnp.where(mine, number, 0.0)
    order = odd_is_below()
    to_odd[...] = jnp.where(order, to_below[...], to_above[...])
    to_even[...] = jnp.where(order, to_above[...], to_below[...])


def deepen_z_kernel(fields, own, odd, even, wide, marks, aux, to_apart, to_near, upward, downward, below, above):
    order = odd_is_below()
    below[...] = jnp.where(order, odd[...], even[...])
    above[...] = jnp.where(order, even[...], odd[...])
    lane = lax.broadcasted_iota(jnp.int32, (128, 128), 1)
    packed = jnp.zeros((64, 128), F32)
    lane64 = lax.broadcasted_iota(jnp.int32, (64, 128), 1)
    for block in range(2):
        edge = jnp.concatenate(
            [below[block * 16 : block * 16 + 16, :], above[block * 16 : block * 16 + 16, :], jnp.zeros((96, 128), F32)],
            axis=0,
        ).T
        turned = pltpu.roll(fields[block * 128 : block * 128 + 128, :], DEEP, 1)
        wide[block * 128 : block * 128 + 128, :] = jnp.where(lane < DEEP, edge, turned)
        beyond = jnp.where(lane < DEEP, turned, edge)
        for half in range(2):
            field = 2 * block + half
            piece = beyond[half * 64 : half * 64 + 64]
            piece = pltpu.roll(piece, 32 * field, 1) if field else piece
            packed = jnp.where((lane64 >= 32 * field) & (lane64 < 32 * field + 32), piece, packed)
    wide[256:320, :] = packed
    for at in range(24):
        upward[at : at + 1, :] = wide[at * 8 + 7 : at * 8 + 8, :]
        downward[at * 2 : at * 2 + 2, :] = wide[at * 8 : at * 8 + 2, :]
    for at in range(16):
        row = 192 + at * 8
        upward[24 + at * 2 : 26 + at * 2, :] = wide[row + 6 : row + 8, :]
        downward[48 + at * 3 : 51 + at * 3, :] = wide[row : row + 3, :]
    halo = below[32:80, :] + above[32:80, :]
    marks[0:12, :] = own[0:12, :]
    marks[12:36, :] = halo[0:24]
    marks[36:40, :] = jnp.broadcast_to(halo[44:45], (4, 128))
    upward[56:96, :] = marks[...]
    downward[96:136, :] = marks[...]
    upward[96:136, :] = jnp.zeros((40, 128), F32)
    order = apart_is_below()
    to_apart[...] = jnp.where(order, downward[...], upward[...])
    to_near[...] = jnp.where(order, upward[...], downward[...])
    aux[...] = jnp.zeros((72, 128), F32)
    for kind in range(3):
        for c in range(3):
            k = 6 + kind if kind < 2 else 8 + c
            aux[24 * kind + 2 * c : 24 * kind + 2 * c + 2, :] = own[2 * k : 2 * k + 2, :]
            for block in range(4):
                row = 24 * kind + 8 + 3 * block + c
                aux[row : row + 1, :] = halo[4 * k + block : 4 * k + block + 1]


def deepen_y_kernel(wide, marks, apart, near, deep, three, upward, downward, below, above):
    order = apart_is_below()
    below[...] = jnp.where(order, apart[...], near[...])
    above[...] = jnp.where(order, near[...], apart[...])
    for at in range(40):
        row = at * YPAD
        deep[row + 2 : row + 10, :] = wide[at * 8 : at * 8 + 8, :]
        if at < 24:
            deep[row : row + 1, :] = jnp.ones((1, 128), F32)
            deep[row + 1 : row + 2, :] = below[at : at + 1, :]
            deep[row + 10 : row + 12, :] = above[at * 2 : at * 2 + 2, :]
            deep[row + 12 : row + 16, :] = jnp.ones((4, 128), F32)
        else:
            near, far = 24 + (at - 24) * 2, 48 + (at - 24) * 3
            deep[row : row + 2, :] = below[near : near + 2, :]
            deep[row + 10 : row + 13, :] = above[far : far + 3, :]
            deep[row + 13 : row + 16, :] = jnp.ones((3, 128), F32)
    for c in range(3):
        upward[c * 13 : c * 13 + 13, :] = deep[c * 128 + 112 : c * 128 + 125, :]
        for k in range(2):
            row = c * 128 + k * YPAD
            downward[c * 26 + k * 13 : c * 26 + k * 13 + 13, :] = deep[row : row + 13, :]
    for at in range(2):
        row = (3 + at) * 128
        for k in range(3):
            if k < 2:
                upward[39 + at * 26 + k * 13 : 52 + at * 26 + k * 13, :] = deep[row + 96 + k * 16 : row + 109 + k * 16, :]
            downward[78 + at * 39 + k * 13 : 91 + at * 39 + k * 13, :] = deep[row + k * 16 : row + k * 16 + 13, :]
    three[0:40, :] = marks[...]
    three[40:80, :] = jnp.where(order, below[56:96, :], above[96:136, :])
    three[80:120, :] = jnp.where(order, above[96:136, :], below[56:96, :])
    upward[96:216, :] = three[...]
    downward[160:280, :] = three[...]


def blocks_used(refs):
    most = jnp.max(jnp.concatenate([ref[first + 36 + 40 * part : first + 37 + 40 * part, :] for ref, first in refs for part in range(3)], axis=0))
    return (most.astype(jnp.int32) + 63) >> 6


def trips(used):
    return jnp.max(used[0:1, :])


def fill_tables(ref, first, along_x, used, plane_weights, z_high, z_low):
    apart = jnp.where(apart_is_below(), -8.0, 8.0).astype(F32)

    def fill(read, along_y, place):
        fractions = jnp.concatenate([read(3), read(4), read(5), jnp.zeros((5, 128), F32)], axis=0)
        weights = delta_weights(fractions)
        plane_weights[0:16, place] = delta_rows(16, read(0) + (along_x + 2.0), weights, 0)
        plane_weights[16:32, place] = delta_rows(16, read(1) + (along_y + 2.0), weights, 1)
        high, rest = halves(delta_rows(160, read(2) + 16.0, weights, 2))
        z_high[0:160, place] = high
        z_low[0:160, place] = rest

    for part, along_y in enumerate((0.0, apart, -apart)):
        top = first + 40 * part
        for half in range(2):
            column = part * 256 + half * 128
            fill(lambda k: ref[top + 2 * k + half : top + 2 * k + half + 1, :], along_y, slice(column, column + 128))
        column = FIRST + part * 128
        fill(lambda k: ref[top + 12 + 4 * k : top + 13 + 4 * k, :], along_y, slice(column, column + 128))

    def further(block, carry):
        for part, along_y in enumerate((0.0, apart, -apart)):
            top = first + 40 * part + 12 + block
            column = pl.multiple_of(STATIC + (block - 1) * 384 + part * 128, 128)
            fill(lambda k: ref[pl.ds(top + 4 * k, 1), :], along_y, pl.ds(column, 128))
        return carry

    lax.fori_loop(1, used, further, 0)
    z_high[160:256, :] = jnp.zeros((96, COLS), BF16)
    z_low[160:256, :] = jnp.zeros((96, COLS), BF16)


def own_tables_kernel(three, plane_weights, z_high, z_low, used):
    count = blocks_used([(three, 0)])
    used[...] = jnp.full((8, 128), count, jnp.int32)
    fill_tables(three, 0, 0.0, count, plane_weights, z_high, z_low)


def side_tables_kernel(below, above, b_weights, b_high, b_low, a_weights, a_high, a_low, used):
    count = blocks_used([(below, 96), (above, 160)])
    used[...] = jnp.full((8, 128), count, jnp.int32)
    fill_tables(below, 96, -8.0, count, b_weights, b_high, b_low)
    fill_tables(above, 160, 8.0, count, a_weights, a_high, a_low)


def interpolate(velocity_high, velocity_low, planes, plane_weights, z_high, z_low, used, image):
    def lines(place):
        partial = plain_dot(velocity_high[...], z_high[:, place]) + plain_dot(velocity_low[...], z_high[:, place])
        partial = partial + plain_dot(velocity_high[...], z_low[:, place])
        result = []
        for c in range(3):
            total = None
            for at, plane in enumerate(planes):
                row = (c * len(planes) + at) * YPAD
                term = partial[row : row + YPAD] * plane_weights[plane : plane + 1, place]
                total = term if total is None else total + term
            result.append(jnp.sum(total * plane_weights[16:32, place], axis=0, keepdims=True))
        return result

    image[...] = jnp.zeros((24, 128), F32)
    for c, line in enumerate(lines(slice(0, MARKERS))):
        image[2 * c : 2 * c + 1, :] = line[:, 0:128]
        image[2 * c + 1 : 2 * c + 2, :] = line[:, 128:256]
    for c, line in enumerate(lines(slice(FIRST, FIRST + 128))):
        image[8 + c : 9 + c, :] = line

    def further(block, carry):
        for c, line in enumerate(lines(pl.ds(pl.multiple_of(STATIC + (block - 1) * 384, 128), 128))):
            image[pl.ds(8 + 3 * block + c, 1), :] = line
        return carry

    lax.fori_loop(1, used, further, 0)


def setup_kernel(deep, below, above, plane_weights, z_high, z_low, aux, used, scale, start, velocity_high, velocity_low, image):
    lane = lax.broadcasted_iota(jnp.int32, (YPAD, 128), 1)
    used_rows = lax.broadcasted_iota(jnp.int32, (YPAD, 128), 0) < 13
    for plane in range(PLANES):
        at = plane * YPAD

        def piece(field):
            if plane < 2:
                row = field * 13 if field < 3 else 39 + (field - 3) * 26 + plane * 13
                return jnp.where(used_rows, below[row : row + 16, :], 1.0)
            if plane < 10:
                row = field * 128 + (plane - 2) * 16
                return deep[row : row + 16, :]
            row = field * 26 if field < 3 else 78 + (field - 3) * 39
            row += (plane - 10) * 13
            return jnp.where(used_rows, above[row : row + 16, :], 1.0)

        packed = piece(4)
        scale[at : at + YPAD, 0:128] = lax.rsqrt(piece(3))
        scale[at : at + YPAD, 128:256] = lax.rsqrt(jnp.where(lane < 32, pltpu.roll(packed, 32, 1), 1.0))
        if 1 <= plane <= 11:
            for c in range(3):
                row = c * INNER + at - YPAD
                top, rest = halves(piece(c))
                velocity_high[row : row + YPAD, 0:128] = top
                velocity_low[row : row + YPAD, 0:128] = rest
                beyond = pltpu.roll(packed, 128 - 32 * c, 1) if c else packed
                top, rest = halves(jnp.where(lane < 32, beyond, 0.0))
                velocity_high[row : row + YPAD, 128:256] = top
                velocity_low[row : row + YPAD, 128:256] = rest
    interpolate(velocity_high, velocity_low, range(1, 12), plane_weights, z_high, z_low, trips(used), image)
    start[...] = aux[0:24, :] * (aux[48:72, :] - image[...])


def fill_tile(rows, planes, plane_weights, weight, left_high, left_low, place):
    along_y = plane_weights[16:32, weight]
    vector = [row * along_y for row in rows]
    for at, plane in enumerate(planes):
        along_x = plane_weights[plane : plane + 1, weight]
        for c in range(3):
            top, rest = halves(vector[c] * along_x)
            row = (c * len(planes) + at) * YPAD
            left_high[row : row + YPAD, place] = top
            left_low[row : row + YPAD, place] = rest


def spread_columns(left_high, left_low, z_high, z_low, left, right):
    total = transposed_dot(left_high[:, left], z_high[:, right]) + transposed_dot(left_low[:, left], z_high[:, right])
    return total + transposed_dot(left_high[:, left], z_low[:, right])


def spread_group(refs, planes, plane_weights, z_high, z_low, used, left_high, left_low, total, begun=None, part0=0):
    count = len(refs)
    for at, (ref, first) in enumerate(refs):
        part = part0 + at
        for half in range(2):
            place = slice(at * 256 + half * 128, at * 256 + half * 128 + 128)
            weight = slice(part * 256 + half * 128, part * 256 + half * 128 + 128)
            rows = [ref[first + 2 * c + half : first + 2 * c + half + 1, :] for c in range(3)]
            fill_tile(rows, planes, plane_weights, weight, left_high, left_low, place)
        place = slice(count * 256 + at * 128, count * 256 + at * 128 + 128)
        weight = slice(FIRST + part * 128, FIRST + part * 128 + 128)
        rows = [ref[first + 8 + c : first + 9 + c, :] for c in range(3)]
        fill_tile(rows, planes, plane_weights, weight, left_high, left_low, place)
    value = spread_columns(
        left_high, left_low, z_high, z_low, slice(0, count * 256), slice(part0 * 256, (part0 + count) * 256)
    )
    value = value + spread_columns(
        left_high, left_low, z_high, z_low, slice(count * 256, count * 384),
        slice(FIRST + part0 * 128, FIRST + (part0 + count) * 128),
    )
    total[...] = value if begun is None else value + begun[...]

    def further(block, carry):
        for at, (ref, first) in enumerate(refs):
            column = pl.multiple_of(STATIC + (block - 1) * 384 + (part0 + at) * 128, 128)
            rows = [ref[pl.ds(first + 8 + 3 * block + c, 1), :] for c in range(3)]
            place = slice(at * 128, at * 128 + 128)
            fill_tile(rows, planes, plane_weights, pl.ds(column, 128), left_high, left_low, place)
        right = pl.ds(pl.multiple_of(STATIC + (block - 1) * 384 + part0 * 128, 128), count * 128)
        total[...] += spread_columns(left_high, left_low, z_high, z_low, slice(0, count * 128), right)
        return carry

    lax.fori_loop(1, used, further, 0)


def respond(moved, planes, outs, scale, velocity_high, velocity_low):
    axial, diagonal = 1.0 / 6.0, 1.0 / 12.0
    up_y = lambda a: pltpu.roll(a, 1, 0)
    down_y = lambda a: pltpu.roll(a, YPAD - 1, 0)
    up_z = lambda a: pltpu.roll(a, 1, 1)
    down_z = lambda a: pltpu.roll(a, LANES - 1, 1)
    onward, back, still = {}, {}, {}
    for at, plane in enumerate(planes):
        factor = scale[plane * YPAD : plane * YPAD + YPAD, :]
        rows = [(c * len(planes) + at) * YPAD for c in range(3)]
        gx, gy, gz = (moved[row : row + YPAD, :] * factor for row in rows)
        hx, hy, hz = gx * diagonal, gy * diagonal, gz * diagonal
        sum_xy, dif_xy = hx + hy, hx - hy
        zx_up, zy_up, zz_up = up_z(hx), up_z(hy), up_z(hz)
        zx_dn, zy_dn, zz_dn = down_z(hx), down_z(hy), down_z(hz)
        xz_sum_up, xz_sum_dn, xz_dif_up, xz_dif_dn = zx_up + zz_up, zx_dn + zz_dn, zx_up - zz_up, zx_dn - zz_dn
        xy_sum_up, xy_sum_dn, xy_dif_up, xy_dif_dn = up_y(sum_xy), down_y(sum_xy), up_y(dif_xy), down_y(dif_xy)
        ax = gx * axial
        onward[plane] = (
            ax + ((xy_sum_up + xy_dif_dn) + (xz_sum_up + xz_dif_dn)),
            xy_sum_up - xy_dif_dn,
            xz_sum_up - xz_dif_dn,
        )
        back[plane] = (
            ax + ((xy_sum_dn + xy_dif_up) + (xz_sum_dn + xz_dif_up)),
            xy_sum_dn - xy_dif_up,
            xz_sum_dn - xz_dif_up,
        )
        yz_same = up_y(zy_up + zz_up)
        yz_same_dn = down_y(zy_dn + zz_dn)
        yz_cross = up_y(zy_dn - zz_dn)
        yz_cross_dn = down_y(zy_up - zz_up)
        same, cross = yz_same + yz_same_dn, yz_cross + yz_cross_dn
        still[plane] = (
            gx,
            gy + ((up_y(hy) + down_y(hy)) * 2.0 + (same + cross)),
            gz + ((zz_up + zz_dn) * 2.0 + (same - cross)),
        )
        for place, out in enumerate(outs):
            if min(out + 1, planes[-1]) != plane:
                continue
            factor = scale[out * YPAD : out * YPAD + YPAD, :] * 0.5
            for c in range(3):
                parts = [group[at][c] for group, at in ((onward, out - 1), (still, out), (back, out + 1)) if at in group]
                total = parts[0]
                for part in parts[1:]:
                    total = total + part
                top, rest = halves(total * factor)
                row = (c * len(outs) + place) * YPAD
                velocity_high[row : row + YPAD, :] = top
                velocity_low[row : row + YPAD, :] = rest


def own_spread(own, plane_weights, z_high, z_low, used, total, left_high, left_low):
    spread_group([(own, 0)], range(1, 12), plane_weights, z_high, z_low, trips(used), left_high, left_low, total)


def own_image(
    begun, apart, near, plane_weights, z_high, z_low, used, scale, result, left_high, left_low, moved, velocity_high,
    velocity_low,
):
    refs = [(apart, 0), (near, 0)]
    planes = range(1, 12)
    count = trips(used)
    spread_group(refs, planes, plane_weights, z_high, z_low, count, left_high, left_low, moved, begun, 1)
    respond(moved, planes, planes, scale, velocity_high, velocity_low)
    interpolate(velocity_high, velocity_low, planes, plane_weights, z_high, z_low, count, result)


def side_image(
    below, begun, three, own_tables, own_used, side_tables, used, scale, left_high, left_low, moved, velocity_high,
    velocity_low, image,
):
    planes, outs = (range(0, 4), range(1, 5)) if below else (range(9, 13), range(8, 12))
    refs = [(three, 24 * part) for part in range(3)]
    spread_group(refs, planes, *side_tables, trips(used), left_high, left_low, moved)
    respond(moved, planes, outs, scale, velocity_high, velocity_low)
    interpolate(velocity_high, velocity_low, outs, *own_tables, trips(own_used), image)
    return begun[...] + image[...]


def below_kernel(begun, three, w, h, l, own_used, sw, sh, sl, used, scale, result, *scratch):
    result[...] = side_image(True, begun, three, (w, h, l), own_used, (sw, sh, sl), used, scale, *scratch)


def above_image(begun, three, w, h, l, own_used, sw, sh, sl, used, scale, aux, vector, *scratch):
    image = side_image(False, begun, three, (w, h, l), own_used, (sw, sh, sl), used, scale, *scratch)
    return aux[0:24, :] * (image + aux[24:48, :] * vector[...])


def above_kernel(begun, three, w, h, l, own_used, sw, sh, sl, used, scale, aux, vector, result, *scratch):
    result[...] = above_image(begun, three, w, h, l, own_used, sw, sh, sl, used, scale, aux, vector, *scratch)


def two_sum(a, b):
    total = a + b
    part = total - a
    return total, (a - (total - part)) + (b - part)


def fast_two_sum(a, b):
    total = a + b
    return total, b - (total - a)


def split(a):
    scaled = a * 4097.0
    high = scaled - (scaled - a)
    return high, a - high


def two_product(a, b):
    product = a * b
    a_high, a_low = split(a)
    b_high, b_low = split(b)
    return product, ((a_high * b_high - product) + a_high * b_low + a_low * b_high) + a_low * b_low


def pair_add(a, b):
    head, tail = two_sum(a[0], b[0])
    return fast_two_sum(head, tail + (a[1] + b[1]))


def pair_negative(a):
    return (-a[0], -a[1])


def pair_multiply(a, b):
    head, tail = two_product(a[0], b[0])
    return fast_two_sum(head, tail + (a[0] * b[1] + a[1] * b[0]))


def pair_divide(a, b):
    first = a[0] / b[0]
    rest = pair_add(a, pair_negative(pair_multiply((first, jnp.zeros_like(first)), b)))
    return fast_two_sum(first, rest[0] / b[0])


ENTRIES = ((0, 0), (0, 1), (0, 2), (0, 3), (1, 1), (1, 2), (1, 3), (2, 2), (2, 3))


def gram_lanes(vectors, entries, packed):
    lane = lax.broadcasted_iota(jnp.int32, (8, 128), 1)
    for at, (i, j) in enumerate(ENTRIES):
        if (i, j) not in entries:
            continue
        value = two_product(vectors[i], vectors[j])
        for axis, steps in ((0, (4, 2, 1)), (1, (64, 32, 16, 8, 4, 2, 1))):
            for step in steps:
                value = pair_add(value, (pltpu.roll(value[0], step, axis), pltpu.roll(value[1], step, axis)))
        packed = jnp.where(lane == at, value[0], jnp.where(lane == 16 + at, value[1], packed))
    return packed


EARLY = tuple(entry for entry in ENTRIES if entry[1] < 3)
LATE = tuple(entry for entry in ENTRIES if entry[1] == 3)


def own_spread_last(own, w, h, l, used, first, second, total, early, *scratch):
    own_spread(own, w, h, l, used, total, *scratch)
    early[...] = gram_lanes([first[0:8, :], second[0:8, :], own[0:8, :]], EARLY, jnp.zeros((8, 128), F32))


def last_kernel(
    begun, three, w, h, l, own_used, sw, sh, sl, used, scale, aux, third, first, second, early, sums, *scratch
):
    fourth = above_image(begun, three, w, h, l, own_used, sw, sh, sl, used, scale, aux, third, *scratch)
    vectors = [first[0:8, :], second[0:8, :], third[0:8, :], fourth[0:8]]
    packed = gram_lanes(vectors, LATE, early[...])
    for block in range(sums.shape[0] // 8):
        sums[block * 8 : block * 8 + 8, :] = packed


def finish_kernel(gathered, first, second, third, forces):
    a = gathered[...]
    count = a.shape[0]
    value = (a, pltpu.roll(a, 112, 1))
    while count > 8:
        count //= 2
        value = pair_add(
            (value[0][0:count], value[1][0:count]), (value[0][count : 2 * count], value[1][count : 2 * count])
        )
    for step in (4, 2, 1):
        value = pair_add(value, (pltpu.roll(value[0], step, 0), pltpu.roll(value[1], step, 0)))
    lane = lax.broadcasted_iota(jnp.int32, (8, 128), 1)
    gram = {}
    for at, (i, j) in enumerate(ENTRIES):
        entry = tuple(
            jnp.broadcast_to(jnp.sum(jnp.where(lane == at, v, 0.0), axis=1, keepdims=True), (8, 128)) for v in value
        )
        gram[i, j] = entry
        gram[j, i] = entry
    add, times = pair_add, pair_multiply
    minus = lambda a, b: pair_add(a, pair_negative(b))

    def form(left, right, shift):
        total = None
        for i, a in enumerate(left):
            for j, b in enumerate(right):
                term = times(times(a, b), gram[i, j + shift])
                total = term if total is None else add(total, term)
        return total

    one = (jnp.ones((8, 128), F32), jnp.zeros((8, 128), F32))
    alpha0 = pair_divide(gram[0, 0], gram[0, 1])
    residual = [one, pair_negative(alpha0)]
    norm1 = form(residual, residual, 0)
    beta0 = pair_divide(norm1, gram[0, 0])
    along1 = [add(one, beta0), pair_negative(alpha0)]
    alpha1 = pair_divide(norm1, form(along1, along1, 1))
    residual = [one, minus(residual[1], times(alpha1, along1[0])), pair_negative(times(alpha1, along1[1]))]
    norm2 = form(residual, residual, 0)
    beta1 = pair_divide(norm2, norm1)
    along2 = [add(one, times(beta1, along1[0])), add(residual[1], times(beta1, along1[1])), residual[2]]
    alpha2 = pair_divide(norm2, form(along2, along2, 1))
    weight0 = add(alpha0, add(times(alpha1, along1[0]), times(alpha2, along2[0])))
    weight1 = add(times(alpha1, along1[1]), times(alpha2, along2[1]))
    weight2 = times(alpha2, along2[2])
    total = weight0[0] * first[0:8, :] + (weight1[0] * second[0:8, :] + weight2[0] * third[0:8, :])
    for c in range(3):
        forces[c : c + 1, 0:128] = total[2 * c : 2 * c + 1, :]
        forces[c : c + 1, 128:256] = total[2 * c + 1 : 2 * c + 2, :]


def call(kernel, name, outs, *operands, memory=None, scratch=()):
    spec = lambda space: pl.BlockSpec(memory_space=space)
    memory = memory or [pltpu.VMEM] * len(operands)
    return pl.pallas_call(
        kernel,
        name=name,
        out_shape=[jax.ShapeDtypeStruct(shape, kind) for shape, kind in outs],
        in_specs=[spec(space) for space in memory],
        out_specs=[spec(pltpu.VMEM)] * len(outs),
        scratch_shapes=list(scratch),
        compiler_params=PARAMS,
    )(*operands)


def body(density, base_velocity, cells, offsets, target, stiffness, counts):
    rows = lambda n: ((n, 128), F32)
    vmem, smem, hbm = pltpu.VMEM, pltpu.SMEM, pltpu.HBM
    table_shapes = [((32, COLS), F32), ((256, COLS), BF16), ((256, COLS), BF16)]
    used_shape = [((8, 128), jnp.int32)]
    arguments = (density, base_velocity, cells, offsets, target, stiffness.reshape(1, MARKERS))
    fields, own, to_odd, to_even = call(
        pack_kernel, "pack", [rows(256), rows(24), rows(80), rows(80)],
        *(pltpu.with_memory_space_constraint(a, hbm) for a in arguments), counts,
        memory=[hbm] * 6 + [smem],
        scratch=[
            vmem((8, 8, 128), F32), vmem((3, 8, 8, 128), F32), vmem((3, MARKERS), jnp.int32),
            vmem((3, MARKERS), F32), vmem((3, MARKERS), F32), vmem((1, MARKERS), F32),
            pltpu.SemaphoreType.DMA((6,)), vmem((80, 128), F32), vmem((80, 128), F32),
        ],
    )
    odd, even = swapped_z(to_odd, to_even)
    wide, marks, aux, to_apart, to_near = call(
        deepen_z_kernel, "deepen_z", [rows(320), rows(40), rows(72), rows(136), rows(136)], fields, own, odd, even,
        scratch=[vmem((136, 128), F32)] * 2 + [vmem((80, 128), F32)] * 2,
    )
    apart, near = swapped_y(to_apart, to_near)
    deep, three, upward, downward = call(
        deepen_y_kernel, "deepen_y", [rows(640), rows(120), rows(216), rows(280)], wide, marks, apart, near,
        scratch=[vmem((136, 128), F32)] * 2,
    )
    below, above = shifted(upward, "gx", 1), shifted(downward, "gx", -1)
    own_tables = call(
        own_tables_kernel, "own_tables", table_shapes + used_shape, three
    )
    side_tables = call(
        side_tables_kernel, "side_tables", table_shapes * 2 + used_shape, below, above
    )
    velocity_scratch = [vmem((3 * INNER, LANES), BF16)] * 2
    image_scratch = vmem((24, 128), F32)
    scale, start = call(
        setup_kernel, "setup", [((ROWS, LANES), F32), rows(24)], deep, below, above, *own_tables[0:3], aux, own_tables[3],
        scratch=velocity_scratch + [image_scratch],
    )

    def image_of(last, vector, *others):
        apart, near = swapped_y(vector, vector)
        begun = call(
            own_spread_last if last else own_spread, "own_spread",
            [((3 * INNER, LANES), F32)] + ([rows(8)] if last else []), vector, *own_tables, *others,
            scratch=[vmem((3 * INNER, 384), BF16)] * 2,
        )
        held = list(begun) + (list(side_tables) if vector is start else [])
        three = lax.optimization_barrier((jnp.concatenate([vector, apart, near], axis=0), *held))[0]
        below_three, above_three = shifted(three, "gx", 1), shifted(three, "gx", -1)
        (own_part,) = call(
            own_image, "own_image", [rows(24)], begun[0], apart, near, *own_tables, scale,
            scratch=[vmem((3 * INNER, 768), BF16)] * 2 + [vmem((3 * INNER, LANES), F32)] + velocity_scratch,
        )
        side_scratch = [vmem((192, STATIC), BF16)] * 2 + [vmem((192, LANES), F32)]
        side_scratch += [vmem((192, LANES), BF16)] * 2 + [image_scratch]
        (part,) = call(
            below_kernel, "below", [rows(24)], own_part, below_three, *own_tables, *side_tables[0:3], side_tables[6], scale,
            scratch=side_scratch,
        )
        (result,) = call(
            last_kernel if last else above_kernel, "above", [rows(256 if last else 24)],
            part, above_three, *own_tables, *side_tables[3:7], scale, aux, vector, *others, *begun[1:],
            scratch=side_scratch,
        )
        return result

    second = image_of(False, start)
    third = image_of(False, second)
    sums = image_of(True, third, start, second)
    gathered = lax.all_to_all(sums, GX_GY_GZ, 0, 0, tiled=True)
    (forces,) = call(finish_kernel, "finish", [((3, MARKERS), F32)], gathered, start, second, third)
    return forces


def solution(mesh):
    finer = Mesh(
        mesh.devices.reshape(mesh.shape["gx"], 4, 2, mesh.shape["gz"]), ("gx", "gy_0", "gy_1", "gz")
    )
    return jax.shard_map(
        body,
        mesh=finer,
        in_specs=(
            P("gx", GY, "gz"),
            P(None, "gx", GY, "gz"),
            P(None, GX_GY_GZ),
            P(None, GX_GY_GZ),
            P(None, GX_GY_GZ),
            P(GX_GY_GZ),
            P(GX_GY_GZ),
        ),
        out_specs=P(None, GX_GY_GZ),
        check_vma=False,
    )
```

```python
import functools

import jax
import jax.numpy as jnp
from jax import lax
from jax.experimental import pallas as pl
from jax.experimental.pallas import tpu as pltpu
from jax.sharding import Mesh
from jax.sharding import PartitionSpec as P

GY = ("gy_0", "gy_1")
GX_GY_GZ = ("gx", "gy_0", "gy_1", "gz")

PLANES = 13
YPAD = 16
ROWS = PLANES * YPAD
INNER = 11 * YPAD
LANES = 256
DEEP = 16
REACH = 12
MARKERS = 256
FIRST = 3 * MARKERS
STATIC = FIRST + 3 * 128
COLS = STATIC + 3 * 384
F32 = jnp.float32
BF16 = jnp.bfloat16
PARAMS = pltpu.CompilerParams(vmem_limit_bytes=12 * 1024 * 1024)


def shifted(shard, axis, by):
    length = lax.axis_size(axis)
    return lax.ppermute(shard, axis, [(i, (i + by) % length) for i in range(length)])


def swapped_y(to_apart, to_near):
    length = lax.axis_size(GY)
    apart = lax.ppermute(to_apart, GY, [(i, (i + 1 if i % 2 else i - 1) % length) for i in range(length)])
    return apart, lax.ppermute(to_near, GY, [(i, i ^ 1) for i in range(length)])


def swapped_z(to_odd, to_even):
    length = lax.axis_size("gz")
    odd = lax.ppermute(to_odd, "gz", [(i, (i + 1 if i % 2 else i - 1) % length) for i in range(length)])
    return odd, lax.ppermute(to_even, "gz", [(i, i ^ 1) for i in range(length)])


def odd_is_below():
    return lax.rem(lax.axis_index("gz"), 2) == 0


def apart_is_below():
    return lax.axis_index("gy_1") == 0


def halves(value):
    high = value.astype(BF16)
    return high, (value - high.astype(F32)).astype(BF16)


def transposed_dot(left, right):
    return lax.dot_general(left, right, (((1,), (1,)), ((), ())), preferred_element_type=F32)


def plain_dot(left, right):
    return lax.dot_general(left, right, (((1,), (0,)), ((), ())), preferred_element_type=F32)


def delta_weights(fraction):
    def inner(radius):
        return (3.0 - 2.0 * radius + jnp.sqrt(jnp.maximum(1.0 + 4.0 * radius - 4.0 * radius * radius, 0.0))) / 8.0

    def outer(radius):
        return (5.0 - 2.0 * radius - jnp.sqrt(jnp.maximum(-7.0 + 12.0 * radius - 4.0 * radius * radius, 0.0))) / 8.0

    return [outer(1.0 + fraction), inner(fraction), inner(1.0 - fraction), outer(2.0 - fraction)]


def delta_rows(extent, cell, weights, at):
    step = lax.broadcasted_iota(jnp.int32, (extent, cell.shape[1]), 0).astype(F32) - cell
    value = jnp.zeros_like(step)
    for place, weight in zip((-1.0, 0.0, 1.0, 2.0), weights):
        value = jnp.where(step == place, weight[at : at + 1], value)
    return value


def pack_kernel(
    density_in, base_in, cells_in, offsets_in, target_in, stiffness_in, counts, fields, own, to_odd, to_even,
    density, base, cells, offsets, target, stiffness, arrived, to_above, to_below,
):
    sources = (density_in, base_in, cells_in, offsets_in, target_in, stiffness_in)
    places = (density, base, cells, offsets, target, stiffness)
    copies = [pltpu.make_async_copy(a, b, arrived.at[i]) for i, (a, b) in enumerate(zip(sources, places))]
    for copy in copies:
        copy.start()
    for copy in copies:
        copy.wait()
    for plane in range(8):
        for field in range(4):
            piece = density[plane] if field == 3 else base[field, plane]
            fields[(field * 8 + plane) * 8 : (field * 8 + plane) * 8 + 8, :] = piece
    for block in range(2):
        turned = fields[block * 128 : block * 128 + 128, :].T
        to_below[block * 16 : block * 16 + 16, :] = turned[0:DEEP]
        to_above[block * 16 : block * 16 + 16, :] = turned[128 - DEEP : 128]
    lane = lax.broadcasted_iota(jnp.int32, (1, MARKERS), 1)
    live = jnp.where(lane < counts[0], 1.0, 0.0).astype(F32)
    inside = [(cells[k : k + 1, :] & (7, 7, 127)[k]).astype(F32) for k in range(3)]
    data = inside + [offsets[k : k + 1, :] for k in range(3)] + [live, stiffness[0:1, :]]
    data += [target[k : k + 1, :] for k in range(3)]
    for k, row in enumerate(data):
        own[2 * k : 2 * k + 1, :] = row[:, 0:128]
        own[2 * k + 1 : 2 * k + 2, :] = row[:, 128:256]
    own[22:24, :] = jnp.zeros((2, 128), F32)
    table = jnp.concatenate(data + [jnp.zeros((5, MARKERS), F32)], axis=0)
    table_high = table.astype(BF16)
    rest = table - table_high.astype(F32)
    table_mid = rest.astype(BF16)
    table_low = (rest - table_mid.astype(F32)).astype(BF16)
    split_table = jnp.concatenate([table_high, table_mid, table_low], axis=0)
    upper = jnp.where(inside[2] >= 128.0 - REACH, live, 0.0)
    lower = jnp.where(inside[2] < 1.0 * REACH, live, 0.0)
    flags = jnp.concatenate([upper, lower, jnp.zeros((14, MARKERS), F32)], axis=0).astype(BF16)
    earlier = lax.broadcasted_iota(jnp.int32, (MARKERS, MARKERS), 0) < lax.broadcasted_iota(
        jnp.int32, (MARKERS, MARKERS), 1
    )
    ranks = plain_dot(flags, jnp.where(earlier, 1.0, 0.0).astype(BF16)).astype(jnp.int32)
    slot = lax.broadcasted_iota(jnp.int32, (512, MARKERS), 0)
    goal = jnp.where(upper > 0.0, ranks[0:1, :], jnp.where(lower > 0.0, ranks[1:2, :], 1024))
    goal = ((goal >> 6) << 7) + (goal & 63) + jnp.where(lower > 0.0, 64, 0)
    moved = transposed_dot(split_table, jnp.where(slot == goal, 1.0, 0.0).astype(BF16))
    moved = (moved[0:16] + moved[16:32]) + moved[32:48]
    first_half = lax.broadcasted_iota(jnp.int32, (1, 128), 1) < 64
    for flag, out, shift, mine in ((upper, to_above, -128.0, first_half), (lower, to_below, 128.0, ~first_half)):
        number = jnp.broadcast_to(jnp.sum(flag, axis=1, keepdims=True), (1, 128))
        for block in range(4):
            columns = slice(block * 128, block * 128 + 128)
            for k in range(11):
                row = moved[k : k + 1, columns]
                if k == 2:
                    row = row + shift * moved[6:7, columns]
                out[32 + 4 * k + block : 33 + 4 * k + block, :] = jnp.where(mine, row, 0.0)
            out[76 + block : 77 + block, :] = jnp.where(mine, number, 0.0)
    order = odd_is_below()
    to_odd[...] = jnp.where(order, to_below[...], to_above[...])
    to_even[...] = jnp.where(order, to_above[...], to_below[...])


def deepen_z_kernel(fields, own, odd, even, wide, marks, aux, to_apart, to_near, upward, downward, below, above):
    order = odd_is_below()
    below[...] = jnp.where(order, odd[...], even[...])
    above[...] = jnp.where(order, even[...], odd[...])
    lane = lax.broadcasted_iota(jnp.int32, (128, 128), 1)
    packed = jnp.zeros((64, 128), F32)
    lane64 = lax.broadcasted_iota(jnp.int32, (64, 128), 1)
    for block in range(2):
        edge = jnp.concatenate(
            [below[block * 16 : block * 16 + 16, :], above[block * 16 : block * 16 + 16, :], jnp.zeros((96, 128), F32)],
            axis=0,
        ).T
        turned = pltpu.roll(fields[block * 128 : block * 128 + 128, :], DEEP, 1)
        wide[block * 128 : block * 128 + 128, :] = jnp.where(lane < DEEP, edge, turned)
        beyond = jnp.where(lane < DEEP, turned, edge)
        for half in range(2):
            field = 2 * block + half
            piece = beyond[half * 64 : half * 64 + 64]
            piece = pltpu.roll(piece, 32 * field, 1) if field else piece
            packed = jnp.where((lane64 >= 32 * field) & (lane64 < 32 * field + 32), piece, packed)
    wide[256:320, :] = packed
    for at in range(24):
        upward[at : at + 1, :] = wide[at * 8 + 7 : at * 8 + 8, :]
        downward[at * 2 : at * 2 + 2, :] = wide[at * 8 : at * 8 + 2, :]
    for at in range(16):
        row = 192 + at * 8
        upward[24 + at * 2 : 26 + at * 2, :] = wide[row + 6 : row + 8, :]
        downward[48 + at * 3 : 51 + at * 3, :] = wide[row : row + 3, :]
    halo = below[32:80, :] + above[32:80, :]
    marks[0:12, :] = own[0:12, :]
    marks[12:36, :] = halo[0:24]
    marks[36:40, :] = jnp.broadcast_to(halo[44:45], (4, 128))
    upward[56:96, :] = marks[...]
    downward[96:136, :] = marks[...]
    upward[96:136, :] = jnp.zeros((40, 128), F32)
    order = apart_is_below()
    to_apart[...] = jnp.where(order, downward[...], upward[...])
    to_near[...] = jnp.where(order, upward[...], downward[...])
    aux[...] = jnp.zeros((72, 128), F32)
    for kind in range(3):
        for c in range(3):
            k = 6 + kind if kind < 2 else 8 + c
            aux[24 * kind + 2 * c : 24 * kind + 2 * c + 2, :] = own[2 * k : 2 * k + 2, :]
            for block in range(4):
                row = 24 * kind + 8 + 3 * block + c
                aux[row : row + 1, :] = halo[4 * k + block : 4 * k + block + 1]


def deepen_y_kernel(wide, marks, apart, near, deep, three, upward, downward, below, above):
    order = apart_is_below()
    below[...] = jnp.where(order, apart[...], near[...])
    above[...] = jnp.where(order, near[...], apart[...])
    for at in range(40):
        row = at * YPAD
        deep[row + 2 : row + 10, :] = wide[at * 8 : at * 8 + 8, :]
        if at < 24:
            deep[row : row + 1, :] = jnp.ones((1, 128), F32)
            deep[row + 1 : row + 2, :] = below[at : at + 1, :]
            deep[row + 10 : row + 12, :] = above[at * 2 : at * 2 + 2, :]
            deep[row + 12 : row + 16, :] = jnp.ones((4, 128), F32)
        else:
            near, far = 24 + (at - 24) * 2, 48 + (at - 24) * 3
            deep[row : row + 2, :] = below[near : near + 2, :]
            deep[row + 10 : row + 13, :] = above[far : far + 3, :]
            deep[row + 13 : row + 16, :] = jnp.ones((3, 128), F32)
    for c in range(3):
        upward[c * 13 : c * 13 + 13, :] = deep[c * 128 + 112 : c * 128 + 125, :]
        for k in range(2):
            row = c * 128 + k * YPAD
            downward[c * 26 + k * 13 : c * 26 + k * 13 + 13, :] = deep[row : row + 13, :]
    for at in range(2):
        row = (3 + at) * 128
        for k in range(3):
            if k < 2:
                upward[39 + at * 26 + k * 13 : 52 + at * 26 + k * 13, :] = deep[row + 96 + k * 16 : row + 109 + k * 16, :]
            downward[78 + at * 39 + k * 13 : 91 + at * 39 + k * 13, :] = deep[row + k * 16 : row + k * 16 + 13, :]
    three[0:40, :] = marks[...]
    three[40:80, :] = jnp.where(order, below[56:96, :], above[96:136, :])
    three[80:120, :] = jnp.where(order, above[96:136, :], below[56:96, :])
    upward[96:216, :] = three[...]
    downward[160:280, :] = three[...]


def blocks_used(refs):
    most = jnp.max(jnp.concatenate([ref[first + 36 + 40 * part : first + 37 + 40 * part, :] for ref, first in refs for part in range(3)], axis=0))
    return (most.astype(jnp.int32) + 63) >> 6


def trips(used):
    return jnp.max(used[0:1, :])


def fill_tables(ref, first, along_x, used, plane_weights, z_high, z_low):
    apart = jnp.where(apart_is_below(), -8.0, 8.0).astype(F32)

    def fill(read, along_y, place):
        fractions = jnp.concatenate([read(3), read(4), read(5), jnp.zeros((5, 128), F32)], axis=0)
        weights = delta_weights(fractions)
        plane_weights[0:16, place] = delta_rows(16, read(0) + (along_x + 2.0), weights, 0)
        plane_weights[16:32, place] = delta_rows(16, read(1) + (along_y + 2.0), weights, 1)
        high, rest = halves(delta_rows(160, read(2) + 16.0, weights, 2))
        z_high[0:160, place] = high
        z_low[0:160, place] = rest

    for part, along_y in enumerate((0.0, apart, -apart)):
        top = first + 40 * part
        for half in range(2):
            column = part * 256 + half * 128
            fill(lambda k: ref[top + 2 * k + half : top + 2 * k + half + 1, :], along_y, slice(column, column + 128))
        column = FIRST + part * 128
        fill(lambda k: ref[top + 12 + 4 * k : top + 13 + 4 * k, :], along_y, slice(column, column + 128))

    def further(block, carry):
        for part, along_y in enumerate((0.0, apart, -apart)):
            top = first + 40 * part + 12 + block
            column = pl.multiple_of(STATIC + (block - 1) * 384 + part * 128, 128)
            fill(lambda k: ref[pl.ds(top + 4 * k, 1), :], along_y, pl.ds(column, 128))
        return carry

    lax.fori_loop(1, used, further, 0)
    z_high[160:256, :] = jnp.zeros((96, COLS), BF16)
    z_low[160:256, :] = jnp.zeros((96, COLS), BF16)


def own_tables_kernel(three, plane_weights, z_high, z_low, used):
    count = blocks_used([(three, 0)])
    used[...] = jnp.full((8, 128), count, jnp.int32)
    fill_tables(three, 0, 0.0, count, plane_weights, z_high, z_low)


def side_tables_kernel(below, above, b_weights, b_high, b_low, a_weights, a_high, a_low, used):
    count = blocks_used([(below, 96), (above, 160)])
    used[...] = jnp.full((8, 128), count, jnp.int32)
    fill_tables(below, 96, -8.0, count, b_weights, b_high, b_low)
    fill_tables(above, 160, 8.0, count, a_weights, a_high, a_low)


def interpolate(velocity_high, velocity_low, planes, plane_weights, z_high, z_low, used, image, halo=True):
    def lines(place):
        partial = plain_dot(velocity_high[...], z_high[:, place]) + plain_dot(velocity_low[...], z_high[:, place])
        partial = partial + plain_dot(velocity_high[...], z_low[:, place])
        result = []
        for c in range(3):
            total = None
            for at, plane in enumerate(planes):
                row = (c * len(planes) + at) * YPAD
                term = partial[row : row + YPAD] * plane_weights[plane : plane + 1, place]
                total = term if total is None else total + term
            result.append(jnp.sum(total * plane_weights[16:32, place], axis=0, keepdims=True))
        return result

    image[...] = jnp.zeros((24, 128), F32)
    for c, line in enumerate(lines(slice(0, MARKERS))):
        image[2 * c : 2 * c + 1, :] = line[:, 0:128]
        image[2 * c + 1 : 2 * c + 2, :] = line[:, 128:256]
    if not halo:
        return
    for c, line in enumerate(lines(slice(FIRST, FIRST + 128))):
        image[8 + c : 9 + c, :] = line

    def further(block, carry):
        for c, line in enumerate(lines(pl.ds(pl.multiple_of(STATIC + (block - 1) * 384, 128), 128))):
            image[pl.ds(8 + 3 * block + c, 1), :] = line
        return carry

    lax.fori_loop(1, used, further, 0)


def setup_kernel(deep, below, above, plane_weights, z_high, z_low, aux, used, scale, start, velocity_high, velocity_low, image):
    lane = lax.broadcasted_iota(jnp.int32, (YPAD, 128), 1)
    used_rows = lax.broadcasted_iota(jnp.int32, (YPAD, 128), 0) < 13
    for plane in range(PLANES):
        at = plane * YPAD

        def piece(field):
            if plane < 2:
                row = field * 13 if field < 3 else 39 + (field - 3) * 26 + plane * 13
                return jnp.where(used_rows, below[row : row + 16, :], 1.0)
            if plane < 10:
                row = field * 128 + (plane - 2) * 16
                return deep[row : row + 16, :]
            row = field * 26 if field < 3 else 78 + (field - 3) * 39
            row += (plane - 10) * 13
            return jnp.where(used_rows, above[row : row + 16, :], 1.0)

        packed = piece(4)
        scale[at : at + YPAD, 0:128] = lax.rsqrt(piece(3))
        scale[at : at + YPAD, 128:256] = lax.rsqrt(jnp.where(lane < 32, pltpu.roll(packed, 32, 1), 1.0))
        if 1 <= plane <= 11:
            for c in range(3):
                row = c * INNER + at - YPAD
                top, rest = halves(piece(c))
                velocity_high[row : row + YPAD, 0:128] = top
                velocity_low[row : row + YPAD, 0:128] = rest
                beyond = pltpu.roll(packed, 128 - 32 * c, 1) if c else packed
                top, rest = halves(jnp.where(lane < 32, beyond, 0.0))
                velocity_high[row : row + YPAD, 128:256] = top
                velocity_low[row : row + YPAD, 128:256] = rest
    interpolate(velocity_high, velocity_low, range(1, 12), plane_weights, z_high, z_low, trips(used), image)
    start[...] = aux[0:24, :] * (aux[48:72, :] - image[...])


def fill_tile(rows, planes, plane_weights, weight, left_high, left_low, place):
    along_y = plane_weights[16:32, weight]
    vector = [row * along_y for row in rows]
    for at, plane in enumerate(planes):
        along_x = plane_weights[plane : plane + 1, weight]
        for c in range(3):
            top, rest = halves(vector[c] * along_x)
            row = (c * len(planes) + at) * YPAD
            left_high[row : row + YPAD, place] = top
            left_low[row : row + YPAD, place] = rest


def spread_columns(left_high, left_low, z_high, z_low, left, right):
    total = transposed_dot(left_high[:, left], z_high[:, right]) + transposed_dot(left_low[:, left], z_high[:, right])
    return total + transposed_dot(left_high[:, left], z_low[:, right])


def spread_group(refs, planes, plane_weights, z_high, z_low, used, left_high, left_low, total, begun=None, part0=0):
    count = len(refs)
    for at, (ref, first) in enumerate(refs):
        part = part0 + at
        for half in range(2):
            place = slice(at * 256 + half * 128, at * 256 + half * 128 + 128)
            weight = slice(part * 256 + half * 128, part * 256 + half * 128 + 128)
            rows = [ref[first + 2 * c + half : first + 2 * c + half + 1, :] for c in range(3)]
            fill_tile(rows, planes, plane_weights, weight, left_high, left_low, place)
        place = slice(count * 256 + at * 128, count * 256 + at * 128 + 128)
        weight = slice(FIRST + part * 128, FIRST + part * 128 + 128)
        rows = [ref[first + 8 + c : first + 9 + c, :] for c in range(3)]
        fill_tile(rows, planes, plane_weights, weight, left_high, left_low, place)
    value = spread_columns(
        left_high, left_low, z_high, z_low, slice(0, count * 256), slice(part0 * 256, (part0 + count) * 256)
    )
    value = value + spread_columns(
        left_high, left_low, z_high, z_low, slice(count * 256, count * 384),
        slice(FIRST + part0 * 128, FIRST + (part0 + count) * 128),
    )
    total[...] = value if begun is None else value + begun[...]

    def further(block, carry):
        for at, (ref, first) in enumerate(refs):
            column = pl.multiple_of(STATIC + (block - 1) * 384 + (part0 + at) * 128, 128)
            rows = [ref[pl.ds(first + 8 + 3 * block + c, 1), :] for c in range(3)]
            place = slice(at * 128, at * 128 + 128)
            fill_tile(rows, planes, plane_weights, pl.ds(column, 128), left_high, left_low, place)
        right = pl.ds(pl.multiple_of(STATIC + (block - 1) * 384 + part0 * 128, 128), count * 128)
        total[...] += spread_columns(left_high, left_low, z_high, z_low, slice(0, count * 128), right)
        return carry

    lax.fori_loop(1, used, further, 0)


def respond(moved, planes, outs, scale, velocity_high, velocity_low):
    axial, diagonal = 1.0 / 6.0, 1.0 / 12.0
    up_y = lambda a: pltpu.roll(a, 1, 0)
    down_y = lambda a: pltpu.roll(a, YPAD - 1, 0)
    up_z = lambda a: pltpu.roll(a, 1, 1)
    down_z = lambda a: pltpu.roll(a, LANES - 1, 1)
    onward, back, still = {}, {}, {}
    for at, plane in enumerate(planes):
        factor = scale[plane * YPAD : plane * YPAD + YPAD, :]
        rows = [(c * len(planes) + at) * YPAD for c in range(3)]
        gx, gy, gz = (moved[row : row + YPAD, :] * factor for row in rows)
        hx, hy, hz = gx * diagonal, gy * diagonal, gz * diagonal
        sum_xy, dif_xy = hx + hy, hx - hy
        zx_up, zy_up, zz_up = up_z(hx), up_z(hy), up_z(hz)
        zx_dn, zy_dn, zz_dn = down_z(hx), down_z(hy), down_z(hz)
        xz_sum_up, xz_sum_dn, xz_dif_up, xz_dif_dn = zx_up + zz_up, zx_dn + zz_dn, zx_up - zz_up, zx_dn - zz_dn
        xy_sum_up, xy_sum_dn, xy_dif_up, xy_dif_dn = up_y(sum_xy), down_y(sum_xy), up_y(dif_xy), down_y(dif_xy)
        ax = gx * axial
        onward[plane] = (
            ax + ((xy_sum_up + xy_dif_dn) + (xz_sum_up + xz_dif_dn)),
            xy_sum_up - xy_dif_dn,
            xz_sum_up - xz_dif_dn,
        )
        back[plane] = (
            ax + ((xy_sum_dn + xy_dif_up) + (xz_sum_dn + xz_dif_up)),
            xy_sum_dn - xy_dif_up,
            xz_sum_dn - xz_dif_up,
        )
        yz_same = up_y(zy_up + zz_up)
        yz_same_dn = down_y(zy_dn + zz_dn)
        yz_cross = up_y(zy_dn - zz_dn)
        yz_cross_dn = down_y(zy_up - zz_up)
        same, cross = yz_same + yz_same_dn, yz_cross + yz_cross_dn
        still[plane] = (
            gx,
            gy + ((up_y(hy) + down_y(hy)) * 2.0 + (same + cross)),
            gz + ((zz_up + zz_dn) * 2.0 + (same - cross)),
        )
        for place, out in enumerate(outs):
            if min(out + 1, planes[-1]) != plane:
                continue
            factor = scale[out * YPAD : out * YPAD + YPAD, :] * 0.5
            for c in range(3):
                parts = [group[at][c] for group, at in ((onward, out - 1), (still, out), (back, out + 1)) if at in group]
                total = parts[0]
                for part in parts[1:]:
                    total = total + part
                top, rest = halves(total * factor)
                row = (c * len(outs) + place) * YPAD
                velocity_high[row : row + YPAD, :] = top
                velocity_low[row : row + YPAD, :] = rest


def own_spread(own, plane_weights, z_high, z_low, used, total, left_high, left_low):
    spread_group([(own, 0)], range(1, 12), plane_weights, z_high, z_low, trips(used), left_high, left_low, total)


def own_image(
    begun, apart, near, plane_weights, z_high, z_low, used, scale, result, left_high, left_low, moved, velocity_high,
    velocity_low, halo=True,
):
    refs = [(apart, 0), (near, 0)]
    planes = range(1, 12)
    count = trips(used)
    spread_group(refs, planes, plane_weights, z_high, z_low, count, left_high, left_low, moved, begun, 1)
    respond(moved, planes, planes, scale, velocity_high, velocity_low)
    interpolate(velocity_high, velocity_low, planes, plane_weights, z_high, z_low, count, result, halo)


def side_image(
    below, begun, three, own_tables, own_used, side_tables, used, scale, left_high, left_low, moved, velocity_high,
    velocity_low, image, halo=True,
):
    planes, outs = (range(0, 4), range(1, 5)) if below else (range(9, 13), range(8, 12))
    refs = [(three, 24 * part) for part in range(3)]
    spread_group(refs, planes, *side_tables, trips(used), left_high, left_low, moved)
    respond(moved, planes, outs, scale, velocity_high, velocity_low)
    interpolate(velocity_high, velocity_low, outs, *own_tables, trips(own_used), image, halo)
    return begun[...] + image[...]


def below_kernel(begun, three, w, h, l, own_used, sw, sh, sl, used, scale, result, *scratch, halo=True):
    result[...] = side_image(
        True, begun, three, (w, h, l), own_used, (sw, sh, sl), used, scale, *scratch, halo=halo
    )


def above_image(begun, three, w, h, l, own_used, sw, sh, sl, used, scale, aux, vector, *scratch, halo=True):
    image = side_image(False, begun, three, (w, h, l), own_used, (sw, sh, sl), used, scale, *scratch, halo=halo)
    return aux[0:24, :] * (image + aux[24:48, :] * vector[...])


def above_kernel(begun, three, w, h, l, own_used, sw, sh, sl, used, scale, aux, vector, result, *scratch):
    result[...] = above_image(begun, three, w, h, l, own_used, sw, sh, sl, used, scale, aux, vector, *scratch)


def two_sum(a, b):
    total = a + b
    part = total - a
    return total, (a - (total - part)) + (b - part)


def fast_two_sum(a, b):
    total = a + b
    return total, b - (total - a)


def split(a):
    scaled = a * 4097.0
    high = scaled - (scaled - a)
    return high, a - high


def two_product(a, b):
    product = a * b
    a_high, a_low = split(a)
    b_high, b_low = split(b)
    return product, ((a_high * b_high - product) + a_high * b_low + a_low * b_high) + a_low * b_low


def pair_add(a, b):
    head, tail = two_sum(a[0], b[0])
    return fast_two_sum(head, tail + (a[1] + b[1]))


def pair_negative(a):
    return (-a[0], -a[1])


def pair_multiply(a, b):
    head, tail = two_product(a[0], b[0])
    return fast_two_sum(head, tail + (a[0] * b[1] + a[1] * b[0]))


def pair_divide(a, b):
    first = a[0] / b[0]
    rest = pair_add(a, pair_negative(pair_multiply((first, jnp.zeros_like(first)), b)))
    return fast_two_sum(first, rest[0] / b[0])


ENTRIES = ((0, 0), (0, 1), (0, 2), (0, 3), (1, 1), (1, 2), (1, 3), (2, 2), (2, 3))


def gram_lanes(vectors, entries, packed):
    lane = lax.broadcasted_iota(jnp.int32, (8, 128), 1)
    for at, (i, j) in enumerate(ENTRIES):
        if (i, j) not in entries:
            continue
        value = two_product(vectors[i], vectors[j])
        for axis, steps in ((0, (4, 2, 1)), (1, (64, 32, 16, 8, 4, 2, 1))):
            for step in steps:
                value = pair_add(value, (pltpu.roll(value[0], step, axis), pltpu.roll(value[1], step, axis)))
        packed = jnp.where(lane == at, value[0], jnp.where(lane == 16 + at, value[1], packed))
    return packed


EARLY = tuple(entry for entry in ENTRIES if entry[1] < 3)
LATE = tuple(entry for entry in ENTRIES if entry[1] == 3)


def own_spread_last(own, w, h, l, used, first, second, total, early, *scratch):
    own_spread(own, w, h, l, used, total, *scratch)
    early[...] = gram_lanes([first[0:8, :], second[0:8, :], own[0:8, :]], EARLY, jnp.zeros((8, 128), F32))


def last_kernel(
    begun, three, w, h, l, own_used, sw, sh, sl, used, scale, aux, third, first, second, early, sums, *scratch
):
    fourth = above_image(begun, three, w, h, l, own_used, sw, sh, sl, used, scale, aux, third, *scratch, halo=False)
    vectors = [first[0:8, :], second[0:8, :], third[0:8, :], fourth[0:8]]
    packed = gram_lanes(vectors, LATE, early[...])
    for block in range(sums.shape[0] // 8):
        sums[block * 8 : block * 8 + 8, :] = packed


def finish_kernel(gathered, first, second, third, forces):
    a = gathered[...]
    count = a.shape[0]
    value = (a, pltpu.roll(a, 112, 1))
    while count > 8:
        count //= 2
        value = pair_add(
            (value[0][0:count], value[1][0:count]), (value[0][count : 2 * count], value[1][count : 2 * count])
        )
    for step in (4, 2, 1):
        value = pair_add(value, (pltpu.roll(value[0], step, 0), pltpu.roll(value[1], step, 0)))
    lane = lax.broadcasted_iota(jnp.int32, (8, 128), 1)
    gram = {}
    for at, (i, j) in enumerate(ENTRIES):
        entry = tuple(
            jnp.broadcast_to(jnp.sum(jnp.where(lane == at, v, 0.0), axis=1, keepdims=True), (8, 128)) for v in value
        )
        gram[i, j] = entry
        gram[j, i] = entry
    add, times = pair_add, pair_multiply
    minus = lambda a, b: pair_add(a, pair_negative(b))

    def form(left, right, shift):
        total = None
        for i, a in enumerate(left):
            for j, b in enumerate(right):
                term = times(times(a, b), gram[i, j + shift])
                total = term if total is None else add(total, term)
        return total

    one = (jnp.ones((8, 128), F32), jnp.zeros((8, 128), F32))
    alpha0 = pair_divide(gram[0, 0], gram[0, 1])
    residual = [one, pair_negative(alpha0)]
    norm1 = form(residual, residual, 0)
    beta0 = pair_divide(norm1, gram[0, 0])
    along1 = [add(one, beta0), pair_negative(alpha0)]
    alpha1 = pair_divide(norm1, form(along1, along1, 1))
    residual = [one, minus(residual[1], times(alpha1, along1[0])), pair_negative(times(alpha1, along1[1]))]
    norm2 = form(residual, residual, 0)
    beta1 = pair_divide(norm2, norm1)
    along2 = [add(one, times(beta1, along1[0])), add(residual[1], times(beta1, along1[1])), residual[2]]
    alpha2 = pair_divide(norm2, form(along2, along2, 1))
    weight0 = add(alpha0, add(times(alpha1, along1[0]), times(alpha2, along2[0])))
    weight1 = add(times(alpha1, along1[1]), times(alpha2, along2[1]))
    weight2 = times(alpha2, along2[2])
    total = weight0[0] * first[0:8, :] + (weight1[0] * second[0:8, :] + weight2[0] * third[0:8, :])
    for c in range(3):
        forces[c : c + 1, 0:128] = total[2 * c : 2 * c + 1, :]
        forces[c : c + 1, 128:256] = total[2 * c + 1 : 2 * c + 2, :]


def call(kernel, name, outs, *operands, memory=None, scratch=()):
    spec = lambda space: pl.BlockSpec(memory_space=space)
    memory = memory or [pltpu.VMEM] * len(operands)
    return pl.pallas_call(
        kernel,
        name=name,
        out_shape=[jax.ShapeDtypeStruct(shape, kind) for shape, kind in outs],
        in_specs=[spec(space) for space in memory],
        out_specs=[spec(pltpu.VMEM)] * len(outs),
        scratch_shapes=list(scratch),
        compiler_params=PARAMS,
    )(*operands)


def body(density, base_velocity, cells, offsets, target, stiffness, counts):
    rows = lambda n: ((n, 128), F32)
    vmem, smem, hbm = pltpu.VMEM, pltpu.SMEM, pltpu.HBM
    table_shapes = [((32, COLS), F32), ((256, COLS), BF16), ((256, COLS), BF16)]
    used_shape = [((8, 128), jnp.int32)]
    arguments = (density, base_velocity, cells, offsets, target, stiffness.reshape(1, MARKERS))
    fields, own, to_odd, to_even = call(
        pack_kernel, "pack", [rows(256), rows(24), rows(80), rows(80)],
        *(pltpu.with_memory_space_constraint(a, hbm) for a in arguments), counts,
        memory=[hbm] * 6 + [smem],
        scratch=[
            vmem((8, 8, 128), F32), vmem((3, 8, 8, 128), F32), vmem((3, MARKERS), jnp.int32),
            vmem((3, MARKERS), F32), vmem((3, MARKERS), F32), vmem((1, MARKERS), F32),
            pltpu.SemaphoreType.DMA((6,)), vmem((80, 128), F32), vmem((80, 128), F32),
        ],
    )
    odd, even = swapped_z(to_odd, to_even)
    wide, marks, aux, to_apart, to_near = call(
        deepen_z_kernel, "deepen_z", [rows(320), rows(40), rows(72), rows(136), rows(136)], fields, own, odd, even,
        scratch=[vmem((136, 128), F32)] * 2 + [vmem((80, 128), F32)] * 2,
    )
    apart, near = swapped_y(to_apart, to_near)
    deep, three, upward, downward = call(
        deepen_y_kernel, "deepen_y", [rows(640), rows(120), rows(216), rows(280)], wide, marks, apart, near,
        scratch=[vmem((136, 128), F32)] * 2,
    )
    below, above = shifted(upward, "gx", 1), shifted(downward, "gx", -1)
    own_tables = call(
        own_tables_kernel, "own_tables", table_shapes + used_shape, three
    )
    side_tables = call(
        side_tables_kernel, "side_tables", table_shapes * 2 + used_shape, below, above
    )
    velocity_scratch = [vmem((3 * INNER, LANES), BF16)] * 2
    image_scratch = vmem((24, 128), F32)
    scale, start = call(
        setup_kernel, "setup", [((ROWS, LANES), F32), rows(24)], deep, below, above, *own_tables[0:3], aux, own_tables[3],
        scratch=velocity_scratch + [image_scratch],
    )

    def image_of(last, vector, *others):
        apart, near = swapped_y(vector, vector)
        begun = call(
            own_spread_last if last else own_spread, "own_spread",
            [((3 * INNER, LANES), F32)] + ([rows(8)] if last else []), vector, *own_tables, *others,
            scratch=[vmem((3 * INNER, 384), BF16)] * 2,
        )
        held = list(begun) + (list(side_tables) if vector is start else [])
        three = lax.optimization_barrier((jnp.concatenate([vector, apart, near], axis=0), *held))[0]
        below_three, above_three = shifted(three, "gx", 1), shifted(three, "gx", -1)
        (own_part,) = call(
            functools.partial(own_image, halo=not last), "own_image", [rows(24)], begun[0], apart, near, *own_tables, scale,
            scratch=[vmem((3 * INNER, 768), BF16)] * 2 + [vmem((3 * INNER, LANES), F32)] + velocity_scratch,
        )
        side_scratch = [vmem((192, STATIC), BF16)] * 2 + [vmem((192, LANES), F32)]
        side_scratch += [vmem((192, LANES), BF16)] * 2 + [image_scratch]
        (part,) = call(
            functools.partial(below_kernel, halo=not last), "below", [rows(24)], own_part, below_three, *own_tables, *side_tables[0:3], side_tables[6], scale,
            scratch=side_scratch,
        )
        (result,) = call(
            last_kernel if last else above_kernel, "above", [rows(256 if last else 24)],
            part, above_three, *own_tables, *side_tables[3:7], scale, aux, vector, *others, *begun[1:],
            scratch=side_scratch,
        )
        return result

    second = image_of(False, start)
    third = image_of(False, second)
    sums = image_of(True, third, start, second)
    gathered = lax.all_to_all(sums, GX_GY_GZ, 0, 0, tiled=True)
    (forces,) = call(finish_kernel, "finish", [((3, MARKERS), F32)], gathered, start, second, third)
    return forces


def solution(mesh):
    finer = Mesh(
        mesh.devices.reshape(mesh.shape["gx"], 4, 2, mesh.shape["gz"]), ("gx", "gy_0", "gy_1", "gz")
    )
    return jax.shard_map(
        body,
        mesh=finer,
        in_specs=(
            P("gx", GY, "gz"),
            P(None, "gx", GY, "gz"),
            P(None, GX_GY_GZ),
            P(None, GX_GY_GZ),
            P(None, GX_GY_GZ),
            P(GX_GY_GZ),
            P(GX_GY_GZ),
        ),
        out_specs=P(None, GX_GY_GZ),
        check_vma=False,
    )
```
